8 devices in a mesh: ens: 1 (over z), col: 2 (over y), row: 4 (over x, core).
Axes of the slice: x: 2, y: 2, z: 1, core: 2. Of those that a mesh axis runs over, the one named last changes fastest.
Arguments:
- vel_re: float32 [64, 3, 32, 32, 16], P('ens', None, None, 'row', 'col')
- vel_im: float32 [64, 3, 32, 32, 16], P('ens', None, None, 'row', 'col')
- scal_re: float32 [64, 32, 32, 16], P('ens', None, 'row', 'col')
- scal_im: float32 [64, 32, 32, 16], P('ens', None, 'row', 'col')
Outputs:
- output 1: float32 [64, 3, 32, 32, 16], P('ens', None, None, 'row', 'col')
- output 2: float32 [64, 3, 32, 32, 16], P('ens', None, None, 'row', 'col')
- output 3: float32 [64, 32, 32, 16], P('ens', None, 'row', 'col')
- output 4: float32 [64, 32, 32, 16], P('ens', None, 'row', 'col')
All inputs are finite; a program needn't handle non-finite values.
Results may differ from the reference program's by a relative error of at most 0.001.
Values are sent between devices in bfloat16 or wider.
A program may use at most 1 GiB of HBM per device.

```python
import math
import jax
import jax.numpy as jnp
from jax import lax

GRID = 32
BATCH = 64
TWO_PI = 2.0 * math.pi


def spectral_grid():
    index_full = jnp.arange(GRID)
    modes_full = jnp.where(index_full < GRID // 2, index_full, index_full - GRID)
    modes_half = jnp.arange(GRID // 2)
    k_scale = TWO_PI / GRID
    k_x = (modes_full * k_scale).astype(jnp.float32)[:, None, None]
    k_y = (modes_full * k_scale).astype(jnp.float32)[None, :, None]
    k_z = (modes_half * k_scale).astype(jnp.float32)[None, None, :]
    band_full = 3 * jnp.abs(modes_full) < GRID
    band_half = 3 * modes_half < GRID
    keep_mask = band_full[:, None, None] & band_full[None, :, None] & band_half[None, None, :]
    return k_x, k_y, k_z, keep_mask


def to_physical(coeffs):
    return jnp.fft.irfftn(coeffs, s=(GRID, GRID, GRID), axes=(-3, -2, -1), norm='ortho')


def to_spectral(values):
    return jnp.fft.rfftn(values, axes=(-3, -2, -1), norm='ortho')[..., : GRID // 2]


def leray_project(vec_hat, k_x, k_y, k_z):
    k_sq = k_x * k_x + k_y * k_y + k_z * k_z
    inv_sq = jnp.where(k_sq > 0, 1.0 / jnp.where(k_sq > 0, k_sq, 1.0), 0.0)
    comp_x = vec_hat[..., 0, :, :, :]
    comp_y = vec_hat[..., 1, :, :, :]
    comp_z = vec_hat[..., 2, :, :, :]
    k_dot = (k_x * comp_x + k_y * comp_y + k_z * comp_z) * inv_sq
    return jnp.stack([comp_x - k_x * k_dot, comp_y - k_y * k_dot, comp_z - k_z * k_dot], axis=-4)


def unit_rms(values, norm_axes):
    return values / jnp.sqrt(jnp.mean(values * values, axis=norm_axes, keepdims=True))


def band_noise(base_key, lead_dims):
    keep_mask = spectral_grid()[3]
    re_key, im_key = jax.random.split(base_key)
    full_shape = lead_dims + (GRID, GRID, GRID // 2)
    coeffs = lax.complex(jax.random.normal(re_key, full_shape, jnp.float32), jax.random.normal(im_key, full_shape, jnp.float32))
    return jnp.where(keep_mask, coeffs, 0.0)


def setup_inputs(seed: int = 0, part: int = 0) -> dict:
    base_key = jax.random.fold_in(jax.random.key(seed), part)
    vel_key, scal_key = jax.random.split(base_key)
    k_x, k_y, k_z, keep_mask = spectral_grid()
    vel_hat = leray_project(band_noise(vel_key, (BATCH, 3)), k_x, k_y, k_z)
    vel_phys = unit_rms(to_physical(vel_hat), (1, 2, 3, 4))
    vel_hat = jnp.where(keep_mask, to_spectral(vel_phys), 0.0)
    scal_phys = unit_rms(to_physical(band_noise(scal_key, (BATCH,))), (1, 2, 3))
    scal_hat = jnp.where(keep_mask, to_spectral(scal_phys), 0.0)
    return {
        'vel_re': jnp.real(vel_hat).astype(jnp.float32),
        'vel_im': jnp.imag(vel_hat).astype(jnp.float32),
        'scal_re': jnp.real(scal_hat).astype(jnp.float32),
        'scal_im': jnp.imag(scal_hat).astype(jnp.float32),
    }


def one_flow(flow_arrays):
    vel_re, vel_im, scal_re, scal_im = flow_arrays
    k_x, k_y, k_z, keep_mask = spectral_grid()
    k_sq = k_x * k_x + k_y * k_y + k_z * k_z
    keep_mask = keep_mask & (k_sq > 0)
    vel_hat = lax.complex(vel_re, vel_im)
    u_x, u_y, u_z = vel_hat[0], vel_hat[1], vel_hat[2]
    vort_hat = 1j * jnp.stack([k_y * u_z - k_z * u_y, k_z * u_x - k_x * u_z, k_x * u_y - k_y * u_x])
    vel_phys = to_physical(vel_hat)
    vort_phys = to_physical(vort_hat)
    scal_phys = to_physical(lax.complex(scal_re, scal_im))
    v_x, v_y, v_z = vel_phys[0], vel_phys[1], vel_phys[2]
    w_x, w_y, w_z = vort_phys[0], vort_phys[1], vort_phys[2]
    cross_prod = jnp.stack([v_y * w_z - v_z * w_y, v_z * w_x - v_x * w_z, v_x * w_y - v_y * w_x])
    scal_flux = vel_phys * scal_phys[None]
    cross_hat = jnp.where(keep_mask, to_spectral(cross_prod), 0.0)
    flux_hat = jnp.where(keep_mask, to_spectral(scal_flux), 0.0)
    vel_rhs = leray_project(cross_hat, k_x, k_y, k_z)
    scal_rhs = -1j * (k_x * flux_hat[0] + k_y * flux_hat[1] + k_z * flux_hat[2])
    return jnp.real(vel_rhs), jnp.imag(vel_rhs), jnp.real(scal_rhs), jnp.imag(scal_rhs)


def reference(vel_re, vel_im, scal_re, scal_im):
    rhs_re, rhs_im, scal_rhs_re, scal_rhs_im = lax.map(one_flow, (vel_re, vel_im, scal_re, scal_im))
    return (rhs_re, rhs_im, scal_rhs_re, scal_rhs_im)
```

```python
import math

import jax
import jax.numpy as jnp
import numpy as np
from jax import lax
from jax.experimental import pallas as pl
from jax.experimental.pallas import tpu as pltpu
from jax.sharding import PartitionSpec as P

N = 32
LANES = 128
FLOWS = 64
ROWS = 2048
TILE = (8, LANES)
D_TILES, S_TILES = 24, 12
K = 256
COLS = 512
TINY = 1e-9
MIB = 1 << 20
PAIR, VEC, FIELDS, PEERS = range(2), range(3), range(4), range(1, 8)
MESH = pl.DeviceIdType.MESH
F32 = jnp.float32
BF16 = jnp.bfloat16
SLOTS = list(range(S_TILES)) + list(range(20, 32))
OWNERS = [("D", 0, 0, 0), ("D", 0, 3, 32), ("S", 0, 1, FLOWS), ("S", 0, 2, 68),
          ("D", 1, 0, 84), ("D", 1, 3, 86), ("S", 1, 1, 116), ("S", 1, 2, 110)]

FIRST = [0, 32, FLOWS, 76]


def mode(j):
    return j if j < N // 2 else j - N


def kept(m):
    return 3 * abs(m) < N


def lane_owner(lane):
    if lane < OWNERS[4][3]:
        return sum(lane >= first for first in FIRST[1:4])
    base = 4 if lane < OWNERS[6][3] else 6
    return base + (lane % 4) // 2


def lane_mode(lane, parity):
    own = lane_owner(lane)
    kind, col, row, start = OWNERS[own]
    off = lane - start
    ky_local, kz_half = off // 4, off % 4
    if row == 2:
        ky_local += 4
    if own == 7 and ky_local > 7:
        return None
    ky = mode(8 * row + ky_local)
    kz = 8 * col + 2 * kz_half + parity
    if not (kept(ky) and kept(kz)):
        return None
    return ky, kz


def split3(x):
    x = np.asarray(x, np.float32)
    hi = x.astype(BF16)
    rest = x - hi.astype(np.float32)
    mid = rest.astype(BF16)
    low = (rest - mid.astype(np.float32)).astype(BF16)
    return np.stack([hi, mid, low])


def tables():
    scale = float(N) ** -1.5
    inv = np.zeros((2, K, COLS))
    fwd = np.zeros((2, COLS, K))
    ky_t = np.zeros((2, LANES))
    kz_t = np.zeros((2, LANES))
    yy, zz = np.meshgrid(np.arange(N), np.arange(N // 2), indexing="ij")
    for parity in PAIR:
        for lane in range(LANES):
            got = lane_mode(lane, parity)
            if got is None:
                continue
            ky, kz = got
            ang = 2 * np.pi * ((ky * yy + kz * zz) % N).reshape(-1) / N
            weight = 1.0 if kz == 0 else 2.0
            inv[parity, lane] = weight * scale * np.cos(ang)
            inv[parity, LANES + lane] = -weight * scale * np.sin(ang)
            fwd[parity, :, lane] = scale * np.cos(ang)
            fwd[parity, :, LANES + lane] = -scale * np.sin(ang)
            ky_t[parity, lane] = ky
            kz_t[parity, lane] = kz
    unit = 2 * np.pi / N
    inv3 = np.stack([split3(inv[p]) for p in PAIR])
    fwd3 = np.stack([split3(fwd[p]) for p in PAIR])
    wave = np.zeros((2, 2, 8, LANES), np.float32)
    wave[:, 0] = (ky_t * unit)[:, None]
    wave[:, 1] = (kz_t * unit)[:, None]
    kx = np.array([mode(j) for j in SLOTS]) * unit
    k_sq = kx[None, :, None] ** 2 + ((ky_t * unit) ** 2 + (kz_t * unit) ** 2)[:, None]
    ok = (k_sq > 0) & np.array([kept(mode(j)) for j in SLOTS])[None, :, None]
    inv_sq = np.where(ok, 1.0 / np.where(k_sq > 0, k_sq, 1.0), 0.0)
    proj = np.zeros((2, D_TILES, 2, 8, LANES), np.float32)
    proj[:, :, 0] = inv_sq[:, :, None]
    proj[:, :, 1] = ok[:, :, None]
    return inv3, fwd3, wave, proj


def cmul_const(a, c, s):
    re, im = a
    if abs(s) < TINY:
        return (re, im) if c > 0 else (-re, -im)
    if abs(c) < TINY:
        return (-im, re) if s > 0 else (im, -re)
    if abs(abs(c) - abs(s)) < TINY:
        r = abs(c)
        sc, ss = (1 if c > 0 else -1), (1 if s > 0 else -1)
        p, q = (re - im) * r, (re + im) * r
        if sc > 0 and ss > 0:
            return p, q
        if sc > 0:
            return q, -p
        if ss > 0:
            return -q, p
        return -p, -q
    return re * c - im * s, re * s + im * c


def fft(vals, sign):
    n = len(vals)
    if n == 1:
        return list(vals)
    even, odd = fft(vals[0::2], sign), fft(vals[1::2], sign)
    out = [None] * n
    for k in range(n // 2):
        a, b = even[k], odd[k]
        if b is not None:
            ang = sign * 2 * math.pi * k / n
            b = cmul_const(b, math.cos(ang), math.sin(ang))
        if a is None and b is None:
            continue
        if b is None:
            out[k], out[k + n // 2] = a, a
        elif a is None:
            out[k], out[k + n // 2] = b, (-b[0], -b[1])
        else:
            out[k] = (a[0] + b[0], a[1] + b[1])
            out[k + n // 2] = (a[0] - b[0], a[1] - b[1])
    return out


def dot(a, b):
    return jnp.dot(a, b, preferred_element_type=F32)


def split_bf16(x):
    hi = x.astype(BF16)
    rest = x - hi.astype(F32)
    mid = rest.astype(BF16)
    low = (rest - mid.astype(F32)).astype(BF16)
    return hi, mid, low


def dev_of(row, col):
    return col * 4 + row


def slot_of(row, col):
    return col * 2 + (1 if row >= 2 else 0)


def six_products(parts, table):
    hi, mid, low = parts
    t_hi, t_mid, t_low = (table[p] for p in VEC)
    acc = dot(low, t_hi) + dot(hi, t_low) + dot(mid, t_mid)
    return acc + dot(mid, t_hi) + dot(hi, t_mid) + dot(hi, t_hi)


def main_kernel(vre, vim, sre, sim, inv_hbm, fwd_hbm, wave, proj, back,
                xin, send, recv_d, recv_s, merged, lhs, phys, prod, spec, res, ret_d, ret_s,
                inv, fwd, in_sem, tab_sem, s1, r1, s2, r2):
    row, col, ens = lax.axis_index("row"), lax.axis_index("col"), lax.axis_index("ens")
    me = dev_of(row, col)
    dense = jnp.logical_or(row == 0, row == 3)
    sparse = jnp.logical_not(dense)
    my_slot = col * 2 + jnp.where(row >= 2, 1, 0)

    loads = []
    for f in FIELDS:
        for ri in PAIR:
            src = (vre, vim)[ri].at[f] if f < 3 else (sre, sim)[ri].at[0]
            for half in PAIR:
                cp = pltpu.make_async_copy(
                    src.at[pl.ds(1280 * half, 768)], xin.at[f, ri, pl.ds(768 * half, 768)], in_sem.at[f, ri, half])
                cp.start()
                loads.append(cp)
    tab = [pltpu.make_async_copy(inv_hbm, inv, tab_sem.at[0]), pltpu.make_async_copy(fwd_hbm, fwd, tab_sem.at[1])]
    for cp in tab:
        cp.start()

    barrier = pltpu.get_barrier_semaphore()

    def peer(k):
        return row ^ (k % 4), col ^ (k // 4)

    for k in PEERS:
        pr, pc = peer(k)
        pl.semaphore_signal(barrier, inc=1, device_id=(ens, pc, pr), device_id_type=MESH)
    pl.semaphore_wait(barrier, 7)

    def pack_dense(f):
        def body(t, carry):
            ri, rest = t // S_TILES, t % S_TILES
            b, q = rest // 6, rest % 6
            blk = xin[f, ri, pl.ds(q * K + b, LANES, stride=2), :]
            send[:, f, t] = blk.T.reshape(8, *TILE)
            return carry
        lax.fori_loop(0, D_TILES, body, 0, unroll=2)

    def pack_sparse(f):
        first = jnp.where(row == 1, 0, 32)

        def body(t, carry):
            ri, rest = t // 6, t % 6
            b, g = rest // 3, rest % 3
            parts = [xin[f, ri, pl.ds(g * COLS + s * FLOWS + first + b, 16, stride=2), :] for s in range(8)]
            send[:, f, t] = jnp.concatenate(parts, axis=0).T.reshape(8, *TILE)
            return carry
        lax.fori_loop(0, S_TILES, body, 0, unroll=2)

    def first_copy(kind, f, pr, pc):
        to = dev_of(pr, pc)
        if kind == "D":
            src, dst = send.at[to, f], recv_d.at[my_slot, f]
        else:
            src, dst = send.at[to, f, pl.ds(0, S_TILES)], recv_s.at[my_slot, f]
        return pltpu.make_async_remote_copy(
            src_ref=src, dst_ref=dst, send_sem=s1.at[to, f], recv_sem=r1.at[me, f],
            device_id=(ens, pc, pr), device_id_type=MESH)

    for f in FIELDS:
        for cp in loads[4 * f:4 * f + 4]:
            cp.wait()

        @pl.when(dense)
        def _():
            pack_dense(f)
            for k in PEERS:
                first_copy("D", f, *peer(k)).start()
            recv_d[my_slot, f] = send[me, f]

        @pl.when(sparse)
        def _():
            pack_sparse(f)
            for k in PEERS:
                first_copy("S", f, *peer(k)).start()
            recv_s[my_slot, f] = send[me, f, 0:S_TILES]

    lane = lax.broadcasted_iota(jnp.int32, TILE, 1)
    low = lane % 4 < 2
    edges = FIRST + [OWNERS[4][3], OWNERS[6][3], LANES]
    spans = [(lane >= lo) & (lane < hi) for lo, hi in zip(edges[:-1], edges[1:])]
    owned = spans[:4] + [spans[4] & low, spans[4] & ~low, spans[5] & low, spans[5] & ~low]

    def wait_field(f):
        for kind, c, r, _ in OWNERS:
            d = dev_of(r, c)
            slot = slot_of(r, c)

            @pl.when(me != d)
            def _():
                if kind == "D":
                    src, dst = send.at[d, f], recv_d.at[slot, f]
                else:
                    src, dst = send.at[d, f, pl.ds(0, S_TILES)], recv_s.at[slot, f]
                pltpu.make_async_remote_copy(
                    src_ref=src, dst_ref=dst, send_sem=s1.at[d, f], recv_sem=r1.at[d, f],
                    device_id=(ens, c, r), device_id_type=MESH).wait_recv()

    def merge(f):
        def body(t, carry):
            rb, g = t // 3, t % 3
            for s8 in range(8):
                q, s = 2 * g + s8 // 4, s8 % 4
                acc = None
                for o, (kind, c, r, start) in enumerate(OWNERS):
                    slot = slot_of(r, c)
                    if kind == "D":
                        tile, shift = recv_d[slot, f, rb * 6 + q], (start - 32 * s) % LANES
                    else:
                        tile, shift = recv_s[slot, f, rb * 3 + g], (start - 16 * s8) % LANES
                    if shift:
                        tile = pltpu.roll(tile, shift, 1)
                    acc = tile if acc is None else jnp.where(owned[o], tile, acc)
                merged[f, rb, 8 * g + s8] = acc
            return carry
        lax.fori_loop(0, S_TILES, body, 0)

    def to_x(f, b, get):
        vals = [None] * N
        for i, j in enumerate(SLOTS):
            if kept(mode(j)):
                vals[j] = get(i)
        out = fft(vals, 1)
        for x in range(0, N, 2):
            for ri in PAIR:
                pair = jnp.concatenate([out[x][ri], out[x + 1][ri]], axis=0)
                for p, part in enumerate(split_bf16(pair)):
                    lhs[f, b, 8 * x:8 * x + 16, K * p + LANES * ri:K * p + LANES * ri + LANES] = part

    def field_x(f, src):
        def body(b, carry):
            to_x(f, b, lambda i: (merged[src, b, i], merged[src, 2 + b, i]))
            return carry
        lax.fori_loop(0, 2, body, 0)

    def curl_x(f):
        c1, c2 = (f + 1) % 3, (f + 2) % 3

        def body(b, carry):
            ky, kz = wave[b, 0], wave[b, 1]

            def get(i):
                kx = 2 * math.pi * mode(SLOTS[i]) / N
                ks = (kx, ky, kz)
                im = ks[c1] * merged[c2, b, i] - ks[c2] * merged[c1, b, i]
                re = ks[c2] * merged[c1, 2 + b, i] - ks[c1] * merged[c2, 2 + b, i]
                return re, im
            to_x(3 + f, b, get)
            return carry
        lax.fori_loop(0, 2, body, 0)

    def to_grid(f):
        halves = []
        for b in PAIR:
            halves.append(six_products([lhs[f, b, :, K * p:K * p + K] for p in VEC], inv.at[b]))
        phys[f, 0] = halves[0] + halves[1]
        phys[f, 1] = halves[0] - halves[1]

    def to_spec(c):
        for b in PAIR:
            spec[c, b] = six_products([prod[b, p] for p in VEC], fwd.at[b])

    def fold(rows, n0, n1):
        for b, v in enumerate((n0 + n1, n0 - n1)):
            for p, part in enumerate(split_bf16(v)):
                prod[b, p, rows, :] = part

    def cross(c):
        c1, c2 = (c + 1) % 3, (c + 2) % 3

        def body(i, carry):
            rows = pl.ds(pl.multiple_of(i * 16, 16), 16)
            n = [phys[c1, h, rows, :] * phys[3 + c2, h, rows, :] - phys[c2, h, rows, :] * phys[3 + c1, h, rows, :]
                 for h in PAIR]
            fold(rows, *n)
            return carry
        lax.fori_loop(0, 16, body, 0)
        to_spec(c)

    def flux(c):
        def body(i, carry):
            rows = pl.ds(pl.multiple_of(i * 16, 16), 16)
            fold(rows, *[phys[c, h, rows, :] * phys[6, h, rows, :] for h in PAIR])
            return carry
        lax.fori_loop(0, 16, body, 0)
        to_spec(c)

    def from_x(c):
        def body(b, carry):
            vals = [(spec[c, b, 8 * x:8 * x + 8, 0:LANES], spec[c, b, 8 * x:8 * x + 8, LANES:K]) for x in range(N)]
            out = fft(vals, -1)
            for i, j in enumerate(SLOTS):
                merged[c, b, i] = out[j][0]
                merged[c, 2 + b, i] = out[j][1]
            return carry
        lax.fori_loop(0, 2, body, 0)

    unit = 2 * math.pi / N

    def kx_of(i):
        j = jnp.where(i < S_TILES, i, i - D_TILES)
        return j.astype(F32) * unit

    def project():
        def body(t, carry):
            b, i = t // D_TILES, t % D_TILES
            ks = (kx_of(i), wave[b, 0], wave[b, 1])
            inv_sq, ok = proj[b, i, 0], proj[b, i, 1]
            for ri in PAIR:
                n = [merged[c, 2 * ri + b, i] for c in VEC]
                kd = (ks[0] * n[0] + ks[1] * n[1] + ks[2] * n[2]) * inv_sq
                for c in VEC:
                    res[c, 2 * ri + b, i] = (n[c] - ks[c] * kd) * ok
            return carry
        lax.fori_loop(0, 48, body, 0, unroll=4)

    def diverge():
        def body(t, carry):
            b, i = t // D_TILES, t % D_TILES
            ks = (kx_of(i), wave[b, 0], wave[b, 1])
            ok = proj[b, i, 1]
            sums = [ks[0] * merged[0, 2 * ri + b, i] + ks[1] * merged[1, 2 * ri + b, i] + ks[2] * merged[2, 2 * ri + b, i]
                    for ri in PAIR]
            res[3, b, i] = sums[1] * ok
            res[3, 2 + b, i] = -sums[0] * ok
            return carry
        lax.fori_loop(0, 48, body, 0, unroll=4)

    def unmerge(f):
        zero = jnp.zeros(TILE, F32)

        def body(t, carry):
            rb, g = t // 3, t % 3
            for o, (kind, c, r, start) in enumerate(OWNERS):
                slot = slot_of(r, c)
                width = 32 if kind == "D" else 16
                valid = None
                if kind == "S":
                    valid = lane % 16 < S_TILES if r == 1 else lane % 16 >= 8
                if c == 1:
                    valid = low if valid is None else valid & low
                for part in range(2 if kind == "D" else 1):
                    acc = None
                    for s in range(LANES // width):
                        i = 8 * g + 4 * part + s
                        tile = res[f, rb, i]
                        shift = (width * s - start) % LANES
                        if shift:
                            tile = pltpu.roll(tile, shift, 1)
                        acc = tile if acc is None else jnp.where(lane // width == s, tile, acc)
                    if valid is not None:
                        acc = jnp.where(valid, acc, zero)
                    if kind == "D":
                        ret_d[slot, f, rb * 6 + 2 * g + part] = acc
                    else:
                        ret_s[slot, f, rb * 3 + g] = acc
            return carry
        lax.fori_loop(0, S_TILES, body, 0)

    def second_copy(kind, f, r, c):
        slot = slot_of(r, c)
        if kind == "D":
            src, dst = ret_d.at[slot, f], back.at[me, f]
        else:
            src, dst = ret_s.at[slot, f], back.at[me, f, pl.ds(0, S_TILES)]
        d = dev_of(r, c)
        return pltpu.make_async_remote_copy(
            src_ref=src, dst_ref=dst, send_sem=s2.at[d, f], recv_sem=r2.at[me, f],
            device_id=(ens, c, r), device_id_type=MESH)

    def arrival(kind, k, f):
        pr, pc = peer(k)
        d = dev_of(pr, pc)
        if kind == "D":
            src, dst = ret_d.at[0, f], back.at[d, f]
        else:
            src, dst = ret_s.at[0, f], back.at[d, f, pl.ds(0, S_TILES)]
        return pltpu.make_async_remote_copy(
            src_ref=src, dst_ref=dst, send_sem=s2.at[d, f], recv_sem=r2.at[d, f],
            device_id=(ens, pc, pr), device_id_type=MESH)

    def send_back(f):
        for kind, c, r, _ in OWNERS:
            d = dev_of(r, c)

            @pl.when(me != d)
            def _():
                second_copy(kind, f, r, c).start()

            @pl.when(me == d)
            def _():
                slot = slot_of(r, c)
                if kind == "D":
                    back[d, f] = ret_d[slot, f]
                else:
                    back[d, f, 0:S_TILES] = ret_s[slot, f]

    for f in VEC:
        wait_field(f)
        merge(f)
        field_x(f, f)
    for f in VEC:
        curl_x(f)
    tab[0].wait()
    lax.fori_loop(0, 6, lambda f, carry: (to_grid(f), carry)[1], 0)
    tab[1].wait()
    for c in VEC:
        cross(c)
        from_x(c)
    project()
    for f in VEC:
        unmerge(f)
        send_back(f)
    wait_field(3)
    merge(3)
    field_x(6, 3)
    to_grid(6)
    for c in VEC:
        flux(c)
        from_x(c)
    diverge()
    unmerge(3)
    send_back(3)

    for kind, mine in (("D", dense), ("S", sparse)):
        @pl.when(mine)
        def _():
            for k in PEERS:
                for f in FIELDS:
                    first_copy(kind, f, *peer(k)).wait_send()
                    arrival(kind, k, f).wait_recv()

    for kind, c, r, _ in OWNERS:
        @pl.when(me != dev_of(r, c))
        def _():
            for f in FIELDS:
                second_copy(kind, f, r, c).wait_send()


def out_kernel(back, ore, oim, tre, tim, buf, sem):
    row = lax.axis_index("row")
    dense = jnp.logical_or(row == 0, row == 3)
    copies = []
    for f in FIELDS:
        for ri in PAIR:
            dst = (ore, oim)[ri].at[f] if f < 3 else (tre, tim)[ri].at[0]
            copies.append(pltpu.make_async_copy(buf.at[f, ri], dst, sem.at[f, ri]))
    for f in FIELDS:
        for ri in PAIR:
            buf[f, ri, 768:1280, :] = jnp.zeros((COLS, FLOWS), F32)

            @pl.when(dense)
            def _():
                def body(t, carry):
                    b, q = t // 6, t % 6
                    tile = back[:, f, ri * S_TILES + t].reshape(FLOWS, LANES).T
                    base = q * K + jnp.where(q >= 3, COLS, 0)
                    buf[f, ri, pl.ds(base + b, LANES, stride=2), :] = tile
                    return carry
                lax.fori_loop(0, S_TILES, body, 0, unroll=2)

            @pl.when(jnp.logical_not(dense))
            def _():
                buf[f, ri, 0:768, :] = jnp.zeros((768, FLOWS), F32)
                buf[f, ri, 1280:ROWS, :] = jnp.zeros((768, FLOWS), F32)
                first = jnp.where(row == 1, 0, 32)

                def body(t, carry):
                    b, g = t // 3, t % 3
                    tile = back[:, f, ri * 6 + t].reshape(FLOWS, LANES).T
                    for s in range(8):
                        i = g * 8 + s
                        j = i + jnp.where(i >= S_TILES, 8, 0)
                        buf[f, ri, pl.ds(j * FLOWS + first + b, 16, stride=2), :] = tile[16 * s:16 * s + 16]
                    return carry
                lax.fori_loop(0, 6, body, 0)

            copies[2 * f + ri].start()
    for cp in copies:
        cp.wait()


def solution(mesh):
    spec_vec = P('ens', None, None, 'row', 'col')
    spec_scal = P('ens', None, 'row', 'col')
    inv_np, fwd_np, wave_np, proj_np = tables()

    def local_term(vel_re, vel_im, scal_re, scal_im):
        vec = [jnp.transpose(a, (1, 2, 3, 4, 0)).reshape(3, ROWS, FLOWS) for a in (vel_re, vel_im)]
        scal = [jnp.transpose(a, (1, 2, 3, 0)).reshape(1, ROWS, FLOWS) for a in (scal_re, scal_im)]
        vmem = pl.BlockSpec(memory_space=pltpu.VMEM)
        hbm = pl.BlockSpec(memory_space=pl.ANY)
        dma = pltpu.SemaphoreType.DMA
        links = dma((8, 4))
        all_tiles = (8, 4, D_TILES, *TILE)
        d_buf = pltpu.VMEM((4, 4, D_TILES, *TILE), F32)
        s_buf = pltpu.VMEM((4, 4, S_TILES, *TILE), F32)
        inv_buf = pltpu.VMEM(inv_np.shape, BF16)
        back = pl.pallas_call(
            main_kernel,
            out_shape=jax.ShapeDtypeStruct(all_tiles, F32),
            in_specs=[hbm] * 6 + [vmem] * 2,
            out_specs=vmem,
            scratch_shapes=[
                pltpu.VMEM((4, 2, 1536, FLOWS), F32), pltpu.VMEM(all_tiles, F32), d_buf, s_buf, d_buf,
                pltpu.VMEM((7, 2, K, 3 * K), BF16), pltpu.VMEM((7, 2, K, COLS), F32), inv_buf,
                pltpu.VMEM((3, 2, K, K), F32), d_buf, d_buf, s_buf, inv_buf, pltpu.VMEM(fwd_np.shape, BF16),
                dma((4, 2, 2)), dma((2,)), links, links, links, links,
            ],
            compiler_params=pltpu.CompilerParams(
                collective_id=0, has_side_effects=True, vmem_limit_bytes=60 * MIB),
            name="flow_home",
        )(*vec, *scal, jnp.asarray(inv_np), jnp.asarray(fwd_np), jnp.asarray(wave_np), jnp.asarray(proj_np))
        outs = pl.pallas_call(
            out_kernel,
            out_shape=[jax.ShapeDtypeStruct((3, ROWS, FLOWS), F32)] * 2 + [jax.ShapeDtypeStruct((1, ROWS, FLOWS), F32)] * 2,
            in_specs=[vmem],
            out_specs=[hbm] * 4,
            scratch_shapes=[pltpu.VMEM((4, 2, ROWS, FLOWS), F32), pltpu.SemaphoreType.DMA((4, 2))],
            compiler_params=pltpu.CompilerParams(vmem_limit_bytes=40 * MIB),
            name="lay_out",
        )(back)
        out_v = [jnp.transpose(a.reshape(3, N, 8, 8, FLOWS), (4, 0, 1, 2, 3)) for a in outs[:2]]
        out_s = [jnp.transpose(a.reshape(N, 8, 8, FLOWS), (3, 0, 1, 2)) for a in outs[2:]]
        return (*out_v, *out_s)

    return jax.shard_map(local_term, mesh=mesh, in_specs=(spec_vec, spec_vec, spec_scal, spec_scal),
                         out_specs=(spec_vec, spec_vec, spec_scal, spec_scal), check_vma=False)
```

```python
import math

import jax
import jax.numpy as jnp
import numpy as np
from jax import lax
from jax.experimental import pallas as pl
from jax.experimental.pallas import tpu as pltpu
from jax.sharding import PartitionSpec as P

N = 32
LANES = 128
FLOWS = 64
ROWS = 2048
TILE = (8, LANES)
K = 256
TINY = 1e-9
MIB = 1 << 20
QUAD, OCT, HALF = 4, 8, 16
PAIR, VEC, FIELDS, PEERS = range(2), range(3), range(QUAD), range(1, OCT)
MESH = pl.DeviceIdType.MESH
F32 = jnp.float32
BF16 = jnp.bfloat16
UNIT = 2 * math.pi / N
SLOTS = list(range(11)) + list(range(22, N))
KEPT = len(SLOTS)
KEPT_ROWS = KEPT * FLOWS
LOW_ROWS = 11 * FLOWS
D_OUT, S_OUT, D_RET, S_RET = 21, 11, HALF, OCT
D_CHUNKS, S_CHUNKS = (0, 6, 11, HALF, 21), (0, 3, 6, OCT, 11)
RET_CHUNKS = (0, QUAD, 10, HALF)
DENSE = [(0, 0), (3, 0), (0, 1), (3, 1)]
SPARSE = [(1, 0), (2, 0), (1, 1), (2, 1)]


def mode(j):
    return j if j < N // 2 else j - N


def kept(m):
    return 3 * abs(m) < N


def home_mode(lane, parity):
    block, p = divmod(lane, N)
    y, high, half = p // QUAD, p % QUAD // 2, p % QUAD
    if block < 2:
        row, col = 3 * block, 0
    elif block == 2:
        row, col, half = 3 * high, 1, p % 2
    elif p < 12:
        row, col = 1, 0
    elif p < 20:
        row, col, y = 2, 0, y + 3
    else:
        row, col, half, y = 1 + high, 1, p % 2, y - 5 + 6 * high
    if y > 7:
        return None
    ky, kz = mode(OCT * row + y), OCT * col + 2 * half + parity
    return (ky, kz) if kept(ky) and kept(kz) else None


def source_mode(lane, row, col, parity):
    width = N if row % 3 == 0 else HALF
    block, p = divmod(lane, width)
    slot = block if width == N else block // 2 + QUAD * (block % 2)
    y = p // QUAD + (QUAD if row == 2 else 0)
    ky, kz = mode(OCT * row + y), OCT * col + 2 * (p % QUAD) + parity
    return slot, ((ky, kz) if kept(ky) and kept(kz) else None)


def basis(kx, ky, kz):
    flat, full = math.hypot(kx, ky), math.hypot(kx, ky, kz)
    if full == 0:
        return np.zeros(3), np.zeros(3)
    if flat == 0:
        return np.array([1.0, 0, 0]), np.array([0, 1.0, 0])
    e1 = np.array([ky, -kx, 0]) / flat
    return e1, np.array([kx * kz, ky * kz, -flat * flat]) / (flat * full)


def split3(x):
    x = np.asarray(x, np.float32)
    hi = x.astype(BF16)
    rest = x - hi.astype(np.float32)
    mid = rest.astype(BF16)
    return hi, mid, (rest - mid.astype(np.float32)).astype(BF16)


def tables():
    scale = float(N) ** -1.5
    half = N // 2
    points = [(y, z) for z in range(1, OCT) for y in range(N)] + [(y, z) for z in (0, OCT) for y in range(half)]
    yy, zz = np.array(points).T
    inv = np.zeros((2, 2, LANES, K))
    wave = np.zeros((2, QUAD, LANES), np.float32)
    home = np.zeros((2, KEPT, 5, LANES), np.float32)
    for parity in PAIR:
        for lane in range(LANES):
            got = home_mode(lane, parity)
            if got is None:
                continue
            ky, kz = got
            ang = UNIT * (ky * (yy + 0.5) + kz * zz)
            inv[parity, 0, lane] = scale * np.cos(ang)
            inv[parity, 1, lane] = -scale * np.sin(ang)
            wave[parity, :, lane] = ky * UNIT, kz * UNIT, math.cos(UNIT * ky / 2), math.sin(UNIT * ky / 2)
            for i, j in enumerate(SLOTS):
                e1, e2 = basis(mode(j), ky, kz)
                home[parity, i, :, lane] = *e1[:2], *e2
    fwd = np.swapaxes(inv, 2, 3)
    weight = np.full((2, 1, LANES, 1), 2.0)
    for lane in range(LANES):
        got = home_mode(lane, 0)
        if got is not None and got[1] == 0:
            weight[0, 0, lane] = 1.0
    hi, mid, low = split3(inv * weight)
    inv3 = np.stack([np.concatenate(pair, axis=2) for pair in ((hi, low), (mid, mid), (hi, hi))], axis=2)
    fwd3 = np.concatenate(split3(fwd), axis=3)
    return inv3, fwd3, wave, home.reshape(-1, LANES)


def source_tables():
    out = np.zeros((OCT, 2, S_OUT, 3, LANES), np.float32)
    for row in FIELDS:
        for col in PAIR:
            per = QUAD if row % 3 == 0 else OCT
            for parity in PAIR:
                for lane in range(LANES):
                    slot, got = source_mode(lane, row, col, parity)
                    for t in range(S_OUT):
                        n = t * per + slot
                        i = n // 2
                        if n >= 2 * KEPT:
                            out[dev_of(row, col), parity, t, 0, lane] = 1.0
                        elif got is not None:
                            e1, e2 = basis(mode(SLOTS[i]), *got)
                            out[dev_of(row, col), parity, t, :, lane] = (e2[1], e1[1], e2[2]) if n % 2 else (e1[0], e2[0], 0)
    return out.reshape(OCT, -1, LANES)


def cmul_const(a, c, s):
    re, im = a
    if abs(s) < TINY:
        return (re, im) if c > 0 else (-re, -im)
    if abs(c) < TINY:
        return (-im, re) if s > 0 else (im, -re)
    if abs(abs(c) - abs(s)) < TINY:
        p, q = (re - im) * abs(c), (re + im) * abs(c)
        if c > 0:
            return (p, q) if s > 0 else (q, -p)
        return (-q, p) if s > 0 else (-p, -q)
    return re * c - im * s, re * s + im * c


def fft(vals, sign):
    n = len(vals)
    if n == 1:
        return list(vals)
    even, odd = fft(vals[0::2], sign), fft(vals[1::2], sign)
    out = [None] * n
    for k in range(n // 2):
        a, b = even[k], odd[k]
        if b is not None:
            ang = sign * 2 * math.pi * k / n
            b = cmul_const(b, math.cos(ang), math.sin(ang))
        if a is None and b is None:
            continue
        if b is None:
            out[k], out[k + n // 2] = a, a
        elif a is None:
            out[k], out[k + n // 2] = b, (-b[0], -b[1])
        else:
            out[k] = (a[0] + b[0], a[1] + b[1])
            out[k + n // 2] = (a[0] - b[0], a[1] - b[1])
    return out


def dot(a, b):
    return jnp.dot(a, b, preferred_element_type=F32)


def split_bf16(x):
    hi = x.astype(BF16)
    rest = x - hi.astype(F32)
    mid = rest.astype(BF16)
    low = (rest - mid.astype(F32)).astype(BF16)
    return hi, mid, low


def dev_of(row, col):
    return col * QUAD + row


def roll(x, shift):
    return pltpu.roll(x, shift % LANES, 1)


def main_kernel(vre, vim, sre, sim, inv_hbm, fwd_hbm, wave_hbm, home_hbm, back,
                xin, send, recv_d, recv_s, merged, lhs, phys, prod, spec, bins, res, ret_d, ret_s,
                inv, fwd, wave, home, in_sem, tab_sem, s1, r1, s2, r2):
    row, col, ens = lax.axis_index("row"), lax.axis_index("col"), lax.axis_index("ens")
    me = dev_of(row, col)
    dense = jnp.logical_or(row == 0, row == 3)
    sparse = jnp.logical_not(dense)
    my_slot = col * 2 + jnp.where(row >= 2, 1, 0)

    loads = []
    for f in FIELDS:
        for ri in PAIR:
            src = (vre, vim)[ri].at[f] if f < 3 else (sre, sim)[ri].at[0]
            for half, (a, size, b) in enumerate(((0, LOW_ROWS, 0), (2 * LOW_ROWS, KEPT_ROWS - LOW_ROWS, LOW_ROWS))):
                cp = pltpu.make_async_copy(
                    src.at[pl.ds(a, size)], xin.at[ri, pl.ds(KEPT_ROWS * f + b, size)], in_sem.at[f, ri, half])
                cp.start()
                loads.append(cp)
    tab = [pltpu.make_async_copy(src, dst, tab_sem.at[i]) for i, (src, dst) in enumerate(
        ((wave_hbm, wave), (inv_hbm, inv), (fwd_hbm, fwd), (home_hbm, home)))]
    for cp in tab:
        cp.start()

    barrier = pltpu.get_barrier_semaphore()

    def peer(k):
        return row ^ (k % QUAD), col ^ (k // QUAD)

    for k in PEERS:
        pr, pc = peer(k)
        pl.semaphore_signal(barrier, inc=1, device_id=(ens, pc, pr), device_id_type=MESH)
    for ri in PAIR:
        xin[ri, QUAD * KEPT_ROWS:, :] = jnp.zeros((QUAD * FLOWS, FLOWS), F32)
    pl.semaphore_wait(barrier, 7)

    def pack_dense(lo, hi):
        def body(n, carry):
            t, rb = n // QUAD, n % QUAD
            blk = xin[rb // 2, pl.ds(t * K + rb % 2, LANES, stride=2), :]
            send[:, t, rb] = blk.T.reshape(OCT, *TILE)
            return carry
        lax.fori_loop(QUAD * lo, QUAD * hi, body, 0, unroll=QUAD)

    def pack_sparse(lo, hi):
        first = jnp.where(row == 1, 0, N)

        def body(n, carry):
            t, rb = n // QUAD, n % QUAD
            base = t * OCT * FLOWS + first + rb % 2
            parts = [xin[rb // 2, pl.ds(base + (p // 2 + QUAD * (p % 2)) * FLOWS, HALF, stride=2), :] for p in range(OCT)]
            send[:, t, rb] = jnp.concatenate(parts, axis=0).T.reshape(OCT, *TILE)
            return carry
        lax.fori_loop(QUAD * lo, QUAD * hi, body, 0, unroll=QUAD)

    def remote(src, dst, sems, i, j, chunk, r, c):
        return pltpu.make_async_remote_copy(
            src_ref=src, dst_ref=dst, send_sem=sems[0].at[i, chunk], recv_sem=sems[1].at[j, chunk],
            device_id=(ens, c, r), device_id_type=MESH)

    def bounds(kind, chunk):
        edges = D_CHUNKS if kind == "D" else S_CHUNKS
        return edges[chunk], edges[chunk + 1]

    def out_copy(kind, chunk, slot, r, c, frm):
        lo, hi = bounds(kind, chunk)
        to = dev_of(r, c)
        part = pl.ds(lo, hi - lo)
        dst = recv_d if kind == "D" else recv_s
        return remote(send.at[to, part], dst.at[slot, part], (s1, r1), to, frm, chunk, r, c)

    for chunk in FIELDS:
        for cp in loads[QUAD * chunk + (QUAD if chunk else 0):QUAD * chunk + OCT]:
            cp.wait()

        for kind, mine, pack, recv in (("D", dense, pack_dense, recv_d), ("S", sparse, pack_sparse, recv_s)):
            @pl.when(mine)
            def _():
                lo, hi = bounds(kind, chunk)
                pack(lo, hi)
                for k in PEERS:
                    out_copy(kind, chunk, my_slot, *peer(k), me).start()
                recv[my_slot, lo:hi] = send[me, lo:hi]

    lane = lax.broadcasted_iota(jnp.int32, TILE, 1)
    low = lane % QUAD < 2
    p32 = lane % N
    left, even, first_half = lane < FLOWS, lane % FLOWS < N, p32 < HALF

    def everyone():
        for kind, group in (("D", DENSE), ("S", SPARSE)):
            for slot, (r, c) in enumerate(group):
                yield kind, slot, r, c

    def wait_chunk(chunk):
        for kind, slot, r, c in everyone():
            @pl.when(me != dev_of(r, c))
            def _():
                out_copy(kind, chunk, slot, r, c, dev_of(r, c)).wait_recv()

    def swap_blocks(tiles, forward):
        def outer(a, b, c, d):
            return (jnp.where(left, a, roll(c, FLOWS)), jnp.where(left, b, roll(d, FLOWS)),
                    jnp.where(left, roll(a, FLOWS), c), jnp.where(left, roll(b, FLOWS), d))

        def inner(a, b, c, d):
            return (jnp.where(even, a, roll(b, N)), jnp.where(even, roll(a, -N), b),
                    jnp.where(even, c, roll(d, N)), jnp.where(even, roll(c, -N), d))
        return inner(*outer(*tiles)) if forward else outer(*inner(*tiles))

    def merge(lo, hi):
        def body(b, carry):
            cos, sin = wave[b, pl.ds(2, 1)], wave[b, pl.ds(3, 1)]
            for t in range(lo, hi):
                got = []
                for ri in PAIR:
                    rb = 2 * ri + b
                    d = [recv_d[o, t, rb] for o in FIELDS]
                    s = [recv_s[o, t // 2, rb] for o in FIELDS]
                    h = HALF * (t % 2)
                    c1 = jnp.where(low, d[2], roll(d[3], 2))
                    s0 = roll(s[0], -h) if h else s[0]
                    rest = jnp.where(low, roll(s[2], 20 - h), roll(s[3], 14 - h))
                    s1_ = jnp.where(p32 < 12, s0, jnp.where(p32 < 20, roll(s[1], QUAD - h), rest))
                    got.append(swap_blocks((d[0], d[1], c1, s1_), True))
                for s, (re, im) in enumerate(zip(*got)):
                    merged[b, QUAD * t + s] = re * cos + im * sin
                    merged[2 + b, QUAD * t + s] = im * cos - re * sin
            return carry
        lax.fori_loop(0, 2, body, 0)

    def to_x(f, b, get):
        vals = [None] * N
        for i, j in enumerate(SLOTS):
            vals[j] = get(i)
        out = fft(vals, 1)
        for x in range(0, N, 2):
            for ri in PAIR:
                hi, mid, lo = split_bf16(jnp.concatenate([out[x][ri], out[x + 1][ri]], axis=0))
                for p, part in enumerate((lo, hi, mid)):
                    lhs[f, b, ri, OCT * x:OCT * x + HALF, LANES * p:LANES * p + LANES] = part

    def field_x(f, src):
        def body(b, carry):
            to_x(f, b, lambda i: (merged[b, src * KEPT + i], merged[2 + b, src * KEPT + i]))
            return carry
        lax.fori_loop(0, 2, body, 0)

    def curl_x(f):
        c1, c2 = (f + 1) % 3, (f + 2) % 3

        def body(b, carry):
            ky, kz = (jnp.broadcast_to(wave[b, pl.ds(i, 1)], TILE) for i in PAIR)

            def get(i):
                ks = (UNIT * mode(SLOTS[i]), ky, kz)
                m1, m2 = c1 * KEPT + i, c2 * KEPT + i
                im = ks[c1] * merged[b, m2] - ks[c2] * merged[b, m1]
                re = ks[c2] * merged[2 + b, m1] - ks[c1] * merged[2 + b, m2]
                return re, im
            to_x(3 + f, b, get)
            return carry
        lax.fori_loop(0, 2, body, 0)

    def to_grid(f):
        sums = []
        for b in PAIR:
            parts = []
            for ri in PAIR:
                low_hi, hi_mid = lhs[f, b, ri, :, 0:K], lhs[f, b, ri, :, LANES:LANES + K]
                acc = dot(low_hi, inv[b, ri, 0]) + dot(hi_mid, inv[b, ri, 1])
                parts.append(acc + dot(hi_mid, inv[b, ri, 2]))
            sums.append((parts[0] + parts[1], parts[0] - parts[1]))
        for side in PAIR:
            phys[f, 2 * side] = sums[0][side] + sums[1][side]
            phys[f, 2 * side + 1] = sums[0][side] - sums[1][side]

    def to_spec(c):
        for b in PAIR:
            for ri in PAIR:
                hi, mid, lo = (prod[b, ri, p] for p in VEC)
                both = dot(hi, fwd[b, ri, :, 0:K]) + dot(mid, fwd[b, ri, :, 0:K])
                small = dot(lo, fwd[b, ri, :, 0:LANES]) + dot(hi, fwd[b, ri, :, K:])
                spec[c, b, ri] = small + both[:, LANES:] + both[:, :LANES]

    def product(c, point):
        def body(i, carry):
            rows = pl.ds(pl.multiple_of(i * HALF, HALF), HALF)
            n = [point(q, rows) for q in FIELDS]
            for b in PAIR:
                side = [n[0] - n[1], n[2] - n[3]] if b else [n[0] + n[1], n[2] + n[3]]
                for ri in PAIR:
                    v = side[0] - side[1] if ri else side[0] + side[1]
                    for p, part in enumerate(split_bf16(v)):
                        prod[b, ri, p, rows, :] = part
            return carry
        lax.fori_loop(0, HALF, body, 0, unroll=2)
        to_spec(c)

    def cross(c):
        c1, c2 = (c + 1) % 3, (c + 2) % 3
        product(c, lambda q, rows: phys[c1, q, rows, :] * phys[3 + c2, q, rows, :]
                - phys[c2, q, rows, :] * phys[3 + c1, q, rows, :])

    def flux(c):
        product(c, lambda q, rows: phys[c, q, rows, :] * phys[6, q, rows, :])

    def from_x(c):
        def body(b, carry):
            vals = [tuple(spec[c, b, ri, OCT * x:OCT * x + OCT, :] for ri in PAIR) for x in range(N)]
            out = fft(vals, -1)
            for i, j in enumerate(SLOTS):
                for ri in PAIR:
                    bins[c, 2 * ri + b, i] = out[j][ri]
            return carry
        lax.fori_loop(0, 2, body, 0)

    def phase(b, re, im):
        cos, sin = wave[b, pl.ds(2, 1)], wave[b, pl.ds(3, 1)]
        return re * cos - im * sin, re * sin + im * cos

    def project():
        def body(t, carry):
            b, i = t // KEPT, t % KEPT
            e = [home[pl.ds(t * 5 + k, 1)] for k in range(5)]
            n = [[bins[c, 2 * ri + b, i] for c in VEC] for ri in PAIR]
            one = [e[0] * n[ri][0] + e[1] * n[ri][1] for ri in PAIR]
            two = [e[2] * n[ri][0] + e[3] * n[ri][1] + e[QUAD] * n[ri][2] for ri in PAIR]
            for which, v in enumerate((one, two)):
                for ri, part in enumerate(phase(b, *v)):
                    res[2 * ri + b, 2 * i + which] = part
            return carry
        lax.fori_loop(0, 2 * KEPT, body, 0, unroll=6)

    def diverge():
        def body(b, carry):
            for i, j in enumerate(SLOTS):
                ks = (UNIT * mode(j), wave[b, pl.ds(0, 1)], wave[b, pl.ds(1, 1)])
                re, im = phase(b, *[sum(ks[c] * bins[c, 2 * ri + b, i] for c in VEC) for ri in PAIR])
                res[b, 2 * KEPT + i] = im
                res[2 + b, 2 * KEPT + i] = -re
            for ri in PAIR:
                res[2 * ri + b, 3 * KEPT] = jnp.zeros(TILE, F32)
            return carry
        lax.fori_loop(0, 2, body, 0)

    def unmerge(lo, hi):
        p16 = lane % HALF
        zero = jnp.zeros(TILE, F32)

        def body(rb, carry):
            for t in range(lo, hi, 2):
                ends = []
                for h in PAIR:
                    tiles = swap_blocks([res[rb, QUAD * (t + h) + s] for s in FIELDS], False)
                    ret_d[0, t + h, rb], ret_d[1, t + h, rb] = tiles[:2]
                    ret_d[2, t + h, rb] = jnp.where(low, tiles[2], zero)
                    ret_d[3, t + h, rb] = jnp.where(low, roll(tiles[2], -2), zero)
                    ends.append(tiles[3])
                for o, (a, ok) in enumerate(((0, p16 < 12), (-QUAD, p16 >= OCT), (-20, (p16 < 12) & low), (-14, (p16 >= OCT) & low))):
                    v = jnp.where(first_half, roll(ends[0], a) if a else ends[0], roll(ends[1], a + HALF))
                    ret_s[o, t // 2, rb] = jnp.where(ok, v, zero)
            return carry
        lax.fori_loop(0, QUAD, body, 0)

    def ret_copy(kind, chunk, slot, r, c, frm):
        lo, hi = RET_CHUNKS[chunk], RET_CHUNKS[chunk + 1]
        if kind == "S":
            lo, hi = lo // 2, hi // 2
        part = pl.ds(lo, hi - lo)
        src = ret_d if kind == "D" else ret_s
        return remote(src.at[slot, part], back.at[frm, part], (s2, r2), dev_of(r, c), frm, chunk, r, c)

    def send_back(chunk):
        for kind, slot, r, c in everyone():
            d = dev_of(r, c)

            @pl.when(me != d)
            def _():
                ret_copy(kind, chunk, slot, r, c, me).start()

            @pl.when(me == d)
            def _():
                lo, hi = RET_CHUNKS[chunk], RET_CHUNKS[chunk + 1]
                if kind == "D":
                    back[d, lo:hi] = ret_d[slot, lo:hi]
                else:
                    back[d, lo // 2:hi // 2] = ret_s[slot, lo // 2:hi // 2]

    tab[0].wait()
    for f in VEC:
        wait_chunk(f)
        merge(*bounds("D", f))
        field_x(f, f)
    for f in VEC:
        curl_x(f)
    tab[1].wait()
    lax.fori_loop(0, 6, lambda f, carry: (to_grid(f), carry)[1], 0)
    tab[2].wait()
    tab[3].wait()
    for c in VEC:
        cross(c)
        from_x(c)
    project()
    for chunk in PAIR:
        unmerge(RET_CHUNKS[chunk], RET_CHUNKS[chunk + 1])
        send_back(chunk)
    wait_chunk(3)
    merge(*bounds("D", 3))
    field_x(6, 3)
    to_grid(6)
    for c in VEC:
        flux(c)
        from_x(c)
    diverge()
    unmerge(*RET_CHUNKS[2:])
    send_back(2)

    for kind, mine in (("D", dense), ("S", sparse)):
        @pl.when(mine)
        def _():
            for k in PEERS:
                pr, pc = peer(k)
                for chunk in FIELDS:
                    out_copy(kind, chunk, my_slot, pr, pc, me).wait_send()
                for chunk in VEC:
                    ret_copy(kind, chunk, 0, pr, pc, dev_of(pr, pc)).wait_recv()

    for kind, slot, r, c in everyone():
        @pl.when(me != dev_of(r, c))
        def _():
            for chunk in VEC:
                ret_copy(kind, chunk, slot, r, c, me).wait_send()


def out_kernel(back, tab_hbm, ore, oim, tre, tim, buf, tab, sem, tab_sem):
    row, col = lax.axis_index("row"), lax.axis_index("col")
    dense = jnp.logical_or(row == 0, row == 3)
    load = pltpu.make_async_copy(tab_hbm.at[dev_of(row, col)], tab, tab_sem)
    load.start()
    odd = lax.broadcasted_iota(jnp.int32, (1, LANES), 1) % FLOWS >= N
    for f in FIELDS:
        for ri in PAIR:
            buf[f, ri, LOW_ROWS:2 * LOW_ROWS, :] = jnp.zeros((LOW_ROWS, FLOWS), F32)

    @pl.when(jnp.logical_not(dense))
    def _():
        for f in FIELDS:
            for ri in PAIR:
                for a, size in ((0, LOW_ROWS), (2 * LOW_ROWS, ROWS - 2 * LOW_ROWS)):
                    buf[f, ri, pl.ds(a, size), :] = jnp.zeros((size, FLOWS), F32)
    load.wait()

    def place(ri, b, kind, f, i, tile, block):
        first = SLOTS[i] * FLOWS + b
        if kind == "D":
            buf[f, ri, pl.ds(first, N, stride=2), :] = tile[N * block:N * block + N]
        else:
            at = N // 2 * (2 * (block % QUAD) + block // QUAD)
            first = first + jnp.where(row == 1, 0, N)
            buf[f, ri, pl.ds(first, HALF, stride=2), :] = tile[at:at + HALF]

    def rebuild(ri, kind):
        per = QUAD if kind == "D" else OCT
        tiles = D_RET if kind == "D" else S_RET
        mixed = -(-2 * KEPT // per)

        def body(b, carry):
            held = None
            for t in range(tiles):
                v = back[:, t, 2 * ri + b].reshape(FLOWS, LANES)
                if t < mixed:
                    k = [tab[pl.ds((b * S_OUT + t) * 3 + q, 1)] for q in VEC]
                    other = jnp.where(odd, roll(v, N), roll(v, -N))
                    out = (v * k[0] + other * k[1]).T
                    z = v * k[2]
                    if t % 2 == 0:
                        held = z
                    if t % 2 == 1 or t == mixed - 1:
                        last = t % 2 == 1
                        zt = (jnp.where(odd, held, roll(z, -N)) if last else z).T
                        for back_by, shift in ((1, 0), (0, 1)) if last else ((0, 0),):
                            for s in range(1, per, 2):
                                n = per * (t - back_by) + s
                                if n < 2 * KEPT:
                                    place(ri, b, kind, 2, n // 2, zt, s - shift)
                else:
                    out = v.T
                for s in range(per):
                    n = per * t + s
                    if n < 2 * KEPT:
                        place(ri, b, kind, n % 2, n // 2, out, s)
                    elif n < 3 * KEPT:
                        place(ri, b, kind, 3, n - 2 * KEPT, out, s)
            return carry
        lax.fori_loop(0, 2, body, 0)

    copies = []
    for ri in PAIR:
        @pl.when(dense)
        def _():
            rebuild(ri, "D")

        @pl.when(jnp.logical_not(dense))
        def _():
            rebuild(ri, "S")

        for f in FIELDS:
            dst = (ore, oim)[ri].at[f] if f < 3 else (tre, tim)[ri].at[0]
            copies.append(pltpu.make_async_copy(buf.at[f, ri], dst, sem.at[f, ri]))
            copies[-1].start()
    for cp in copies:
        cp.wait()


def solution(mesh):
    spec_vec = P('ens', None, None, 'row', 'col')
    spec_scal = P('ens', None, 'row', 'col')
    consts = tables()
    src_np = source_tables()
    vmem = pl.BlockSpec(memory_space=pltpu.VMEM)
    hbm = pl.BlockSpec(memory_space=pl.ANY)
    dma = pltpu.SemaphoreType.DMA
    links = dma((OCT, QUAD))

    def f32(*lead):
        return pltpu.VMEM((*lead, *TILE), F32)

    def local_term(vel_re, vel_im, scal_re, scal_im):
        vec = [jnp.transpose(a, (1, 2, 3, QUAD, 0)).reshape(3, ROWS, FLOWS) for a in (vel_re, vel_im)]
        scal = [jnp.transpose(a, (1, 2, 3, 0)).reshape(1, ROWS, FLOWS) for a in (scal_re, scal_im)]
        back = pl.pallas_call(
            main_kernel,
            out_shape=jax.ShapeDtypeStruct((OCT, D_RET, QUAD, *TILE), F32),
            in_specs=[hbm] * OCT,
            out_specs=vmem,
            scratch_shapes=[
                pltpu.VMEM((2, QUAD * KEPT_ROWS + QUAD * FLOWS, FLOWS), F32), f32(OCT, D_OUT, QUAD), f32(QUAD, D_OUT, QUAD), f32(QUAD, S_OUT, QUAD),
                f32(QUAD, QUAD * KEPT), pltpu.VMEM((7, 2, 2, K, 3 * LANES), BF16), pltpu.VMEM((7, QUAD, K, K), F32),
                pltpu.VMEM((2, 2, 3, K, K), BF16), pltpu.VMEM((3, 2, 2, K, LANES), F32), f32(3, QUAD, KEPT),
                f32(QUAD, QUAD * D_RET), f32(QUAD, D_RET, QUAD), f32(QUAD, S_RET, QUAD),
                *[pltpu.VMEM(a.shape, a.dtype) for a in consts],
                dma((QUAD, 2, 2)), dma((QUAD,)), links, links, links, links,
            ],
            compiler_params=pltpu.CompilerParams(
                collective_id=0, has_side_effects=True, vmem_limit_bytes=60 * MIB),
            name="flow_home",
        )(*vec, *scal, *[jnp.asarray(a) for a in consts])
        outs = pl.pallas_call(
            out_kernel,
            out_shape=[jax.ShapeDtypeStruct((c, ROWS, FLOWS), F32) for c in (3, 3, 1, 1)],
            in_specs=[vmem, hbm],
            out_specs=[hbm] * QUAD,
            scratch_shapes=[pltpu.VMEM((QUAD, 2, ROWS, FLOWS), F32), pltpu.VMEM(src_np.shape[1:], F32), dma((QUAD, 2)), dma],
            compiler_params=pltpu.CompilerParams(vmem_limit_bytes=40 * MIB),
            name="lay_out",
        )(back, jnp.asarray(src_np))
        out_v = [jnp.transpose(a.reshape(3, N, OCT, OCT, FLOWS), (QUAD, 0, 1, 2, 3)) for a in outs[:2]]
        out_s = [jnp.transpose(a.reshape(N, OCT, OCT, FLOWS), (3, 0, 1, 2)) for a in outs[2:]]
        return (*out_v, *out_s)

    return jax.shard_map(local_term, mesh=mesh, in_specs=(spec_vec, spec_vec, spec_scal, spec_scal),
                         out_specs=(spec_vec, spec_vec, spec_scal, spec_scal), check_vma=False)
```

```python
import math

import jax
import jax.numpy as jnp
import numpy as np
from jax import lax
from jax.experimental import pallas as pl
from jax.experimental.pallas import tpu as pltpu
from jax.sharding import PartitionSpec as P

N = 32
LANES = 128
FLOWS = 64
ROWS = 2048
TILE = (8, LANES)
K = 256
TINY = 1e-9
MIB = 1 << 20
QUAD, OCT, HALF = 4, 8, 16
PAIR, VEC, FIELDS, PEERS = range(2), range(3), range(QUAD), range(1, OCT)
MESH = pl.DeviceIdType.MESH
F32 = jnp.float32
BF16 = jnp.bfloat16
UNIT = 2 * math.pi / N
SLOTS = list(range(11)) + list(range(22, N))
KEPT = len(SLOTS)
KEPT_ROWS = KEPT * FLOWS
LOW_ROWS = 11 * FLOWS
D_OUT, S_OUT, D_RET, S_RET = 21, 11, HALF, OCT
D_CHUNKS, S_CHUNKS = (0, 6, 11, HALF, 21), (0, 3, 6, OCT, 11)
RET_CHUNKS = (0, QUAD, 10, HALF)
DENSE = [(0, 0), (3, 0), (0, 1), (3, 1)]
SPARSE = [(1, 0), (2, 0), (1, 1), (2, 1)]


def mode(j):
    return j if j < N // 2 else j - N


def kept(m):
    return 3 * abs(m) < N


def home_mode(lane, parity):
    block, p = divmod(lane, N)
    y, high, half = p // QUAD, p % QUAD // 2, p % QUAD
    if block < 2:
        row, col = 3 * block, 0
    elif block == 2:
        row, col, half = 3 * high, 1, p % 2
    elif p < 12:
        row, col = 1, 0
    elif p < 20:
        row, col, y = 2, 0, y + 3
    else:
        row, col, half, y = 1 + high, 1, p % 2, y - 5 + 6 * high
    if y > 7:
        return None
    ky, kz = mode(OCT * row + y), OCT * col + 2 * half + parity
    return (ky, kz) if kept(ky) and kept(kz) else None


def source_mode(lane, row, col, parity):
    width = N if row % 3 == 0 else HALF
    block, p = divmod(lane, width)
    slot = block if width == N else block // 2 + QUAD * (block % 2)
    y = p // QUAD + (QUAD if row == 2 else 0)
    ky, kz = mode(OCT * row + y), OCT * col + 2 * (p % QUAD) + parity
    return slot, ((ky, kz) if kept(ky) and kept(kz) else None)


def basis(kx, ky, kz):
    flat, full = math.hypot(kx, ky), math.hypot(kx, ky, kz)
    if full == 0:
        return np.zeros(3), np.zeros(3)
    if flat == 0:
        return np.array([1.0, 0, 0]), np.array([0, 1.0, 0])
    e1 = np.array([ky, -kx, 0]) / flat
    return e1, np.array([kx * kz, ky * kz, -flat * flat]) / (flat * full)


def split3(x):
    x = np.asarray(x, np.float32)
    hi = x.astype(BF16)
    rest = x - hi.astype(np.float32)
    mid = rest.astype(BF16)
    return hi, mid, (rest - mid.astype(np.float32)).astype(BF16)


def tables():
    scale = float(N) ** -1.5
    half = N // 2
    points = [(y, z) for z in range(1, OCT) for y in range(N)] + [(y, z) for z in (0, OCT) for y in range(half)]
    yy, zz = np.array(points).T
    inv = np.zeros((2, 2, LANES, K))
    wave = np.zeros((2, QUAD, LANES), np.float32)
    home = np.zeros((2, KEPT, 5, LANES), np.float32)
    for parity in PAIR:
        for lane in range(LANES):
            got = home_mode(lane, parity)
            if got is None:
                continue
            ky, kz = got
            ang = UNIT * (ky * (yy + 0.5) + kz * zz)
            inv[parity, 0, lane] = scale * np.cos(ang)
            inv[parity, 1, lane] = -scale * np.sin(ang)
            wave[parity, :, lane] = ky * UNIT, kz * UNIT, math.cos(UNIT * ky / 2), math.sin(UNIT * ky / 2)
            for i, j in enumerate(SLOTS):
                e1, e2 = basis(mode(j), ky, kz)
                home[parity, i, :, lane] = *e1[:2], *e2
    fwd = np.swapaxes(inv, 2, 3)
    weight = np.full((2, 1, LANES, 1), 2.0)
    for lane in range(LANES):
        got = home_mode(lane, 0)
        if got is not None and got[1] == 0:
            weight[0, 0, lane] = 1.0
    inv3 = np.stack(split3(inv * weight))
    fwd3 = np.concatenate(split3(fwd), axis=3)
    return inv3, fwd3, wave, home.reshape(-1, LANES)


def source_tables():
    out = np.zeros((OCT, 2, S_OUT, 3, LANES), np.float32)
    for row in FIELDS:
        for col in PAIR:
            per = QUAD if row % 3 == 0 else OCT
            for parity in PAIR:
                for lane in range(LANES):
                    slot, got = source_mode(lane, row, col, parity)
                    for t in range(S_OUT):
                        n = t * per + slot
                        i = n // 2
                        if n >= 2 * KEPT:
                            out[dev_of(row, col), parity, t, 0, lane] = 1.0
                        elif got is not None:
                            e1, e2 = basis(mode(SLOTS[i]), *got)
                            out[dev_of(row, col), parity, t, :, lane] = (e2[1], e1[1], e2[2]) if n % 2 else (e1[0], e2[0], 0)
    return out.reshape(OCT, -1, LANES)


def cmul_const(a, c, s):
    re, im = a
    if abs(s) < TINY:
        return (re, im) if c > 0 else (-re, -im)
    if abs(c) < TINY:
        return (-im, re) if s > 0 else (im, -re)
    if abs(abs(c) - abs(s)) < TINY:
        p, q = (re - im) * abs(c), (re + im) * abs(c)
        if c > 0:
            return (p, q) if s > 0 else (q, -p)
        return (-q, p) if s > 0 else (-p, -q)
    return re * c - im * s, re * s + im * c


def fft(vals, sign):
    n = len(vals)
    if n == 1:
        return list(vals)
    even, odd = fft(vals[0::2], sign), fft(vals[1::2], sign)
    out = [None] * n
    for k in range(n // 2):
        a, b = even[k], odd[k]
        if b is not None:
            ang = sign * 2 * math.pi * k / n
            b = cmul_const(b, math.cos(ang), math.sin(ang))
        if a is None and b is None:
            continue
        if b is None:
            out[k], out[k + n // 2] = a, a
        elif a is None:
            out[k], out[k + n // 2] = b, (-b[0], -b[1])
        else:
            out[k] = (a[0] + b[0], a[1] + b[1])
            out[k + n // 2] = (a[0] - b[0], a[1] - b[1])
    return out


def dot(a, b):
    return jnp.dot(a, b, preferred_element_type=F32)


def split_bf16(x):
    hi = x.astype(BF16)
    rest = x - hi.astype(F32)
    mid = rest.astype(BF16)
    low = (rest - mid.astype(F32)).astype(BF16)
    return hi, mid, low


def dev_of(row, col):
    return col * QUAD + row


def roll(x, shift):
    return pltpu.roll(x, shift % LANES, 1)


def main_kernel(vre, vim, sre, sim, inv_hbm, fwd_hbm, wave_hbm, home_hbm, back,
                xin, send, recv_d, recv_s, merged, lhs, phys, prod, spec, bins, res, ret_d, ret_s,
                inv, fwd, wave, home, in_sem, tab_sem, own_sem, s1, r1, s2, r2):
    row, col, ens = lax.axis_index("row"), lax.axis_index("col"), lax.axis_index("ens")
    me = dev_of(row, col)
    dense = jnp.logical_or(row == 0, row == 3)
    sparse = jnp.logical_not(dense)
    my_slot = col * 2 + jnp.where(row >= 2, 1, 0)

    loads = []
    for f in FIELDS:
        for ri in PAIR:
            src = (vre, vim)[ri].at[f] if f < 3 else (sre, sim)[ri].at[0]
            for half, (a, size, b) in enumerate(((0, LOW_ROWS, 0), (2 * LOW_ROWS, KEPT_ROWS - LOW_ROWS, LOW_ROWS))):
                cp = pltpu.make_async_copy(
                    src.at[pl.ds(a, size)], xin.at[ri, pl.ds(KEPT_ROWS * f + b, size)], in_sem.at[f, ri, half])
                cp.start()
                loads.append(cp)
    wanted = [(wave_hbm, wave), (fwd_hbm, fwd), (home_hbm, home)]
    wanted += [(inv_hbm.at[part], inv.at[:, :, pair, pl.ds(LANES * h, LANES)])
               for pair, parts in enumerate(((0, 2), (1, 1), (0, 0))) for h, part in enumerate(parts)]
    tab = [pltpu.make_async_copy(src, dst, tab_sem.at[i]) for i, (src, dst) in enumerate(wanted)]
    for cp in tab:
        cp.start()

    barrier = pltpu.get_barrier_semaphore()

    def peer(k):
        return row ^ (k % QUAD), col ^ (k // QUAD)

    for k in PEERS:
        pr, pc = peer(k)
        pl.semaphore_signal(barrier, inc=1, device_id=(ens, pc, pr), device_id_type=MESH)
    for ri in PAIR:
        xin[ri, QUAD * KEPT_ROWS:, :] = jnp.zeros((QUAD * FLOWS, FLOWS), F32)
    pl.semaphore_wait(barrier, 7)

    def pack_dense(lo, hi):
        def body(n, carry):
            t, rb = n // QUAD, n % QUAD
            blk = xin[rb // 2, pl.ds(t * K + rb % 2, LANES, stride=2), :]
            send[:, t, rb] = blk.T.reshape(OCT, *TILE)
            return carry
        lax.fori_loop(QUAD * lo, QUAD * hi, body, 0, unroll=QUAD)

    def pack_sparse(lo, hi):
        first = jnp.where(row == 1, 0, N)

        def body(n, carry):
            t, rb = n // QUAD, n % QUAD
            base = t * OCT * FLOWS + first + rb % 2
            parts = [xin[rb // 2, pl.ds(base + (p // 2 + QUAD * (p % 2)) * FLOWS, HALF, stride=2), :] for p in range(OCT)]
            send[:, t, rb] = jnp.concatenate(parts, axis=0).T.reshape(OCT, *TILE)
            return carry
        lax.fori_loop(QUAD * lo, QUAD * hi, body, 0, unroll=QUAD)

    def remote(src, dst, sems, i, j, chunk, r, c):
        return pltpu.make_async_remote_copy(
            src_ref=src, dst_ref=dst, send_sem=sems[0].at[i, chunk], recv_sem=sems[1].at[j, chunk],
            device_id=(ens, c, r), device_id_type=MESH)

    def bounds(kind, chunk):
        edges = D_CHUNKS if kind == "D" else S_CHUNKS
        return edges[chunk], edges[chunk + 1]

    def out_copy(kind, chunk, slot, r, c, frm):
        lo, hi = bounds(kind, chunk)
        to = dev_of(r, c)
        part = pl.ds(lo, hi - lo)
        dst = recv_d if kind == "D" else recv_s
        return remote(send.at[to, part], dst.at[slot, part], (s1, r1), to, frm, chunk, r, c)

    for chunk in FIELDS:
        for cp in loads[QUAD * chunk + (QUAD if chunk else 0):QUAD * chunk + OCT]:
            cp.wait()

        for kind, mine, pack, recv in (("D", dense, pack_dense, recv_d), ("S", sparse, pack_sparse, recv_s)):
            @pl.when(mine)
            def _():
                lo, hi = bounds(kind, chunk)
                pack(lo, hi)
                for k in PEERS:
                    out_copy(kind, chunk, my_slot, *peer(k), me).start()
                recv[my_slot, lo:hi] = send[me, lo:hi]

    lane = lax.broadcasted_iota(jnp.int32, TILE, 1)
    low = lane % QUAD < 2
    p32 = lane % N
    left, even, first_half = lane < FLOWS, lane % FLOWS < N, p32 < HALF

    def everyone():
        for kind, group in (("D", DENSE), ("S", SPARSE)):
            for slot, (r, c) in enumerate(group):
                yield kind, slot, r, c

    def wait_chunk(chunk):
        for kind, slot, r, c in everyone():
            @pl.when(me != dev_of(r, c))
            def _():
                out_copy(kind, chunk, slot, r, c, dev_of(r, c)).wait_recv()

    def swap_blocks(tiles, forward):
        def outer(a, b, c, d):
            return (jnp.where(left, a, roll(c, FLOWS)), jnp.where(left, b, roll(d, FLOWS)),
                    jnp.where(left, roll(a, FLOWS), c), jnp.where(left, roll(b, FLOWS), d))

        def inner(a, b, c, d):
            return (jnp.where(even, a, roll(b, N)), jnp.where(even, roll(a, -N), b),
                    jnp.where(even, c, roll(d, N)), jnp.where(even, roll(c, -N), d))
        return inner(*outer(*tiles)) if forward else outer(*inner(*tiles))

    def merge(lo, hi):
        def body(b, carry):
            cos, sin = wave[b, pl.ds(2, 1)], wave[b, pl.ds(3, 1)]
            for t in range(lo, hi):
                got = []
                for ri in PAIR:
                    rb = 2 * ri + b
                    d = [recv_d[o, t, rb] for o in FIELDS]
                    s = [recv_s[o, t // 2, rb] for o in FIELDS]
                    h = HALF * (t % 2)
                    c1 = jnp.where(low, d[2], roll(d[3], 2))
                    s0 = roll(s[0], -h) if h else s[0]
                    rest = jnp.where(low, roll(s[2], 20 - h), roll(s[3], 14 - h))
                    s1_ = jnp.where(p32 < 12, s0, jnp.where(p32 < 20, roll(s[1], QUAD - h), rest))
                    got.append(swap_blocks((d[0], d[1], c1, s1_), True))
                for s, (re, im) in enumerate(zip(*got)):
                    merged[b, QUAD * t + s] = re * cos + im * sin
                    merged[2 + b, QUAD * t + s] = im * cos - re * sin
            return carry
        lax.fori_loop(0, 2, body, 0)

    def to_x(f, b, get):
        vals = [None] * N
        for i, j in enumerate(SLOTS):
            vals[j] = get(i)
        out = fft(vals, 1)
        for x in range(0, N, 2):
            for ri in PAIR:
                hi, mid, lo = split_bf16(jnp.concatenate([out[x][ri], out[x + 1][ri]], axis=0))
                for p, part in enumerate((lo, hi, mid)):
                    lhs[f, b, ri, OCT * x:OCT * x + HALF, LANES * p:LANES * p + LANES] = part

    def field_x(f, src):
        def body(b, carry):
            to_x(f, b, lambda i: (merged[b, src * KEPT + i], merged[2 + b, src * KEPT + i]))
            return carry
        lax.fori_loop(0, 2, body, 0)

    def curl_x(f):
        c1, c2 = (f + 1) % 3, (f + 2) % 3

        def body(b, carry):
            ky, kz = (jnp.broadcast_to(wave[b, pl.ds(i, 1)], TILE) for i in PAIR)

            def get(i):
                ks = (UNIT * mode(SLOTS[i]), ky, kz)
                m1, m2 = c1 * KEPT + i, c2 * KEPT + i
                im = ks[c1] * merged[b, m2] - ks[c2] * merged[b, m1]
                re = ks[c2] * merged[2 + b, m1] - ks[c1] * merged[2 + b, m2]
                return re, im
            to_x(3 + f, b, get)
            return carry
        lax.fori_loop(0, 2, body, 0)

    def to_grid(f):
        sums = []
        for b in PAIR:
            parts = []
            for ri in PAIR:
                low_hi, hi_mid = lhs[f, b, ri, :, 0:K], lhs[f, b, ri, :, LANES:LANES + K]
                acc = dot(low_hi, inv[b, ri, 0]) + dot(hi_mid, inv[b, ri, 1])
                parts.append(acc + dot(hi_mid, inv[b, ri, 2]))
            sums.append((parts[0] + parts[1], parts[0] - parts[1]))
        for side in PAIR:
            phys[f, 2 * side] = sums[0][side] + sums[1][side]
            phys[f, 2 * side + 1] = sums[0][side] - sums[1][side]

    def to_spec(c):
        for b in PAIR:
            for ri in PAIR:
                hi, mid, lo = (prod[c, b, ri, p] for p in VEC)
                both = dot(hi, fwd[b, ri, :, 0:K]) + dot(mid, fwd[b, ri, :, 0:K])
                small = dot(lo, fwd[b, ri, :, 0:LANES]) + dot(hi, fwd[b, ri, :, K:])
                spec[c, b, ri] = small + both[:, LANES:] + both[:, :LANES]

    def product(c, point):
        def body(i, carry):
            rows = pl.ds(pl.multiple_of(i * HALF, HALF), HALF)
            n = [point(q, rows) for q in FIELDS]
            for b in PAIR:
                side = [n[0] - n[1], n[2] - n[3]] if b else [n[0] + n[1], n[2] + n[3]]
                for ri in PAIR:
                    v = side[0] - side[1] if ri else side[0] + side[1]
                    for p, part in enumerate(split_bf16(v)):
                        prod[c, b, ri, p, rows, :] = part
            return carry
        lax.fori_loop(0, HALF, body, 0, unroll=2)

    def cross(c):
        c1, c2 = (c + 1) % 3, (c + 2) % 3
        product(c, lambda q, rows: phys[c1, q, rows, :] * phys[3 + c2, q, rows, :]
                - phys[c2, q, rows, :] * phys[3 + c1, q, rows, :])

    def flux(c):
        product(c, lambda q, rows: phys[c, q, rows, :] * phys[6, q, rows, :])

    def from_x(c):
        def body(b, carry):
            vals = [tuple(spec[c, b, ri, OCT * x:OCT * x + OCT, :] for ri in PAIR) for x in range(N)]
            out = fft(vals, -1)
            for i, j in enumerate(SLOTS):
                for ri in PAIR:
                    bins[c, 2 * ri + b, i] = out[j][ri]
            return carry
        lax.fori_loop(0, 2, body, 0)

    def phase(b, re, im):
        cos, sin = wave[b, pl.ds(2, 1)], wave[b, pl.ds(3, 1)]
        return re * cos - im * sin, re * sin + im * cos

    def project():
        def body(t, carry):
            b, i = t // KEPT, t % KEPT
            e = [home[pl.ds(t * 5 + k, 1)] for k in range(5)]
            n = [[bins[c, 2 * ri + b, i] for c in VEC] for ri in PAIR]
            one = [e[0] * n[ri][0] + e[1] * n[ri][1] for ri in PAIR]
            two = [e[2] * n[ri][0] + e[3] * n[ri][1] + e[QUAD] * n[ri][2] for ri in PAIR]
            for which, v in enumerate((one, two)):
                for ri, part in enumerate(phase(b, *v)):
                    res[2 * ri + b, 2 * i + which] = part
            return carry
        lax.fori_loop(0, 2 * KEPT, body, 0, unroll=6)

    def diverge():
        def body(b, carry):
            for i, j in enumerate(SLOTS):
                ks = (UNIT * mode(j), wave[b, pl.ds(0, 1)], wave[b, pl.ds(1, 1)])
                re, im = phase(b, *[sum(ks[c] * bins[c, 2 * ri + b, i] for c in VEC) for ri in PAIR])
                res[b, 2 * KEPT + i] = im
                res[2 + b, 2 * KEPT + i] = -re
            for ri in PAIR:
                res[2 * ri + b, 3 * KEPT] = jnp.zeros(TILE, F32)
            return carry
        lax.fori_loop(0, 2, body, 0)

    def unmerge(lo, hi):
        p16 = lane % HALF
        zero = jnp.zeros(TILE, F32)

        def body(rb, carry):
            for t in range(lo, hi, 2):
                ends = []
                for h in PAIR:
                    tiles = swap_blocks([res[rb, QUAD * (t + h) + s] for s in FIELDS], False)
                    ret_d[0, t + h, rb], ret_d[1, t + h, rb] = tiles[:2]
                    ret_d[2, t + h, rb] = jnp.where(low, tiles[2], zero)
                    ret_d[3, t + h, rb] = jnp.where(low, roll(tiles[2], -2), zero)
                    ends.append(tiles[3])
                for o, (a, ok) in enumerate(((0, p16 < 12), (-QUAD, p16 >= OCT), (-20, (p16 < 12) & low), (-14, (p16 >= OCT) & low))):
                    v = jnp.where(first_half, roll(ends[0], a) if a else ends[0], roll(ends[1], a + HALF))
                    ret_s[o, t // 2, rb] = jnp.where(ok, v, zero)
            return carry
        lax.fori_loop(0, QUAD, body, 0)

    def ret_part(kind, chunk):
        lo, hi = RET_CHUNKS[chunk], RET_CHUNKS[chunk + 1]
        if kind == "S":
            lo, hi = lo // 2, hi // 2
        return ret_d if kind == "D" else ret_s, pl.ds(lo, hi - lo)

    def ret_copy(kind, chunk, slot, r, c, frm):
        src, part = ret_part(kind, chunk)
        return remote(src.at[slot, part], back.at[frm, part], (s2, r2), dev_of(r, c), frm, chunk, r, c)

    def own_copy(kind, chunk, slot, d):
        src, part = ret_part(kind, chunk)
        return pltpu.make_async_copy(src.at[slot, part], back.at[d, part], own_sem.at[chunk])

    def send_back(chunk):
        for kind, slot, r, c in everyone():
            d = dev_of(r, c)

            @pl.when(me != d)
            def _():
                ret_copy(kind, chunk, slot, r, c, me).start()

            @pl.when(me == d)
            def _():
                own_copy(kind, chunk, slot, d).start()

    tab[0].wait()
    for f in VEC:
        wait_chunk(f)
        merge(*bounds("D", f))
        field_x(f, f)
        if f == 0:
            for cp in tab[3:]:
                cp.wait()
            to_grid(0)
        elif f == 1:
            curl_x(2)
            to_grid(1)
            to_grid(5)
    curl_x(0)
    curl_x(1)
    for f in VEC:
        to_grid(2 + f)
    tab[1].wait()
    tab[2].wait()
    for c in VEC:
        cross(c)
    for c in VEC:
        to_spec(c)
        from_x(c)
    project()
    for chunk in PAIR:
        unmerge(RET_CHUNKS[chunk], RET_CHUNKS[chunk + 1])
        send_back(chunk)
    wait_chunk(3)
    merge(*bounds("D", 3))
    field_x(6, 3)
    to_grid(6)
    for c in VEC:
        flux(c)
    for c in VEC:
        to_spec(c)
        from_x(c)
    diverge()
    unmerge(*RET_CHUNKS[2:])
    send_back(2)

    for kind, mine in (("D", dense), ("S", sparse)):
        @pl.when(mine)
        def _():
            for k in PEERS:
                pr, pc = peer(k)
                for chunk in FIELDS:
                    out_copy(kind, chunk, my_slot, pr, pc, me).wait_send()
                for chunk in VEC:
                    ret_copy(kind, chunk, 0, pr, pc, dev_of(pr, pc)).wait_recv()

    for kind, slot, r, c in everyone():
        d = dev_of(r, c)

        @pl.when(me != d)
        def _():
            for chunk in VEC:
                ret_copy(kind, chunk, slot, r, c, me).wait_send()

        @pl.when(me == d)
        def _():
            for chunk in VEC:
                own_copy(kind, chunk, slot, d).wait()


def out_kernel(back_hbm, tab_hbm, ore, oim, tre, tim, buf, tab, back, blank, sem, in_sem, tab_sem):
    row, col = lax.axis_index("row"), lax.axis_index("col")
    dense = jnp.logical_or(row == 0, row == 3)
    loads = [pltpu.make_async_copy(back_hbm.at[:, :, pl.ds(2 * ri, 2)], back.at[:, :, pl.ds(2 * ri, 2)], in_sem.at[ri])
             for ri in PAIR]
    load = pltpu.make_async_copy(tab_hbm.at[dev_of(row, col)], tab, tab_sem)
    for cp in (*loads, load):
        cp.start()
    odd = lax.broadcasted_iota(jnp.int32, (1, LANES), 1) % FLOWS >= N

    def store(f, ri, which):
        first = (0, LOW_ROWS, 2 * LOW_ROWS)[which]
        part = pl.ds(first, LOW_ROWS if which < 2 else ROWS - first)
        dst = (ore, oim)[ri].at[f] if f < 3 else (tre, tim)[ri].at[0]
        src = blank if which == 1 else buf.at[f, ri, part]
        return pltpu.make_async_copy(src, dst.at[part], sem.at[f, ri, which])

    blank[...] = jnp.zeros_like(blank)
    for f in FIELDS:
        for ri in PAIR:
            store(f, ri, 1).start()

    @pl.when(jnp.logical_not(dense))
    def _():
        for f in FIELDS:
            for ri in PAIR:
                for first, size in ((0, LOW_ROWS), (2 * LOW_ROWS, ROWS - 2 * LOW_ROWS)):
                    buf[f, ri, pl.ds(first, size), :] = jnp.zeros((size, FLOWS), F32)
    load.wait()

    def place(ri, b, kind, f, i, tile, block):
        first = SLOTS[i] * FLOWS + b
        if kind == "D":
            buf[f, ri, pl.ds(first, N, stride=2), :] = tile[N * block:N * block + N]
        else:
            at = N // 2 * (2 * (block % QUAD) + block // QUAD)
            first = first + jnp.where(row == 1, 0, N)
            buf[f, ri, pl.ds(first, HALF, stride=2), :] = tile[at:at + HALF]

    def rebuild(ri, kind):
        per = QUAD if kind == "D" else OCT
        tiles = D_RET if kind == "D" else S_RET
        mixed = -(-2 * KEPT // per)

        held = [None, None]
        ends = (5, 10, 13, 15) if kind == "D" else (3, 5, 6, 7)
        for t in range(tiles):
            for b in PAIR:
                v = back[:, t, 2 * ri + b].reshape(FLOWS, LANES)
                if t < mixed:
                    k = [tab[pl.ds((b * S_OUT + t) * 3 + q, 1)] for q in VEC]
                    other = jnp.where(odd, roll(v, N), roll(v, -N))
                    out = (v * k[0] + other * k[1]).T
                    z = v * k[2]
                    last = t % 2 == 1
                    if last or t == mixed - 1:
                        zt = (jnp.where(odd, held[b], roll(z, -N)) if last else z).T
                        for back_by, shift in ((1, 0), (0, 1)) if last else ((0, 0),):
                            for s in range(1, per, 2):
                                n = per * (t - back_by) + s
                                if n < 2 * KEPT:
                                    place(ri, b, kind, 2, n // 2, zt, s - shift)
                    held[b] = z
                else:
                    out = v.T
                for s in range(per):
                    n = per * t + s
                    if n < 2 * KEPT:
                        place(ri, b, kind, n % 2, n // 2, out, s)
                    elif n < 3 * KEPT:
                        place(ri, b, kind, 3, n - 2 * KEPT, out, s)
            if t in ends:
                e = ends.index(t)
                for f in VEC if e < 2 else (3,):
                    store(f, ri, 2 * (e % 2)).start()

    for ri in PAIR:
        loads[ri].wait()

        @pl.when(dense)
        def _():
            rebuild(ri, "D")

        @pl.when(jnp.logical_not(dense))
        def _():
            rebuild(ri, "S")
    for f in FIELDS:
        for ri in PAIR:
            for which in VEC:
                store(f, ri, which).wait()


def solution(mesh):
    spec_vec = P('ens', None, None, 'row', 'col')
    spec_scal = P('ens', None, 'row', 'col')
    consts = tables()
    src_np = source_tables()
    hbm = pl.BlockSpec(memory_space=pl.ANY)
    dma = pltpu.SemaphoreType.DMA
    links = dma((OCT, QUAD))

    def f32(*lead):
        return pltpu.VMEM((*lead, *TILE), F32)

    def local_term(vel_re, vel_im, scal_re, scal_im):
        vec = [jnp.transpose(a, (1, 2, 3, QUAD, 0)).reshape(3, ROWS, FLOWS) for a in (vel_re, vel_im)]
        scal = [jnp.transpose(a, (1, 2, 3, 0)).reshape(1, ROWS, FLOWS) for a in (scal_re, scal_im)]
        back = pl.pallas_call(
            main_kernel,
            out_shape=jax.ShapeDtypeStruct((OCT, D_RET, QUAD, *TILE), F32),
            in_specs=[hbm] * OCT,
            out_specs=hbm,
            scratch_shapes=[
                pltpu.VMEM((2, QUAD * KEPT_ROWS + QUAD * FLOWS, FLOWS), F32), f32(OCT, D_OUT, QUAD), f32(QUAD, D_OUT, QUAD), f32(QUAD, S_OUT, QUAD),
                f32(QUAD, QUAD * KEPT), pltpu.VMEM((7, 2, 2, K, 3 * LANES), BF16), pltpu.VMEM((7, QUAD, K, K), F32),
                pltpu.VMEM((3, 2, 2, 3, K, K), BF16), pltpu.VMEM((3, 2, 2, K, LANES), F32), f32(3, QUAD, KEPT),
                f32(QUAD, QUAD * D_RET), f32(QUAD, D_RET, QUAD), f32(QUAD, S_RET, QUAD),
                pltpu.VMEM((2, 2, 3, K, K), BF16), *[pltpu.VMEM(a.shape, a.dtype) for a in consts[1:]],
                dma((QUAD, 2, 2)), dma((9,)), dma((3,)), links, links, links, links,
            ],
            compiler_params=pltpu.CompilerParams(
                collective_id=0, has_side_effects=True, vmem_limit_bytes=60 * MIB),
            name="flow_home",
        )(*vec, *scal, *[jnp.asarray(a) for a in consts])
        outs = pl.pallas_call(
            out_kernel,
            out_shape=[jax.ShapeDtypeStruct((c, ROWS, FLOWS), F32) for c in (3, 3, 1, 1)],
            in_specs=[hbm, hbm],
            out_specs=[hbm] * QUAD,
            scratch_shapes=[pltpu.VMEM((QUAD, 2, ROWS, FLOWS), F32), pltpu.VMEM(src_np.shape[1:], F32),
                            f32(OCT, D_RET, QUAD), pltpu.VMEM((LOW_ROWS, FLOWS), F32), dma((QUAD, 2, 3)), dma((2,)), dma],
            compiler_params=pltpu.CompilerParams(vmem_limit_bytes=60 * MIB),
            name="lay_out",
        )(back, jnp.asarray(src_np))
        out_v = [jnp.transpose(a.reshape(3, N, OCT, OCT, FLOWS), (QUAD, 0, 1, 2, 3)) for a in outs[:2]]
        out_s = [jnp.transpose(a.reshape(N, OCT, OCT, FLOWS), (3, 0, 1, 2)) for a in outs[2:]]
        return (*out_v, *out_s)

    return jax.shard_map(local_term, mesh=mesh, in_specs=(spec_vec, spec_vec, spec_scal, spec_scal),
                         out_specs=(spec_vec, spec_vec, spec_scal, spec_scal), check_vma=False)
```

```python
import math

import jax
import jax.numpy as jnp
import numpy as np
from jax import lax
from jax.experimental import pallas as pl
from jax.experimental.pallas import tpu as pltpu
from jax.sharding import PartitionSpec as P

N = 32
LANES = 128
FLOWS = 64
ROWS = 2048
TILE = (8, LANES)
K = 256
TINY = 1e-9
MIB = 1 << 20
QUAD, OCT, HALF = 4, 8, 16
PARTS = RE, IM = slice(0, 2), slice(2, 4)
PAIR, VEC, FIELDS, PEERS = range(2), range(3), range(QUAD), range(1, OCT)
MESH = pl.DeviceIdType.MESH
F32 = jnp.float32
BF16 = jnp.bfloat16
UNIT = 2 * math.pi / N
SLOTS = list(range(11)) + list(range(22, N))
KEPT = len(SLOTS)
KEPT_ROWS = KEPT * FLOWS
LOW_ROWS = 11 * FLOWS
D_OUT, S_OUT, D_RET, S_RET = 21, 11, HALF, OCT
D_CHUNKS, S_CHUNKS = (0, 6, 11, HALF, 21), (0, 3, 6, OCT, 11)
RET_CHUNKS = (0, QUAD, 10, HALF)
DENSE, SPARSE = ([(r, c) for c in PAIR for r in rows] for rows in ((0, 3), (1, 2)))


def mode(j):
    return j if j < N // 2 else j - N


def kept(m):
    return 3 * abs(m) < N


def home_mode(lane, parity):
    block, p = divmod(lane, N)
    y, high, half = p // QUAD, p % QUAD // 2, p % QUAD
    if block < 2:
        row, col = 3 * block, 0
    elif block == 2:
        row, col, half = 3 * high, 1, p % 2
    elif p < 12:
        row, col = 1, 0
    elif p < 20:
        row, col, y = 2, 0, y + 3
    else:
        row, col, half, y = 1 + high, 1, p % 2, y - 5 + 6 * high
    if y > 7:
        return None
    ky, kz = mode(OCT * row + y), OCT * col + 2 * half + parity
    return (ky, kz) if kept(ky) and kept(kz) else None


def source_mode(lane, row, col, parity):
    width = N if row % 3 == 0 else HALF
    block, p = divmod(lane, width)
    slot = block if width == N else block // 2 + QUAD * (block % 2)
    y = p // QUAD + (QUAD if row == 2 else 0)
    ky, kz = mode(OCT * row + y), OCT * col + 2 * (p % QUAD) + parity
    return slot, ((ky, kz) if kept(ky) and kept(kz) else None)


def basis(kx, ky, kz):
    flat, full = math.hypot(kx, ky), math.hypot(kx, ky, kz)
    if full == 0:
        return np.zeros(3), np.zeros(3)
    if flat == 0:
        return np.array([1.0, 0, 0]), np.array([0, 1.0, 0])
    e1 = np.array([ky, -kx, 0]) / flat
    return e1, np.array([kx * kz, ky * kz, -flat * flat]) / (flat * full)


def split3(x):
    x = np.asarray(x, np.float32)
    hi = x.astype(BF16)
    rest = x - hi.astype(np.float32)
    mid = rest.astype(BF16)
    return hi, mid, (rest - mid.astype(np.float32)).astype(BF16)


def tables():
    scale = float(N) ** -1.5
    half = N // 2
    points = [(y, z) for z in range(1, OCT) for y in range(N)] + [(y, z) for z in (0, OCT) for y in range(half)]
    yy, zz = np.array(points).T
    inv = np.zeros((2, 2, LANES, K))
    wave = np.zeros((2, QUAD, LANES), np.float32)
    home = np.zeros((2, 5, KEPT, 1, LANES), np.float32)
    for parity in PAIR:
        for lane in range(LANES):
            got = home_mode(lane, parity)
            if got is None:
                continue
            ky, kz = got
            ang = UNIT * (ky * (yy + 0.5) + kz * zz)
            inv[parity, 0, lane] = scale * np.cos(ang)
            inv[parity, 1, lane] = -scale * np.sin(ang)
            wave[parity, :, lane] = ky * UNIT, kz * UNIT, math.cos(UNIT * ky / 2), math.sin(UNIT * ky / 2)
            for i, j in enumerate(SLOTS):
                e1, e2 = basis(mode(j), ky, kz)
                home[parity, :, i, 0, lane] = *e1[:2], *e2
    fwd = np.swapaxes(inv, 2, 3)
    weight = np.full((2, 1, LANES, 1), 2.0)
    for lane in range(LANES):
        got = home_mode(lane, 0)
        if got is not None and got[1] == 0:
            weight[0, 0, lane] = 1.0
    inv3 = np.stack(split3(inv * weight))
    fwd3 = np.concatenate(split3(fwd), axis=3)
    return inv3, fwd3, wave, home


def source_tables():
    out = np.zeros((OCT, 2, S_OUT, 3, LANES), np.float32)
    for row in FIELDS:
        for col in PAIR:
            per = QUAD if row % 3 == 0 else OCT
            for parity in PAIR:
                for lane in range(LANES):
                    slot, got = source_mode(lane, row, col, parity)
                    for t in range(S_OUT):
                        n = t * per + slot
                        i = n // 2
                        if n >= 2 * KEPT:
                            out[dev_of(row, col), parity, t, 0, lane] = 1.0
                        elif got is not None:
                            e1, e2 = basis(mode(SLOTS[i]), *got)
                            out[dev_of(row, col), parity, t, :, lane] = (e2[1], e1[1], e2[2]) if n % 2 else (e1[0], e2[0], 0)
    return out.reshape(OCT, -1, LANES)


def cmul_const(a, c, s):
    re, im = a
    if abs(s) < TINY:
        return (re, im) if c > 0 else (-re, -im)
    if abs(c) < TINY:
        return (-im, re) if s > 0 else (im, -re)
    if abs(abs(c) - abs(s)) < TINY:
        p, q = (re - im) * abs(c), (re + im) * abs(c)
        if c > 0:
            return (p, q) if s > 0 else (q, -p)
        return (-q, p) if s > 0 else (-p, -q)
    return re * c - im * s, re * s + im * c


def fft(vals, sign):
    n = len(vals)
    if n == 1:
        return list(vals)
    even, odd = fft(vals[0::2], sign), fft(vals[1::2], sign)
    out = [None] * n
    for k in range(n // 2):
        a, b = even[k], odd[k]
        if b is not None:
            ang = sign * 2 * math.pi * k / n
            b = cmul_const(b, math.cos(ang), math.sin(ang))
        if a is None and b is None:
            continue
        if b is None:
            out[k], out[k + n // 2] = a, a
        elif a is None:
            out[k], out[k + n // 2] = b, (-b[0], -b[1])
        else:
            out[k] = (a[0] + b[0], a[1] + b[1])
            out[k + n // 2] = (a[0] - b[0], a[1] - b[1])
    return out


def dot(a, b):
    return jnp.dot(a, b, preferred_element_type=F32)


def split_bf16(x):
    hi = x.astype(BF16)
    rest = x - hi.astype(F32)
    mid = rest.astype(BF16)
    low = (rest - mid.astype(F32)).astype(BF16)
    return hi, mid, low


def dev_of(row, col):
    return col * QUAD + row


def unrolled(n):
    def run(body):
        lax.fori_loop(0, n, lambda i, carry: (body(i), carry)[1], 0, unroll=True)
    return run


def roll(x, shift):
    return pltpu.roll(x, shift % LANES, x.ndim - 1)


def main_kernel(vre, vim, sre, sim, inv_hbm, fwd_hbm, wave_hbm, home_hbm, back,
                xin, send, recv_d, recv_s, merged, lhs, phys, prod, spec, bins, res, ret_d, ret_s,
                inv, fwd, wave, home, in_sem, tab_sem, own_sem, s1, r1, s2, r2):
    row, col, ens = lax.axis_index("row"), lax.axis_index("col"), lax.axis_index("ens")
    me = dev_of(row, col)
    dense = jnp.logical_or(row == 0, row == 3)
    sparse = jnp.logical_not(dense)
    my_slot = col * 2 + jnp.where(row >= 2, 1, 0)

    loads = []
    for f in FIELDS:
        for ri in PAIR:
            src = (vre, vim)[ri].at[f] if f < 3 else (sre, sim)[ri].at[0]
            for half, (a, size, b) in enumerate(((0, LOW_ROWS, 0), (2 * LOW_ROWS, KEPT_ROWS - LOW_ROWS, LOW_ROWS))):
                cp = pltpu.make_async_copy(
                    src.at[pl.ds(a, size)], xin.at[ri, pl.ds(KEPT_ROWS * f + b, size)], in_sem.at[f, ri, half])
                cp.start()
                loads.append(cp)
    wanted = [(wave_hbm, wave), (fwd_hbm, fwd), (home_hbm, home)]
    wanted += [(inv_hbm.at[part], inv.at[:, :, pair, pl.ds(LANES * h, LANES)])
               for pair, parts in enumerate(((0, 2), (1, 1), (0, 0))) for h, part in enumerate(parts)]
    tab = [pltpu.make_async_copy(src, dst, tab_sem.at[i]) for i, (src, dst) in enumerate(wanted)]
    for cp in tab:
        cp.start()

    barrier = pltpu.get_barrier_semaphore()

    def peer(k):
        return row ^ (k % QUAD), col ^ (k // QUAD)

    for k in PEERS:
        pr, pc = peer(k)
        pl.semaphore_signal(barrier, inc=1, device_id=(ens, pc, pr), device_id_type=MESH)
    for ri in PAIR:
        xin[ri, QUAD * KEPT_ROWS:, :] = jnp.zeros((QUAD * FLOWS, FLOWS), F32)
    pl.semaphore_wait(barrier, 7)

    def pack_dense(lo, hi):
        def body(n, carry):
            t, rb = lax.div(n, QUAD), lax.rem(n, QUAD)
            blk = xin[lax.div(rb, 2), pl.ds(t * K + lax.rem(rb, 2), LANES, stride=2), :]
            send[:, t, rb] = blk.T.reshape(OCT, *TILE)
            return carry
        lax.fori_loop(QUAD * lo, QUAD * hi, body, 0, unroll=QUAD)

    def pack_sparse(lo, hi):
        first = jnp.where(row == 1, 0, N)

        def body(n, carry):
            t, rb = lax.div(n, QUAD), lax.rem(n, QUAD)
            base, ri = t * OCT * FLOWS + first + lax.rem(rb, 2), lax.div(rb, 2)
            parts = [xin[ri, pl.ds(base + (p // 2 + QUAD * (p % 2)) * FLOWS, HALF, stride=2), :] for p in range(OCT)]
            send[:, t, rb] = jnp.concatenate(parts, axis=0).T.reshape(OCT, *TILE)
            return carry
        lax.fori_loop(QUAD * lo, QUAD * hi, body, 0, unroll=QUAD)

    def remote(src, dst, sems, i, j, chunk, r, c):
        return pltpu.make_async_remote_copy(
            src_ref=src, dst_ref=dst, send_sem=sems[0].at[i, chunk], recv_sem=sems[1].at[j, chunk],
            device_id=(ens, c, r), device_id_type=MESH)

    def bounds(kind, chunk):
        edges = D_CHUNKS if kind == "D" else S_CHUNKS
        return edges[chunk], edges[chunk + 1]

    def out_copy(kind, chunk, slot, r, c, frm):
        lo, hi = bounds(kind, chunk)
        to = dev_of(r, c)
        part = pl.ds(lo, hi - lo)
        dst = recv_d if kind == "D" else recv_s
        return remote(send.at[to, part], dst.at[slot, part], (s1, r1), to, frm, chunk, r, c)

    for chunk in FIELDS:
        for cp in loads[QUAD * chunk + (QUAD if chunk else 0):QUAD * chunk + OCT]:
            cp.wait()

        for kind, mine, pack, recv in (("D", dense, pack_dense, recv_d), ("S", sparse, pack_sparse, recv_s)):
            @pl.when(mine)
            def _():
                lo, hi = bounds(kind, chunk)
                pack(lo, hi)
                for k in PEERS:
                    out_copy(kind, chunk, my_slot, *peer(k), me).start()
                recv[my_slot, lo:hi] = send[me, lo:hi]

    lane = lax.broadcasted_iota(jnp.int32, TILE, 1)
    low = lane % QUAD < 2
    p32 = lane % N
    left, even, first_half = lane < FLOWS, lane % FLOWS < N, p32 < HALF

    def everyone():
        for kind, group in (("D", DENSE), ("S", SPARSE)):
            for slot, (r, c) in enumerate(group):
                yield kind, slot, r, c

    def wait_chunk(chunk):
        for kind, slot, r, c in everyone():
            @pl.when(me != dev_of(r, c))
            def _():
                out_copy(kind, chunk, slot, r, c, dev_of(r, c)).wait_recv()

    def swap_blocks(tiles, forward):
        def outer(a, b, c, d):
            ca, db = roll(jnp.where(left, c, a), FLOWS), roll(jnp.where(left, d, b), FLOWS)
            return jnp.where(left, a, ca), jnp.where(left, b, db), jnp.where(left, ca, c), jnp.where(left, db, d)

        def inner(a, b, c, d):
            return (jnp.where(even, a, roll(b, N)), jnp.where(even, roll(a, -N), b),
                    jnp.where(even, c, roll(d, N)), jnp.where(even, roll(c, -N), d))
        return inner(*outer(*tiles)) if forward else outer(*inner(*tiles))

    def merge(lo, hi):
        cos, sin = wave[:, pl.ds(2, 1)], wave[:, pl.ds(3, 1)]
        for t in range(lo, hi):
            got = []
            for part in PARTS:
                d = [recv_d[o, t, part] for o in FIELDS]
                s = [recv_s[o, t // 2, part] for o in FIELDS]
                h = HALF * (t % 2)
                c1 = jnp.where(low, d[2], roll(d[3], 2))
                s0 = roll(s[0], -h) if h else s[0]
                rest = jnp.where(low, roll(s[2], 20 - h), roll(s[3], 14 - h))
                s1_ = jnp.where(p32 < 12, s0, jnp.where(p32 < 20, roll(s[1], QUAD - h), rest))
                got.append(swap_blocks((d[0], d[1], c1, s1_), True))
            for s, (re, im) in enumerate(zip(*got)):
                merged[RE, QUAD * t + s] = re * cos + im * sin
                merged[IM, QUAD * t + s] = im * cos - re * sin

    def to_x(f, get):
        vals = [None] * N
        for i, j in enumerate(SLOTS):
            vals[j] = get(i)
        out = fft(vals, 1)
        for x in range(0, N, 2):
            for ri in PAIR:
                hi, mid, lo = split_bf16(jnp.concatenate([out[x][ri], out[x + 1][ri]], axis=1))
                for p, part in enumerate((lo, hi, mid)):
                    lhs[:, ri, f, OCT * x:OCT * x + HALF, LANES * p:LANES * p + LANES] = part

    def field_x(f, src):
        to_x(f, lambda i: (merged[RE, src * KEPT + i], merged[IM, src * KEPT + i]))

    def curl_x(f):
        c1, c2 = (f + 1) % 3, (f + 2) % 3
        ky, kz = wave[:, pl.ds(0, 1)], wave[:, pl.ds(1, 1)]

        def get(i):
            ks = (UNIT * mode(SLOTS[i]), ky, kz)
            m1, m2 = c1 * KEPT + i, c2 * KEPT + i
            im = ks[c1] * merged[RE, m2] - ks[c2] * merged[RE, m1]
            re = ks[c2] * merged[IM, m1] - ks[c1] * merged[IM, m2]
            return re, im
        to_x(3 + f, get)

    def to_grid(f):
        sums = []
        for b in PAIR:
            parts = []
            for ri in PAIR:
                low_hi, hi_mid = lhs[b, ri, f, :, 0:K], lhs[b, ri, f, :, LANES:LANES + K]
                acc = dot(low_hi, inv[b, ri, 0]) + dot(hi_mid, inv[b, ri, 1])
                parts.append(acc + dot(hi_mid, inv[b, ri, 2]))
            sums.append((parts[0] + parts[1], parts[0] - parts[1]))
        for side in PAIR:
            phys[2 * side, f] = sums[0][side] + sums[1][side]
            phys[2 * side + 1, f] = sums[0][side] - sums[1][side]

    def to_spec(c):
        for b in PAIR:
            for ri in PAIR:
                hi, mid, lo = (prod[b, ri, p, c] for p in VEC)
                both = dot(hi, fwd[b, ri, :, 0:K]) + dot(mid, fwd[b, ri, :, 0:K])
                small = dot(lo, fwd[b, ri, :, 0:LANES]) + dot(hi, fwd[b, ri, :, K:])
                spec[b, ri, c] = small + both[:, LANES:] + both[:, :LANES]

    def product(c, point):
        for at in range(0, K, FLOWS):
            rows = slice(at, at + FLOWS)
            n = [point(lambda f: phys[q, f, rows]) for q in FIELDS]
            for b in PAIR:
                side = [n[0] - n[1], n[2] - n[3]] if b else [n[0] + n[1], n[2] + n[3]]
                for ri in PAIR:
                    v = side[0] - side[1] if ri else side[0] + side[1]
                    for p, part in enumerate(split_bf16(v)):
                        prod[b, ri, p, c, rows] = part

    def cross(c):
        c1, c2 = lax.rem(c + 1, 3), lax.rem(c + 2, 3)
        product(c, lambda at: at(c1) * at(3 + c2) - at(c2) * at(3 + c1))

    def flux(c):
        product(c, lambda at: at(c) * at(6))

    def from_x(c):
        vals = [tuple(spec[:, ri, c, OCT * x:OCT * x + OCT] for ri in PAIR) for x in range(N)]
        out = fft(vals, -1)
        for i, j in enumerate(SLOTS):
            bins[c, RE, i], bins[c, IM, i] = out[j]

    def phase(re, im):
        cos, sin = wave[:, pl.ds(2, 1)], wave[:, pl.ds(3, 1)]
        if re.ndim > 3:
            cos, sin = cos[:, None], sin[:, None]
        return re * cos - im * sin, re * sin + im * cos

    def project():
        for lo in range(0, KEPT, 7):
            i = slice(lo, lo + 7)
            e = [home[:, k, i] for k in range(5)]
            n = [[bins[c, part, i] for c in VEC] for part in PARTS]
            one = [e[0] * v[0] + e[1] * v[1] for v in n]
            two = [e[2] * v[0] + e[3] * v[1] + e[QUAD] * v[2] for v in n]
            for which, v in enumerate((one, two)):
                for part, w in zip(PARTS, phase(*v)):
                    res[part, which, i] = w

    def diverge():
        for i, j in enumerate(SLOTS):
            ks = (UNIT * mode(j), wave[:, pl.ds(0, 1)], wave[:, pl.ds(1, 1)])
            re, im = phase(*[sum(ks[c] * bins[c, part, i] for c in VEC) for part in PARTS])
            res[RE, 2, i] = im
            res[IM, 2, i] = -re
        res[:, 2, KEPT] = jnp.zeros((QUAD, *TILE), F32)

    def result(n):
        return res[:, n % 2, n // 2] if n < 2 * KEPT else res[:, 2, n - 2 * KEPT]

    def unmerge(lo, hi):
        p16 = lane % HALF
        zero = jnp.zeros(TILE, F32)

        for t in range(lo, hi, 2):
            ends = []
            for h in PAIR:
                tiles = swap_blocks([result(QUAD * (t + h) + s) for s in FIELDS], False)
                ret_d[0, t + h], ret_d[1, t + h] = tiles[:2]
                ret_d[2, t + h] = jnp.where(low, tiles[2], zero)
                ret_d[3, t + h] = jnp.where(low, roll(tiles[2], -2), zero)
                ends.append(tiles[3])
            for o, (a, ok) in enumerate(((0, p16 < 12), (-4, p16 >= 8), (-20, (p16 < 12) & low), (-14, (p16 >= 8) & low))):
                v = jnp.where(first_half, roll(ends[0], a) if a else ends[0], roll(ends[1], a + HALF))
                ret_s[o, t // 2] = jnp.where(ok, v, zero)

    def ret_part(kind, chunk):
        lo, hi = RET_CHUNKS[chunk], RET_CHUNKS[chunk + 1]
        if kind == "S":
            lo, hi = lo // 2, hi // 2
        return ret_d if kind == "D" else ret_s, pl.ds(lo, hi - lo)

    def ret_copy(kind, chunk, slot, r, c, frm):
        src, part = ret_part(kind, chunk)
        return remote(src.at[slot, part], back.at[frm, part], (s2, r2), dev_of(r, c), frm, chunk, r, c)

    def own_copy(kind, chunk, slot, d):
        src, part = ret_part(kind, chunk)
        return pltpu.make_async_copy(src.at[slot, part], back.at[d, part], own_sem.at[chunk])

    def send_back(chunk):
        for kind, slot, r, c in everyone():
            d = dev_of(r, c)

            @pl.when(me != d)
            def _():
                ret_copy(kind, chunk, slot, r, c, me).start()

            @pl.when(me == d)
            def _():
                own_copy(kind, chunk, slot, d).start()

    tab[0].wait()
    for f in VEC:
        wait_chunk(f)
        merge(*bounds("D", f))
        field_x(f, f)
        if f == 0:
            for cp in tab[3:]:
                cp.wait()
            to_grid(0)
        elif f == 1:
            curl_x(2)
            to_grid(1)
            to_grid(5)
    tab[1].wait()
    tab[2].wait()
    to_grid(2)
    curl_x(0)
    to_grid(3)
    curl_x(1)
    to_grid(QUAD)

    @unrolled(3)
    def _(c):
        cross(c)
        to_spec(c)
        from_x(c)

    project()
    for chunk in PAIR:
        unmerge(RET_CHUNKS[chunk], RET_CHUNKS[chunk + 1])
        send_back(chunk)
    wait_chunk(3)
    merge(*bounds("D", 3))
    field_x(6, 3)
    to_grid(6)
    def flux_part(c, carry):
        flux(c)
        to_spec(c)
        from_x(c)
        return carry
    lax.fori_loop(0, 3, flux_part, 0)

    diverge()
    unmerge(*RET_CHUNKS[2:])
    send_back(2)

    for kind, mine in (("D", dense), ("S", sparse)):
        @pl.when(mine)
        def _():
            for k in PEERS:
                pr, pc = peer(k)
                for chunk in FIELDS:
                    out_copy(kind, chunk, my_slot, pr, pc, me).wait_send()
                for chunk in VEC:
                    ret_copy(kind, chunk, 0, pr, pc, dev_of(pr, pc)).wait_recv()

    for kind, slot, r, c in everyone():
        d = dev_of(r, c)

        @pl.when(me != d)
        def _():
            for chunk in VEC:
                ret_copy(kind, chunk, slot, r, c, me).wait_send()

        @pl.when(me == d)
        def _():
            for chunk in VEC:
                own_copy(kind, chunk, slot, d).wait()


def out_kernel(back_hbm, tab_hbm, ore, oim, tre, tim, buf, tab, back, blank, sem, in_sem, tab_sem):
    row, col = lax.axis_index("row"), lax.axis_index("col")
    dense = jnp.logical_or(row == 0, row == 3)
    loads = [pltpu.make_async_copy(back_hbm.at[:, :, pl.ds(2 * ri, 2)], back.at[:, :, pl.ds(2 * ri, 2)], in_sem.at[ri])
             for ri in PAIR]
    load = pltpu.make_async_copy(tab_hbm.at[dev_of(row, col)], tab, tab_sem)
    for cp in (*loads, load):
        cp.start()
    odd = lax.broadcasted_iota(jnp.int32, (1, LANES), 1) % FLOWS >= N

    def store(f, ri, which):
        first = (0, LOW_ROWS, 2 * LOW_ROWS)[which]
        part = pl.ds(first, LOW_ROWS if which < 2 else ROWS - first)
        dst = (ore, oim)[ri].at[f] if f < 3 else (tre, tim)[ri].at[0]
        src = blank if which == 1 else buf.at[f, ri, part]
        return pltpu.make_async_copy(src, dst.at[part], sem.at[f, ri, which])

    blank[...] = jnp.zeros_like(blank)
    for f in FIELDS:
        for ri in PAIR:
            store(f, ri, 1).start()

    @pl.when(jnp.logical_not(dense))
    def _():
        for f in FIELDS:
            for ri in PAIR:
                for first, size in ((0, LOW_ROWS), (2 * LOW_ROWS, ROWS - 2 * LOW_ROWS)):
                    buf[f, ri, pl.ds(first, size), :] = jnp.zeros((size, FLOWS), F32)
    load.wait()

    def place(ri, b, kind, f, i, tile, block):
        first = SLOTS[i] * FLOWS + b
        if kind == "D":
            buf[f, ri, pl.ds(first, N, stride=2), :] = tile[N * block:N * block + N]
        else:
            at = N // 2 * (2 * (block % QUAD) + block // QUAD)
            first = first + jnp.where(row == 1, 0, N)
            buf[f, ri, pl.ds(first, HALF, stride=2), :] = tile[at:at + HALF]

    def rebuild(ri, kind):
        per = QUAD if kind == "D" else OCT
        tiles = D_RET if kind == "D" else S_RET
        mixed = -(-2 * KEPT // per)

        held = [None, None]
        ends = (5, 10, 13, 15) if kind == "D" else (3, 5, 6, 7)
        for t in range(tiles):
            for b in PAIR:
                v = back[:, t, 2 * ri + b].reshape(FLOWS, LANES)
                if t < mixed:
                    k = [tab[pl.ds((b * S_OUT + t) * 3 + q, 1)] for q in VEC]
                    other = jnp.where(odd, roll(v, N), roll(v, -N))
                    out = (v * k[0] + other * k[1]).T
                    z = v * k[2]
                    last = t % 2 == 1
                    if last or t == mixed - 1:
                        zt = (jnp.where(odd, held[b], roll(z, -N)) if last else z).T
                        for back_by, shift in ((1, 0), (0, 1)) if last else ((0, 0),):
                            for s in range(1, per, 2):
                                n = per * (t - back_by) + s
                                if n < 2 * KEPT:
                                    place(ri, b, kind, 2, n // 2, zt, s - shift)
                    held[b] = z
                else:
                    out = v.T
                for s in range(per):
                    n = per * t + s
                    if n < 2 * KEPT:
                        place(ri, b, kind, n % 2, n // 2, out, s)
                    elif n < 3 * KEPT:
                        place(ri, b, kind, 3, n - 2 * KEPT, out, s)
            if t in ends:
                e = ends.index(t)
                for f in VEC if e < 2 else (3,):
                    store(f, ri, 2 * (e % 2)).start()

    for ri in PAIR:
        loads[ri].wait()

        @pl.when(dense)
        def _():
            rebuild(ri, "D")

        @pl.when(jnp.logical_not(dense))
        def _():
            rebuild(ri, "S")
    for f in FIELDS:
        for ri in PAIR:
            for which in VEC:
                store(f, ri, which).wait()


def solution(mesh):
    spec_vec = P('ens', None, None, 'row', 'col')
    spec_scal = P('ens', None, 'row', 'col')
    consts = tables()
    src_np = source_tables()
    hbm = pl.BlockSpec(memory_space=pl.ANY)
    dma = pltpu.SemaphoreType.DMA
    links = dma((OCT, QUAD))

    def f32(*lead):
        return pltpu.VMEM((*lead, *TILE), F32)

    def local_term(vel_re, vel_im, scal_re, scal_im):
        vec = [jnp.transpose(a, (1, 2, 3, QUAD, 0)).reshape(3, ROWS, FLOWS) for a in (vel_re, vel_im)]
        scal = [jnp.transpose(a, (1, 2, 3, 0)).reshape(1, ROWS, FLOWS) for a in (scal_re, scal_im)]
        back = pl.pallas_call(
            main_kernel,
            out_shape=jax.ShapeDtypeStruct((OCT, D_RET, QUAD, *TILE), F32),
            in_specs=[hbm] * OCT,
            out_specs=hbm,
            scratch_shapes=[
                pltpu.VMEM((2, QUAD * KEPT_ROWS + QUAD * FLOWS, FLOWS), F32), f32(OCT, D_OUT, QUAD), f32(QUAD, D_OUT, QUAD), f32(QUAD, S_OUT, QUAD),
                f32(QUAD, QUAD * KEPT), pltpu.VMEM((2, 2, 7, K, 3 * LANES), BF16), pltpu.VMEM((QUAD, 7, K, K), F32),
                pltpu.VMEM((2, 2, 3, 3, K, K), BF16), pltpu.VMEM((2, 2, 3, K, LANES), F32), f32(3, QUAD, KEPT),
                f32(QUAD, 3, KEPT + 1), f32(QUAD, D_RET, QUAD), f32(QUAD, S_RET, QUAD),
                pltpu.VMEM((2, 2, 3, K, K), BF16), *[pltpu.VMEM(a.shape, a.dtype) for a in consts[1:]],
                dma((QUAD, 2, 2)), dma((9,)), dma((3,)), links, links, links, links,
            ],
            compiler_params=pltpu.CompilerParams(
                collective_id=0, has_side_effects=True, vmem_limit_bytes=60 * MIB),
            name="flow_home",
        )(*vec, *scal, *[jnp.asarray(a) for a in consts])
        outs = pl.pallas_call(
            out_kernel,
            out_shape=[jax.ShapeDtypeStruct((c, ROWS, FLOWS), F32) for c in (3, 3, 1, 1)],
            in_specs=[hbm, hbm],
            out_specs=[hbm] * QUAD,
            scratch_shapes=[pltpu.VMEM((QUAD, 2, ROWS, FLOWS), F32), pltpu.VMEM(src_np.shape[1:], F32),
                            f32(OCT, D_RET, QUAD), pltpu.VMEM((LOW_ROWS, FLOWS), F32), dma((QUAD, 2, 3)), dma((2,)), dma],
            compiler_params=pltpu.CompilerParams(vmem_limit_bytes=60 * MIB),
            name="lay_out",
        )(back, jnp.asarray(src_np))
        out_v = [jnp.transpose(a.reshape(3, N, OCT, OCT, FLOWS), (QUAD, 0, 1, 2, 3)) for a in outs[:2]]
        out_s = [jnp.transpose(a.reshape(N, OCT, OCT, FLOWS), (3, 0, 1, 2)) for a in outs[2:]]
        return (*out_v, *out_s)

    return jax.shard_map(local_term, mesh=mesh, in_specs=(spec_vec, spec_vec, spec_scal, spec_scal),
                         out_specs=(spec_vec, spec_vec, spec_scal, spec_scal), check_vma=False)
```

```python
import math

import jax
import jax.numpy as jnp
import numpy as np
from jax import lax
from jax.experimental import pallas as pl
from jax.experimental.pallas import tpu as pltpu
from jax.sharding import PartitionSpec as P

N = 32
LANES = 128
FLOWS = 64
ROWS = 2048
TILE = (8, LANES)
K = 256
TINY = 1e-9
MIB = 1 << 20
THREE, QUAD, SEVEN, OCT, HALF = 3, 4, 7, 8, 16
PARTS = RE, IM = slice(0, 2), slice(2, QUAD)
PAIR, VEC, FIELDS, PEERS = range(2), range(THREE), range(QUAD), range(1, OCT)
MESH = pl.DeviceIdType.MESH
F32 = jnp.float32
BF16 = jnp.bfloat16
UNIT = 2 * math.pi / N
SLOTS = list(range(11)) + list(range(22, N))
KEPT = len(SLOTS)
KEPT_ROWS = KEPT * FLOWS
LOW_ROWS = 11 * FLOWS
KINDS = {"D": (0, THREE), "A": (1,), "B": (2,)}
OUT = {"D": (N,) * 21, "A": (OCT, OCT, QUAD, OCT, QUAD, OCT, OCT, QUAD), "B": (OCT,) * 6}
RET = {"D": (N,) * HALF, "A": (OCT, OCT, QUAD, OCT, OCT, QUAD), "B": (OCT,) * QUAD}
OUT_EDGES = {"D": (0, 6, 11, HALF, 21), "A": (0, THREE, 5, 6, OCT), "B": (0, 2, THREE, QUAD, 6)}
RET_EDGES = {"D": (0, QUAD, 10, HALF), "A": (0, 1, THREE, 6), "B": (0, 1, 2, QUAD)}
SOURCES = [(kind, k * len(rows) + i, r, k) for kind, rows in KINDS.items() for k in PAIR for i, r in enumerate(rows)]


def units(kind, table, t):
    widths = table[kind]
    w = widths[t]
    per, nth = N // w, widths[:t].count(w)
    first = 48 if kind == "B" else HALF * (w == QUAD)
    out = []
    for s in FIELDS:
        for g in range(per):
            slot, start = QUAD * (per * nth + g) + s, first
            if slot >= QUAD * KEPT:
                slot, start = QUAD * (KEPT - 1) + s, first if kind == "B" else OCT * min(g - 5, 1)
            out.append((slot, N * s + w * g, w, start))
    return out


def place_of(kind, table, w, nth):
    return [t for t, v in enumerate(table[kind]) if v == w][nth]


def mode(j):
    return j if j < N // 2 else j - N


def kept(m):
    return THREE * abs(m) < N


def home_mode(lane, parity):
    block, p = divmod(lane, N)
    y, high, half = p // QUAD, p % QUAD // 2, p % QUAD
    if block < 2:
        row, col = THREE * block, 0
    elif block == 2:
        row, col, half = THREE * high, 1, p % 2
    elif p < 12:
        row, col = 1, 0
    elif p < 20:
        row, col, y = 2, 0, y + THREE
    else:
        row, col, half, y = 1 + high, 1, p % 2, y - 5 + 6 * high
    if y > SEVEN:
        return None
    ky, kz = mode(OCT * row + y), OCT * col + 2 * half + parity
    return (ky, kz) if kept(ky) and kept(kz) else None


def basis(kx, ky, kz):
    flat, full = math.hypot(kx, ky), math.hypot(kx, ky, kz)
    if full == 0:
        return np.zeros(THREE), np.zeros(THREE)
    if flat == 0:
        return np.array([1.0, 0, 0]), np.array([0, 1.0, 0])
    e1 = np.array([ky, -kx, 0]) / flat
    return e1, np.array([kx * kz, ky * kz, -flat * flat]) / (flat * full)


def split3(x):
    x = np.asarray(x, np.float32)
    hi = x.astype(BF16)
    rest = x - hi.astype(np.float32)
    mid = rest.astype(BF16)
    return hi, mid, (rest - mid.astype(np.float32)).astype(BF16)


def tables():
    scale = float(N) ** -1.5
    half = N // 2
    points = [(y, z) for z in range(1, OCT) for y in range(N)] + [(y, z) for z in (0, OCT) for y in range(half)]
    yy, zz = np.array(points).T
    inv = np.zeros((2, 2, LANES, K))
    wave = np.zeros((2, QUAD, LANES), np.float32)
    home = np.zeros((2, 5, KEPT, 1, LANES), np.float32)
    for parity in PAIR:
        for lane in range(LANES):
            got = home_mode(lane, parity)
            if got is None:
                continue
            ky, kz = got
            ang = UNIT * (ky * (yy + 0.5) + kz * zz)
            inv[parity, 0, lane] = scale * np.cos(ang)
            inv[parity, 1, lane] = -scale * np.sin(ang)
            wave[parity, :, lane] = ky * UNIT, kz * UNIT, math.cos(UNIT * ky / 2), math.sin(UNIT * ky / 2)
            for i, j in enumerate(SLOTS):
                e1, e2 = basis(mode(j), ky, kz)
                home[parity, :, i, 0, lane] = *e1[:2], *e2
    fwd = np.swapaxes(inv, 2, THREE)
    weight = np.full((2, 1, LANES, 1), 2.0)
    for lane in range(LANES):
        got = home_mode(lane, 0)
        if got is not None and got[1] == 0:
            weight[0, 0, lane] = 1.0
    inv3 = np.stack(split3(inv * weight))
    fwd3 = np.concatenate(split3(fwd), axis=THREE)
    return inv3, fwd3, wave, home


def source_tables():
    out = np.zeros((OCT, 2, HALF, THREE, LANES), np.float32)
    for kind, _, row, col in SOURCES:
        for t in range(len(RET[kind])):
            for n, lane, w, start in units(kind, RET, t):
                for o in range(w):
                    y, half = divmod(start // 2 + o, QUAD)
                    for parity in PAIR:
                        ky, kz = mode(OCT * row + y), OCT * col + 2 * half + parity
                        to = out[dev_of(row, col), parity, t, :, lane + o]
                        if n >= 2 * KEPT:
                            to[0] = 1
                        elif kept(ky) and kept(kz):
                            e1, e2 = basis(mode(SLOTS[n // 2]), ky, kz)
                            to[:] = (e2[1], e1[1], e2[2]) if n % 2 else (e1[0], e2[0], 0)
    return out.reshape(OCT, -1, LANES)


def cmul_const(a, c, s):
    re, im = a
    if abs(s) < TINY:
        return (re, im) if c > 0 else (-re, -im)
    if abs(c) < TINY:
        return (-im, re) if s > 0 else (im, -re)
    if abs(abs(c) - abs(s)) < TINY:
        p, q = (re - im) * abs(c), (re + im) * abs(c)
        if c > 0:
            return (p, q) if s > 0 else (q, -p)
        return (-q, p) if s > 0 else (-p, -q)
    return re * c - im * s, re * s + im * c


def fft(vals, sign):
    n = len(vals)
    if n == 1:
        return list(vals)
    even, odd = fft(vals[0::2], sign), fft(vals[1::2], sign)
    out = [None] * n
    for k in range(n // 2):
        a, b = even[k], odd[k]
        if b is not None:
            ang = sign * 2 * math.pi * k / n
            b = cmul_const(b, math.cos(ang), math.sin(ang))
        if a is None and b is None:
            continue
        if b is None:
            out[k], out[k + n // 2] = a, a
        elif a is None:
            out[k], out[k + n // 2] = b, (-b[0], -b[1])
        else:
            out[k] = (a[0] + b[0], a[1] + b[1])
            out[k + n // 2] = (a[0] - b[0], a[1] - b[1])
    return out


def dot(a, b):
    return jnp.dot(a, b, preferred_element_type=F32)


def split_bf16(x):
    hi = x.astype(BF16)
    rest = x - hi.astype(F32)
    mid = rest.astype(BF16)
    low = (rest - mid.astype(F32)).astype(BF16)
    return hi, mid, low


def dev_of(row, col):
    return col * QUAD + row


def kinds_here(row):
    tests = {"D": jnp.logical_or(row == 0, row == THREE), "A": row == 1, "B": row == 2}
    return list(tests.items())


def unrolled(n):
    def run(body):
        lax.fori_loop(0, n, lambda i, carry: (body(i), carry)[1], 0, unroll=True)
    return run


def roll(x, shift):
    shift %= LANES
    return pltpu.roll(x, shift, x.ndim - 1) if shift else x


def main_kernel(vre, vim, sre, sim, inv_hbm, fwd_hbm, wave_hbm, home_hbm, back,
                xin, send, recv_d, recv_a, recv_b, merged, lhs, phys, prod, spec, bins, res, ends, ret_d, ret_a, ret_b, stage,
                inv, fwd, wave, home, in_sem, tab_sem, own_sem, s1, r1, s2, r2):
    row, col, ens = lax.axis_index("row"), lax.axis_index("col"), lax.axis_index("ens")
    me = dev_of(row, col)
    recv = {"D": recv_d, "A": recv_a, "B": recv_b}
    ret = {"D": ret_d, "A": ret_a, "B": ret_b}
    mine = kinds_here(row)
    my_slot = {"D": col * 2 + jnp.where(row == THREE, 1, 0), "A": col, "B": col}

    loads = []
    for f in FIELDS:
        for ri in PAIR:
            src = (vre, vim)[ri].at[f] if f < THREE else (sre, sim)[ri].at[0]
            for half, (a, size, b) in enumerate(((0, LOW_ROWS, 0), (2 * LOW_ROWS, KEPT_ROWS - LOW_ROWS, LOW_ROWS))):
                cp = pltpu.make_async_copy(
                    src.at[pl.ds(a, size)], xin.at[ri, pl.ds(KEPT_ROWS * f + b, size)], in_sem.at[f, ri, half])
                cp.start()
                loads.append(cp)
    wanted = [(wave_hbm, wave), (fwd_hbm, fwd), (home_hbm, home)]
    wanted += [(inv_hbm.at[part], inv.at[:, :, pair, pl.ds(LANES * h, LANES)])
               for pair, parts in enumerate(((0, 2), (1, 1), (0, 0))) for h, part in enumerate(parts)]
    tab = [pltpu.make_async_copy(src, dst, tab_sem.at[i]) for i, (src, dst) in enumerate(wanted)]
    for cp in tab:
        cp.start()

    barrier = pltpu.get_barrier_semaphore()

    def peer(k):
        return row ^ (k % QUAD), col ^ (k // QUAD)

    for k in PEERS:
        pr, pc = peer(k)
        pl.semaphore_signal(barrier, inc=1, device_id=(ens, pc, pr), device_id_type=MESH)
    pl.semaphore_wait(barrier, SEVEN)

    def pack(kind, lo, hi):
        if kind == "D":
            def body(n, carry):
                t, rb = lax.div(n, QUAD), lax.rem(n, QUAD)
                blk = xin[lax.div(rb, 2), pl.ds(t * K + lax.rem(rb, 2), LANES, stride=2), :]
                send[:, t, rb] = blk.T.reshape(OCT, *TILE)
                return carry
            lax.fori_loop(QUAD * lo, QUAD * hi, body, 0, unroll=QUAD)
            return

        def few(rb, carry):
            ri, b = lax.div(rb, 2), lax.rem(rb, 2)
            for t in range(lo, hi):
                parts = [xin[ri, pl.ds(slot * FLOWS + start + b, w, stride=2), :] for slot, _, w, start in units(kind, OUT, t)]
                if OUT[kind][t] < OCT:
                    for (_, lane, w, _), part in zip(units(kind, OUT, t), parts):
                        stage[lane:lane + w, :] = part
                    blk = stage[...]
                else:
                    order = np.argsort([u[1] for u in units(kind, OUT, t)])
                    blk = jnp.concatenate([parts[i] for i in order], axis=0)
                send[:, t, rb] = blk.T.reshape(OCT, *TILE)
            return carry
        lax.fori_loop(0, QUAD, few, 0)

    def remote(src, dst, sems, i, j, chunk, r, c):
        return pltpu.make_async_remote_copy(
            src_ref=src, dst_ref=dst, send_sem=sems[0].at[i, chunk], recv_sem=sems[1].at[j, chunk],
            device_id=(ens, c, r), device_id_type=MESH)

    def out_copy(kind, chunk, slot, r, c, frm):
        lo, hi = OUT_EDGES[kind][chunk:chunk + 2]
        to = dev_of(r, c)
        part = pl.ds(lo, hi - lo)
        return remote(send.at[to, part], recv[kind].at[slot, part], (s1, r1), to, frm, chunk, r, c)

    for chunk in FIELDS:
        for cp in loads[OCT * chunk:OCT * chunk + OCT]:
            cp.wait()

        for kind, here in mine:
            @pl.when(here)
            def _():
                lo, hi = OUT_EDGES[kind][chunk:chunk + 2]
                pack(kind, lo, hi)
                for k in PEERS:
                    out_copy(kind, chunk, my_slot[kind], *peer(k), me).start()
                recv[kind][my_slot[kind], lo:hi] = send[me, lo:hi]

    lane = lax.broadcasted_iota(jnp.int32, TILE, 1)
    low = lane % QUAD < 2
    p32 = lane % N
    left, even = lane < FLOWS, lane % FLOWS < N

    def wait_chunk(chunk):
        for kind, slot, r, c in SOURCES:
            @pl.when(me != dev_of(r, c))
            def _():
                out_copy(kind, chunk, slot, r, c, dev_of(r, c)).wait_recv()

    def swap_blocks(tiles, forward):
        def outer(a, b, c, d):
            ca, db = roll(jnp.where(left, c, a), FLOWS), roll(jnp.where(left, d, b), FLOWS)
            return jnp.where(left, a, ca), jnp.where(left, b, db), jnp.where(left, ca, c), jnp.where(left, db, d)

        def inner(a, b, c, d):
            return (jnp.where(even, a, roll(b, N)), jnp.where(even, roll(a, -N), b),
                    jnp.where(even, c, roll(d, N)), jnp.where(even, roll(c, -N), d))
        return inner(*outer(*tiles)) if forward else outer(*inner(*tiles))

    def merge(lo, hi):
        cos, sin = wave[:, pl.ds(2, 1)], wave[:, pl.ds(THREE, 1)]
        for t in range(lo, hi):
            got = []
            for part in PARTS:
                d = [recv_d[o, t, part] for o in FIELDS]
                g, g4 = OCT * (t % QUAD), QUAD * (t % OCT)
                a4 = place_of("A", OUT, QUAD, t // OCT)
                a8, at = (a4, 20) if t == KEPT - 1 else (place_of("A", OUT, OCT, t // QUAD), g)
                c1 = jnp.where(low, d[2], roll(d[THREE], 2))
                v = [(roll(recv_a[c, a8, part], 20 * c - at), roll(recv_a[c, a4, part], 20 * c + OCT - g4),
                      roll(recv_b[c, t // QUAD, part], 10 * c + 12 - g)) for c in PAIR]
                rest = jnp.where(low, jnp.where(p32 < 28, v[1][0], v[1][1]), v[1][2])
                s1_ = jnp.where(p32 < OCT, v[0][0], jnp.where(p32 < 12, v[0][1], jnp.where(p32 < 20, v[0][2], rest)))
                got.append(swap_blocks((d[0], d[1], c1, s1_), True))
            for s, (re, im) in enumerate(zip(*got)):
                merged[RE, QUAD * t + s] = re * cos + im * sin
                merged[IM, QUAD * t + s] = im * cos - re * sin

    def to_x(f, get):
        vals = [None] * N
        for i, j in enumerate(SLOTS):
            vals[j] = get(i)
        out = fft(vals, 1)
        for x in range(0, N, 2):
            for ri in PAIR:
                hi, mid, lo = split_bf16(jnp.concatenate([out[x][ri], out[x + 1][ri]], axis=1))
                for p, part in enumerate((lo, hi, mid)):
                    lhs[:, ri, f, OCT * x:OCT * x + HALF, LANES * p:LANES * p + LANES] = part

    def field_x(f, src):
        to_x(f, lambda i: (merged[RE, src * KEPT + i], merged[IM, src * KEPT + i]))

    def curl_x(f):
        c1, c2 = (f + 1) % THREE, (f + 2) % THREE
        ky, kz = wave[:, pl.ds(0, 1)], wave[:, pl.ds(1, 1)]

        def get(i):
            ks = (UNIT * mode(SLOTS[i]), ky, kz)
            m1, m2 = c1 * KEPT + i, c2 * KEPT + i
            im = ks[c1] * merged[RE, m2] - ks[c2] * merged[RE, m1]
            re = ks[c2] * merged[IM, m1] - ks[c1] * merged[IM, m2]
            return re, im
        to_x(THREE + f, get)

    def to_grid(f):
        sums = []
        for b in PAIR:
            parts = []
            for ri in PAIR:
                low_hi, hi_mid = lhs[b, ri, f, :, 0:K], lhs[b, ri, f, :, LANES:LANES + K]
                acc = dot(low_hi, inv[b, ri, 0]) + dot(hi_mid, inv[b, ri, 1])
                parts.append(acc + dot(hi_mid, inv[b, ri, 2]))
            sums.append((parts[0] + parts[1], parts[0] - parts[1]))
        for side in PAIR:
            phys[2 * side, f] = sums[0][side] + sums[1][side]
            phys[2 * side + 1, f] = sums[0][side] - sums[1][side]

    def to_spec(c):
        for b in PAIR:
            for ri in PAIR:
                hi, mid, lo = (prod[b, ri, p, c] for p in VEC)
                both = dot(hi, fwd[b, ri, :, 0:K]) + dot(mid, fwd[b, ri, :, 0:K])
                small = dot(lo, fwd[b, ri, :, 0:LANES]) + dot(hi, fwd[b, ri, :, K:])
                spec[b, ri, c] = small + both[:, LANES:] + both[:, :LANES]

    def product(c, point):
        for at in range(0, K, FLOWS):
            rows = slice(at, at + FLOWS)
            n = [point(lambda f: phys[q, f, rows]) for q in FIELDS]
            for b in PAIR:
                side = [n[0] - n[1], n[2] - n[THREE]] if b else [n[0] + n[1], n[2] + n[THREE]]
                for ri in PAIR:
                    v = side[0] - side[1] if ri else side[0] + side[1]
                    for p, part in enumerate(split_bf16(v)):
                        prod[b, ri, p, c, rows] = part

    def cross(c):
        c1, c2 = lax.rem(c + 1, THREE), lax.rem(c + 2, THREE)
        product(c, lambda at: at(c1) * at(THREE + c2) - at(c2) * at(THREE + c1))

    def flux(c):
        product(c, lambda at: at(c) * at(6))

    def from_x(c):
        vals = [tuple(spec[:, ri, c, OCT * x:OCT * x + OCT] for ri in PAIR) for x in range(N)]
        out = fft(vals, -1)
        for i, j in enumerate(SLOTS):
            bins[c, RE, i], bins[c, IM, i] = out[j]

    def phase(re, im):
        cos, sin = wave[:, pl.ds(2, 1)], wave[:, pl.ds(THREE, 1)]
        if re.ndim > THREE:
            cos, sin = cos[:, None], sin[:, None]
        return re * cos - im * sin, re * sin + im * cos

    def project():
        for lo in range(0, KEPT, SEVEN):
            i = slice(lo, lo + SEVEN)
            e = [home[:, k, i] for k in range(5)]
            n = [[bins[c, part, i] for c in VEC] for part in PARTS]
            one = [e[0] * v[0] + e[1] * v[1] for v in n]
            two = [e[2] * v[0] + e[THREE] * v[1] + e[QUAD] * v[2] for v in n]
            for which, v in enumerate((one, two)):
                for part, w in zip(PARTS, phase(*v)):
                    res[part, which, i] = w

    def diverge():
        for i, j in enumerate(SLOTS):
            ks = (UNIT * mode(j), wave[:, pl.ds(0, 1)], wave[:, pl.ds(1, 1)])
            re, im = phase(*[sum(ks[c] * bins[c, part, i] for c in VEC) for part in PARTS])
            res[RE, 2, i] = im
            res[IM, 2, i] = -re
        res[:, 2, KEPT] = jnp.zeros((QUAD, *TILE), F32)

    def result(n):
        return res[:, n % 2, n // 2] if n < 2 * KEPT else res[:, 2, n - 2 * KEPT]

    def unmerge(chunk):
        zero = jnp.zeros(TILE, F32)
        for t in range(*RET_EDGES["D"][chunk:chunk + 2]):
            tiles = swap_blocks([result(QUAD * t + s) for s in FIELDS], False)
            ret_d[0, t], ret_d[1, t] = tiles[:2]
            ret_d[2, t] = jnp.where(low, tiles[2], zero)
            ret_d[THREE, t] = jnp.where(low, roll(tiles[2], -2), zero)
            ends[t] = tiles[THREE]
        for kind in "AB":
            for t in range(*RET_EDGES[kind][chunk:chunk + 2]):
                w = RET[kind][t]
                per, nth = N // w, RET[kind][:t].count(w)
                for c in PAIR:
                    first = 12 + 10 * c if kind == "B" else 20 * c + OCT * (w < OCT)
                    v = None
                    for g in range(per):
                        part = roll(ends[per * nth + g], w * g - first)
                        v = part if v is None else jnp.where(p32 >= w * g, part, v)
                    ret[kind][c, t] = jnp.where(low, v, zero) if c else v

    def ret_part(kind, chunk):
        lo, hi = RET_EDGES[kind][chunk:chunk + 2]
        return ret[kind], pl.ds(lo, hi - lo)

    def ret_copy(kind, chunk, slot, r, c, frm):
        src, part = ret_part(kind, chunk)
        return remote(src.at[slot, part], back.at[frm, part], (s2, r2), dev_of(r, c), frm, chunk, r, c)

    def own_copy(kind, chunk, slot, d):
        src, part = ret_part(kind, chunk)
        return pltpu.make_async_copy(src.at[slot, part], back.at[d, part], own_sem.at[chunk])

    def send_back(chunk):
        for kind, slot, r, c in SOURCES:
            d = dev_of(r, c)

            @pl.when(me != d)
            def _():
                ret_copy(kind, chunk, slot, r, c, me).start()

            @pl.when(me == d)
            def _():
                own_copy(kind, chunk, slot, d).start()

    tab[0].wait()
    for f in VEC:
        wait_chunk(f)
        merge(*OUT_EDGES["D"][f:f + 2])
        field_x(f, f)
        if f == 0:
            for cp in tab[THREE:]:
                cp.wait()
            to_grid(0)
        elif f == 1:
            curl_x(2)
            to_grid(1)
            to_grid(5)
    tab[1].wait()
    tab[2].wait()
    to_grid(2)
    curl_x(0)
    to_grid(THREE)
    curl_x(1)
    to_grid(QUAD)

    @unrolled(THREE)
    def _(c):
        cross(c)
        to_spec(c)
        from_x(c)

    project()
    for chunk in PAIR:
        unmerge(chunk)
        send_back(chunk)
    wait_chunk(THREE)
    merge(*OUT_EDGES["D"][THREE:])
    field_x(6, THREE)
    to_grid(6)
    def flux_part(c, carry):
        flux(c)
        to_spec(c)
        from_x(c)
        return carry
    lax.fori_loop(0, THREE, flux_part, 0)

    diverge()
    unmerge(2)
    send_back(2)

    for kind, here in mine:
        @pl.when(here)
        def _():
            for k in PEERS:
                pr, pc = peer(k)
                for chunk in FIELDS:
                    out_copy(kind, chunk, my_slot[kind], pr, pc, me).wait_send()
                for chunk in VEC:
                    ret_copy(kind, chunk, 0, pr, pc, dev_of(pr, pc)).wait_recv()

    for kind, slot, r, c in SOURCES:
        d = dev_of(r, c)

        @pl.when(me != d)
        def _():
            for chunk in VEC:
                ret_copy(kind, chunk, slot, r, c, me).wait_send()

        @pl.when(me == d)
        def _():
            for chunk in VEC:
                own_copy(kind, chunk, slot, d).wait()


def out_kernel(back_hbm, tab_hbm, ore, oim, tre, tim, buf, tab, back, blank, stage, sem, in_sem, tab_sem):
    row, col = lax.axis_index("row"), lax.axis_index("col")
    dense = kinds_here(row)[0][1]
    loads = [pltpu.make_async_copy(back_hbm.at[:, :, pl.ds(2 * ri, 2)], back.at[:, :, pl.ds(2 * ri, 2)], in_sem.at[ri])
             for ri in PAIR]
    load = pltpu.make_async_copy(tab_hbm.at[dev_of(row, col)], tab, tab_sem)
    for cp in (*loads, load):
        cp.start()
    odd = lax.broadcasted_iota(jnp.int32, (1, LANES), 1) % FLOWS >= N

    def store(f, ri, which):
        first = (0, LOW_ROWS, 2 * LOW_ROWS)[which]
        part = pl.ds(first, LOW_ROWS if which < 2 else ROWS - first)
        dst = (ore, oim)[ri].at[f] if f < THREE else (tre, tim)[ri].at[0]
        src = blank if which == 1 else buf.at[f, ri, part]
        return pltpu.make_async_copy(src, dst.at[part], sem.at[f, ri, which])

    blank[...] = jnp.zeros_like(blank)
    for f in FIELDS:
        for ri in PAIR:
            store(f, ri, 1).start()

    @pl.when(jnp.logical_not(dense))
    def _():
        for f in FIELDS:
            for ri in PAIR:
                for first, size in ((0, LOW_ROWS), (2 * LOW_ROWS, ROWS - 2 * LOW_ROWS)):
                    buf[f, ri, pl.ds(first, size), :] = jnp.zeros((size, FLOWS), F32)
    load.wait()

    def place(ri, b, kind, tile, t, shift, which):
        if RET[kind][t] < OCT:
            stage[...] = tile
        for n, lane, w, start in units(kind, RET, t):
            at = lane - N * shift
            if n < 2 * KEPT:
                if which and n % 2 == 0:
                    continue
                f, i = (2 if which else n % 2), n // 2
            elif which or n >= THREE * KEPT:
                continue
            else:
                f, i = THREE, n - 2 * KEPT
            part = stage[at:at + w, :] if w < OCT else tile[at:at + w]
            buf[f, ri, pl.ds(SLOTS[i] * FLOWS + b + start, w, stride=2), :] = part

    def rebuild(ri, kind):
        tiles = len(RET[kind])
        mixed = [t for t in range(tiles) if min(u[0] for u in units(kind, RET, t)) < 2 * KEPT]
        held = {}
        for t in range(tiles):
            for b in PAIR:
                v = back[:, t, 2 * ri + b].reshape(FLOWS, LANES)
                if t not in mixed:
                    place(ri, b, kind, v.T, t, 0, False)
                    continue
                k = [tab[pl.ds((b * HALF + t) * THREE + q, 1)] for q in VEC]
                other = jnp.where(odd, roll(v, N), roll(v, -N))
                place(ri, b, kind, (v * k[0] + other * k[1]).T, t, 0, False)
                z = v * k[2]
                if b in held:
                    old, zo = held.pop(b)
                    zt = jnp.where(odd, zo, roll(z, -N)).T
                    place(ri, b, kind, zt, old, 0, True)
                    place(ri, b, kind, zt, t, 1, True)
                elif t == mixed[-1]:
                    place(ri, b, kind, z.T, t, 0, True)
                else:
                    held[b] = t, z
            ends = (5, 10, 13, 15) if kind == "D" else ()
            if t in ends:
                e = ends.index(t)
                for f in VEC if e < 2 else (THREE,):
                    store(f, ri, 2 * (e % 2)).start()
        if kind != "D":
            for f in FIELDS:
                for which in (0, 2):
                    store(f, ri, which).start()

    for ri in PAIR:
        loads[ri].wait()

        for kind, here in kinds_here(row):
            @pl.when(here)
            def _():
                rebuild(ri, kind)
    for f in FIELDS:
        for ri in PAIR:
            for which in VEC:
                store(f, ri, which).wait()


def solution(mesh):
    spec_vec = P('ens', None, None, 'row', 'col')
    spec_scal = P('ens', None, 'row', 'col')
    consts = tables()
    src_np = source_tables()
    hbm = pl.BlockSpec(memory_space=pl.ANY)
    dma = pltpu.SemaphoreType.DMA
    links = dma((OCT, QUAD))

    def f32(*lead):
        return pltpu.VMEM((*lead, *TILE), F32)

    def local_term(vel_re, vel_im, scal_re, scal_im):
        vec = [jnp.transpose(a, (1, 2, THREE, QUAD, 0)).reshape(THREE, ROWS, FLOWS) for a in (vel_re, vel_im)]
        scal = [jnp.transpose(a, (1, 2, THREE, 0)).reshape(1, ROWS, FLOWS) for a in (scal_re, scal_im)]
        back = pl.pallas_call(
            main_kernel,
            out_shape=jax.ShapeDtypeStruct((OCT, HALF, QUAD, *TILE), F32),
            in_specs=[hbm] * OCT,
            out_specs=hbm,
            scratch_shapes=[
                pltpu.VMEM((2, QUAD * KEPT_ROWS, FLOWS), F32), f32(OCT, len(OUT["D"]), QUAD),
                *[f32(2 * len(rows), len(OUT[kind]), QUAD) for kind, rows in KINDS.items()],
                f32(QUAD, QUAD * KEPT), pltpu.VMEM((2, 2, SEVEN, K, THREE * LANES), BF16), pltpu.VMEM((QUAD, SEVEN, K, K), F32),
                pltpu.VMEM((2, 2, THREE, THREE, K, K), BF16), pltpu.VMEM((2, 2, THREE, K, LANES), F32), f32(THREE, QUAD, KEPT),
                f32(QUAD, THREE, KEPT + 1), f32(HALF, QUAD),
                *[f32(2 * len(rows), len(RET[kind]), QUAD) for kind, rows in KINDS.items()], pltpu.VMEM((LANES, FLOWS), F32),
                pltpu.VMEM((2, 2, THREE, K, K), BF16), *[pltpu.VMEM(a.shape, a.dtype) for a in consts[1:]],
                dma((QUAD, 2, 2)), dma((9,)), dma((THREE,)), links, links, links, links,
            ],
            compiler_params=pltpu.CompilerParams(
                collective_id=0, has_side_effects=True, vmem_limit_bytes=60 * MIB),
            name="flow_home",
        )(*vec, *scal, *[jnp.asarray(a) for a in consts])
        outs = pl.pallas_call(
            out_kernel,
            out_shape=[jax.ShapeDtypeStruct((c, ROWS, FLOWS), F32) for c in (THREE, THREE, 1, 1)],
            in_specs=[hbm, hbm],
            out_specs=[hbm] * QUAD,
            scratch_shapes=[pltpu.VMEM((QUAD, 2, ROWS, FLOWS), F32), pltpu.VMEM(src_np.shape[1:], F32),
                            f32(OCT, HALF, QUAD), pltpu.VMEM((LOW_ROWS, FLOWS), F32), pltpu.VMEM((LANES, FLOWS), F32), dma((QUAD, 2, THREE)), dma((2,)), dma],
            compiler_params=pltpu.CompilerParams(vmem_limit_bytes=60 * MIB),
            name="lay_out",
        )(back, jnp.asarray(src_np))
        out_v = [jnp.transpose(a.reshape(THREE, N, OCT, OCT, FLOWS), (QUAD, 0, 1, 2, THREE)) for a in outs[:2]]
        out_s = [jnp.transpose(a.reshape(N, OCT, OCT, FLOWS), (THREE, 0, 1, 2)) for a in outs[2:]]
        return (*out_v, *out_s)

    return jax.shard_map(local_term, mesh=mesh, in_specs=(spec_vec, spec_vec, spec_scal, spec_scal),
                         out_specs=(spec_vec, spec_vec, spec_scal, spec_scal), check_vma=False)
```

```python
import math

import jax
import jax.numpy as jnp
import numpy as np
from jax import lax
from jax.experimental import pallas as pl
from jax.experimental.pallas import tpu as pltpu
from jax.sharding import PartitionSpec as P

N = 32
LANES = 128
FLOWS = 64
ROWS = 2048
TILE = (8, LANES)
K = 256
TINY = 1e-9
MIB = 1 << 20
THREE, QUAD, SEVEN, OCT, HALF = 3, 4, 7, 8, 16
PARTS = RE, IM = slice(0, 2), slice(2, QUAD)
PAIR, VEC, FIELDS, PEERS = range(2), range(THREE), range(QUAD), range(1, OCT)
MESH = pl.DeviceIdType.MESH
F32 = jnp.float32
BF16 = jnp.bfloat16
UNIT = 2 * math.pi / N
SLOTS = list(range(11)) + list(range(22, N))
KEPT = len(SLOTS)
KEPT_ROWS = KEPT * FLOWS
LOW_ROWS = 11 * FLOWS
KINDS = {"D": (0, THREE), "A": (1,), "B": (2,)}
OUT = {"D": (N,) * 21, "A": (OCT, OCT, QUAD, OCT, QUAD, OCT, OCT, QUAD), "B": (OCT,) * 6}
RET = {"D": (N,) * HALF, "A": (OCT, OCT, QUAD, OCT, OCT, QUAD), "B": (OCT,) * QUAD}
OUT_EDGES = {"D": (0, 6, 11, HALF, 21), "A": (0, THREE, 5, 6, OCT), "B": (0, 2, THREE, QUAD, 6)}
RET_EDGES = {"D": (0, QUAD, 10, HALF), "A": (0, 1, THREE, 6), "B": (0, 1, 2, QUAD)}
SOURCES = [(kind, k * len(rows) + i, r, k) for kind, rows in KINDS.items() for k in PAIR for i, r in enumerate(rows)]


def units(kind, table, t):
    widths = table[kind]
    w = widths[t]
    per, nth = N // w, widths[:t].count(w)
    first = 48 if kind == "B" else HALF * (w == QUAD)
    out = []
    for s in FIELDS:
        for g in range(per):
            slot, start = QUAD * (per * nth + g) + s, first
            if slot >= QUAD * KEPT:
                slot, start = QUAD * (KEPT - 1) + s, first if kind == "B" else OCT * min(g - 5, 1)
            out.append((slot, N * s + w * g, w, start))
    return out


def place_of(kind, table, w, nth):
    return [t for t, v in enumerate(table[kind]) if v == w][nth]


def mode(j):
    return j if j < N // 2 else j - N


def kept(m):
    return THREE * abs(m) < N


def home_mode(lane, parity):
    block, p = divmod(lane, N)
    y, high, half = p // QUAD, p % QUAD // 2, p % QUAD
    if block < 2:
        row, col = THREE * block, 0
    elif block == 2:
        row, col, half = THREE * high, 1, p % 2
    elif p < 12:
        row, col = 1, 0
    elif p < 20:
        row, col, y = 2, 0, y + THREE
    else:
        row, col, half, y = 1 + high, 1, p % 2, y - 5 + 6 * high
    if y > SEVEN:
        return None
    ky, kz = mode(OCT * row + y), OCT * col + 2 * half + parity
    return (ky, kz) if kept(ky) and kept(kz) else None


def basis(kx, ky, kz):
    flat, full = math.hypot(kx, ky), math.hypot(kx, ky, kz)
    if full == 0:
        return np.zeros(THREE), np.zeros(THREE)
    if flat == 0:
        return np.array([1.0, 0, 0]), np.array([0, 1.0, 0])
    e1 = np.array([ky, -kx, 0]) / flat
    return e1, np.array([kx * kz, ky * kz, -flat * flat]) / (flat * full)


def split3(x):
    x = np.asarray(x, np.float32)
    hi = x.astype(BF16)
    rest = x - hi.astype(np.float32)
    mid = rest.astype(BF16)
    return hi, mid, (rest - mid.astype(np.float32)).astype(BF16)


def tables():
    scale = float(N) ** -1.5
    half = N // 2
    points = [(y, z) for z in range(1, OCT) for y in range(N)] + [(y, z) for z in (0, OCT) for y in range(half)]
    yy, zz = np.array(points).T
    inv = np.zeros((2, 2, LANES, K))
    wave = np.zeros((2, QUAD, LANES), np.float32)
    home = np.zeros((2, 5, KEPT, 1, LANES), np.float32)
    for parity in PAIR:
        for lane in range(LANES):
            got = home_mode(lane, parity)
            if got is None:
                continue
            ky, kz = got
            ang = UNIT * (ky * (yy + 0.5) + kz * zz)
            inv[parity, 0, lane] = scale * np.cos(ang)
            inv[parity, 1, lane] = -scale * np.sin(ang)
            wave[parity, :, lane] = ky * UNIT, kz * UNIT, math.cos(UNIT * ky / 2), math.sin(UNIT * ky / 2)
            for i, j in enumerate(SLOTS):
                e1, e2 = basis(mode(j), ky, kz)
                home[parity, :, i, 0, lane] = *e1[:2], *e2
    fwd = np.swapaxes(inv, 2, THREE)
    weight = np.full((2, 1, LANES, 1), 2.0)
    for lane in range(LANES):
        got = home_mode(lane, 0)
        if got is not None and got[1] == 0:
            weight[0, 0, lane] = 1.0
    inv3 = np.stack(split3(inv * weight))
    fwd3 = np.concatenate(split3(fwd), axis=THREE)
    return inv3, fwd3, wave, home


def source_tables():
    out = np.zeros((OCT, 2, HALF, THREE, LANES), np.float32)
    for kind, _, row, col in SOURCES:
        for t in range(len(RET[kind])):
            for n, lane, w, start in units(kind, RET, t):
                for o in range(w):
                    y, half = divmod(start // 2 + o, QUAD)
                    for parity in PAIR:
                        ky, kz = mode(OCT * row + y), OCT * col + 2 * half + parity
                        to = out[dev_of(row, col), parity, t, :, lane + o]
                        if n >= 2 * KEPT:
                            to[0] = 1
                        elif kept(ky) and kept(kz):
                            e1, e2 = basis(mode(SLOTS[n // 2]), ky, kz)
                            to[:] = (e2[1], e1[1], e2[2]) if n % 2 else (e1[0], e2[0], 0)
    return out.reshape(OCT, -1, LANES)


def cmul_const(a, c, s):
    re, im = a
    if abs(s) < TINY:
        return (re, im) if c > 0 else (-re, -im)
    if abs(c) < TINY:
        return (-im, re) if s > 0 else (im, -re)
    if abs(abs(c) - abs(s)) < TINY:
        p, q = (re - im) * abs(c), (re + im) * abs(c)
        if c > 0:
            return (p, q) if s > 0 else (q, -p)
        return (-q, p) if s > 0 else (-p, -q)
    return re * c - im * s, re * s + im * c


def fft(vals, sign):
    n = len(vals)
    if n == 1:
        return list(vals)
    even, odd = fft(vals[0::2], sign), fft(vals[1::2], sign)
    out = [None] * n
    for k in range(n // 2):
        a, b = even[k], odd[k]
        if b is not None:
            ang = sign * 2 * math.pi * k / n
            b = cmul_const(b, math.cos(ang), math.sin(ang))
        if a is None and b is None:
            continue
        if b is None:
            out[k], out[k + n // 2] = a, a
        elif a is None:
            out[k], out[k + n // 2] = b, (-b[0], -b[1])
        else:
            out[k] = (a[0] + b[0], a[1] + b[1])
            out[k + n // 2] = (a[0] - b[0], a[1] - b[1])
    return out


def dot(a, b):
    return jnp.dot(a, b, preferred_element_type=F32)


def split_bf16(x):
    hi = x.astype(BF16)
    rest = x - hi.astype(F32)
    mid = rest.astype(BF16)
    low = (rest - mid.astype(F32)).astype(BF16)
    return hi, mid, low


def dev_of(row, col):
    return col * QUAD + row


def kinds_here(row):
    tests = {"D": jnp.logical_or(row == 0, row == THREE), "A": row == 1, "B": row == 2}
    return list(tests.items())


def unrolled(n):
    def run(body):
        lax.fori_loop(0, n, lambda i, carry: (body(i), carry)[1], 0, unroll=True)
    return run


def roll(x, shift):
    shift %= LANES
    return pltpu.roll(x, shift, x.ndim - 1) if shift else x


def main_kernel(vre, vim, sre, sim, inv_hbm, fwd_hbm, wave_hbm, home_hbm, back,
                xin, send, recv_d, recv_a, recv_b, merged, lhs, phys, prod, spec, bins, res, ends, ret_d, ret_a, ret_b, stage,
                inv, fwd, wave, home, in_sem, tab_sem, own_sem, s1, r1, s2, r2):
    row, col, ens = lax.axis_index("row"), lax.axis_index("col"), lax.axis_index("ens")
    me = dev_of(row, col)
    recv = {"D": recv_d, "A": recv_a, "B": recv_b}
    ret = {"D": ret_d, "A": ret_a, "B": ret_b}
    mine = kinds_here(row)
    my_slot = {"D": col * 2 + jnp.where(row == THREE, 1, 0), "A": col, "B": col}

    loads = []
    for f in FIELDS:
        for ri in PAIR:
            src = (vre, vim)[ri].at[f] if f < THREE else (sre, sim)[ri].at[0]
            for half, (a, size, b) in enumerate(((0, LOW_ROWS, 0), (2 * LOW_ROWS, KEPT_ROWS - LOW_ROWS, LOW_ROWS))):
                cp = pltpu.make_async_copy(
                    src.at[pl.ds(a, size)], xin.at[ri, pl.ds(KEPT_ROWS * f + b, size)], in_sem.at[f, ri, half])
                loads.append(cp)
    first, later = loads[:OCT], loads[OCT:]
    for cp in first:
        cp.start()
    wanted = [(wave_hbm, wave), (fwd_hbm, fwd), (home_hbm, home)]
    wanted += [(inv_hbm.at[part], inv.at[:, :, pair, pl.ds(LANES * h, LANES)])
               for pair, parts in enumerate(((0, 2), (1, 1), (0, 0))) for h, part in enumerate(parts)]
    tab = [pltpu.make_async_copy(src, dst, tab_sem.at[i]) for i, (src, dst) in enumerate(wanted)]
    barrier = pltpu.get_barrier_semaphore()

    def peer(k):
        return row ^ (k % QUAD), col ^ (k // QUAD)

    for k in PEERS:
        pr, pc = peer(k)
        pl.semaphore_signal(barrier, inc=1, device_id=(ens, pc, pr), device_id_type=MESH)

    def pack(kind, lo, hi):
        if kind == "D":
            def body(n, carry):
                t, rb = lax.div(n, QUAD), lax.rem(n, QUAD)
                blk = xin[lax.div(rb, 2), pl.ds(t * K + lax.rem(rb, 2), LANES, stride=2), :]
                send[:, t, rb] = blk.T.reshape(OCT, *TILE)
                return carry
            lax.fori_loop(QUAD * lo, QUAD * hi, body, 0, unroll=QUAD)
            return

        def few(rb, carry):
            ri, b = lax.div(rb, 2), lax.rem(rb, 2)
            for t in range(lo, hi):
                parts = [xin[ri, pl.ds(slot * FLOWS + start + b, w, stride=2), :] for slot, _, w, start in units(kind, OUT, t)]
                if OUT[kind][t] < OCT:
                    for (_, lane, w, _), part in zip(units(kind, OUT, t), parts):
                        stage[lane:lane + w, :] = part
                    blk = stage[...]
                else:
                    order = np.argsort([u[1] for u in units(kind, OUT, t)])
                    blk = jnp.concatenate([parts[i] for i in order], axis=0)
                send[:, t, rb] = blk.T.reshape(OCT, *TILE)
            return carry
        lax.fori_loop(0, QUAD, few, 0, unroll=2)

    def remote(src, dst, sems, i, j, chunk, r, c):
        return pltpu.make_async_remote_copy(
            src_ref=src, dst_ref=dst, send_sem=sems[0].at[i, chunk], recv_sem=sems[1].at[j, chunk],
            device_id=(ens, c, r), device_id_type=MESH)

    def out_copy(kind, chunk, slot, r, c, frm):
        lo, hi = OUT_EDGES[kind][chunk:chunk + 2]
        to = dev_of(r, c)
        part = pl.ds(lo, hi - lo)
        return remote(send.at[to, part], recv[kind].at[slot, part], (s1, r1), to, frm, chunk, r, c)

    for chunk in FIELDS:
        for cp in (first, later, (), ())[chunk]:
            cp.wait()
        if chunk == 0:
            for cp in (*later, *tab):
                cp.start()
        for kind, here in mine:
            @pl.when(here)
            def _():
                pack(kind, *OUT_EDGES[kind][chunk:chunk + 2])
        if chunk == 0:
            pl.semaphore_wait(barrier, SEVEN)
        for kind, here in mine:
            @pl.when(here)
            def _():
                lo, hi = OUT_EDGES[kind][chunk:chunk + 2]
                for k in PEERS:
                    out_copy(kind, chunk, my_slot[kind], *peer(k), me).start()
                recv[kind][my_slot[kind], lo:hi] = send[me, lo:hi]

    lane = lax.broadcasted_iota(jnp.int32, TILE, 1)
    low = lane % QUAD < 2
    p32 = lane % N
    left, even = lane < FLOWS, lane % FLOWS < N

    def wait_chunk(chunk):
        for kind, slot, r, c in SOURCES:
            @pl.when(me != dev_of(r, c))
            def _():
                out_copy(kind, chunk, slot, r, c, dev_of(r, c)).wait_recv()

    def swap_blocks(tiles, forward):
        def outer(a, b, c, d):
            ca, db = roll(jnp.where(left, c, a), FLOWS), roll(jnp.where(left, d, b), FLOWS)
            return jnp.where(left, a, ca), jnp.where(left, b, db), jnp.where(left, ca, c), jnp.where(left, db, d)

        def inner(a, b, c, d):
            return (jnp.where(even, a, roll(b, N)), jnp.where(even, roll(a, -N), b),
                    jnp.where(even, c, roll(d, N)), jnp.where(even, roll(c, -N), d))
        return inner(*outer(*tiles)) if forward else outer(*inner(*tiles))

    def merge(lo, hi):
        cos, sin = wave[:, pl.ds(2, 1)], wave[:, pl.ds(THREE, 1)]
        for t in range(lo, hi):
            got = []
            for part in PARTS:
                d = [recv_d[o, t, part] for o in FIELDS]
                g, g4 = OCT * (t % QUAD), QUAD * (t % OCT)
                a4 = place_of("A", OUT, QUAD, t // OCT)
                a8, at = (a4, 20) if t == KEPT - 1 else (place_of("A", OUT, OCT, t // QUAD), g)
                c1 = jnp.where(low, d[2], roll(d[THREE], 2))
                v = [(roll(recv_a[c, a8, part], 20 * c - at), roll(recv_a[c, a4, part], 20 * c + OCT - g4),
                      roll(recv_b[c, t // QUAD, part], 10 * c + 12 - g)) for c in PAIR]
                rest = jnp.where(low, jnp.where(p32 < 28, v[1][0], v[1][1]), v[1][2])
                s1_ = jnp.where(p32 < OCT, v[0][0], jnp.where(p32 < 12, v[0][1], jnp.where(p32 < 20, v[0][2], rest)))
                got.append(swap_blocks((d[0], d[1], c1, s1_), True))
            for s, (re, im) in enumerate(zip(*got)):
                merged[RE, QUAD * t + s] = re * cos + im * sin
                merged[IM, QUAD * t + s] = im * cos - re * sin

    def to_x(f, get):
        vals = [None] * N
        for i, j in enumerate(SLOTS):
            vals[j] = get(i)
        out = fft(vals, 1)
        for x in range(0, N, 2):
            for ri in PAIR:
                hi, mid, lo = split_bf16(jnp.concatenate([out[x][ri], out[x + 1][ri]], axis=1))
                for p, part in enumerate((lo, hi, mid)):
                    lhs[:, ri, f, OCT * x:OCT * x + HALF, LANES * p:LANES * p + LANES] = part

    def field_x(f, src):
        to_x(f, lambda i: (merged[RE, src * KEPT + i], merged[IM, src * KEPT + i]))

    def curl_x(f):
        c1, c2 = (f + 1) % THREE, (f + 2) % THREE
        ky, kz = wave[:, pl.ds(0, 1)], wave[:, pl.ds(1, 1)]

        def get(i):
            ks = (UNIT * mode(SLOTS[i]), ky, kz)
            m1, m2 = c1 * KEPT + i, c2 * KEPT + i
            im = ks[c1] * merged[RE, m2] - ks[c2] * merged[RE, m1]
            re = ks[c2] * merged[IM, m1] - ks[c1] * merged[IM, m2]
            return re, im
        to_x(THREE + f, get)

    def to_grid(f):
        sums = []
        for b in PAIR:
            parts = []
            for ri in PAIR:
                low_hi, hi_mid = lhs[b, ri, f, :, 0:K], lhs[b, ri, f, :, LANES:LANES + K]
                acc = dot(low_hi, inv[b, ri, 0]) + dot(hi_mid, inv[b, ri, 1])
                parts.append(acc + dot(hi_mid, inv[b, ri, 2]))
            sums.append((parts[0] + parts[1], parts[0] - parts[1]))
        for side in PAIR:
            phys[2 * side, f] = sums[0][side] + sums[1][side]
            phys[2 * side + 1, f] = sums[0][side] - sums[1][side]

    def to_spec(c):
        for b in PAIR:
            for ri in PAIR:
                hi, mid, lo = (prod[b, ri, p, c] for p in VEC)
                both = dot(hi, fwd[b, ri, :, 0:K]) + dot(mid, fwd[b, ri, :, 0:K])
                small = dot(lo, fwd[b, ri, :, 0:LANES]) + dot(hi, fwd[b, ri, :, K:])
                spec[b, ri, c] = small + both[:, LANES:] + both[:, :LANES]

    def product(c, point):
        for at in range(0, K, FLOWS):
            rows = slice(at, at + FLOWS)
            n = [point(lambda f: phys[q, f, rows]) for q in FIELDS]
            for b in PAIR:
                side = [n[0] - n[1], n[2] - n[THREE]] if b else [n[0] + n[1], n[2] + n[THREE]]
                for ri in PAIR:
                    v = side[0] - side[1] if ri else side[0] + side[1]
                    for p, part in enumerate(split_bf16(v)):
                        prod[b, ri, p, c, rows] = part

    def cross(c):
        c1, c2 = lax.rem(c + 1, THREE), lax.rem(c + 2, THREE)
        product(c, lambda at: at(c1) * at(THREE + c2) - at(c2) * at(THREE + c1))

    def flux(c):
        product(c, lambda at: at(c) * at(6))

    def from_x(c):
        vals = [tuple(spec[:, ri, c, OCT * x:OCT * x + OCT] for ri in PAIR) for x in range(N)]
        out = fft(vals, -1)
        for i, j in enumerate(SLOTS):
            bins[c, RE, i], bins[c, IM, i] = out[j]

    def phase(re, im):
        cos, sin = wave[:, pl.ds(2, 1)], wave[:, pl.ds(THREE, 1)]
        if re.ndim > THREE:
            cos, sin = cos[:, None], sin[:, None]
        return re * cos - im * sin, re * sin + im * cos

    def project():
        for lo in range(0, KEPT, SEVEN):
            i = slice(lo, lo + SEVEN)
            e = [home[:, k, i] for k in range(5)]
            n = [[bins[c, part, i] for c in VEC] for part in PARTS]
            one = [e[0] * v[0] + e[1] * v[1] for v in n]
            two = [e[2] * v[0] + e[THREE] * v[1] + e[QUAD] * v[2] for v in n]
            for which, v in enumerate((one, two)):
                for part, w in zip(PARTS, phase(*v)):
                    res[part, which, i] = w

    def diverge():
        for i, j in enumerate(SLOTS):
            ks = (UNIT * mode(j), wave[:, pl.ds(0, 1)], wave[:, pl.ds(1, 1)])
            re, im = phase(*[sum(ks[c] * bins[c, part, i] for c in VEC) for part in PARTS])
            res[RE, 2, i] = im
            res[IM, 2, i] = -re
        res[:, 2, KEPT] = jnp.zeros((QUAD, *TILE), F32)

    def result(n):
        return res[:, n % 2, n // 2] if n < 2 * KEPT else res[:, 2, n - 2 * KEPT]

    def unmerge(chunk):
        zero = jnp.zeros(TILE, F32)
        for t in range(*RET_EDGES["D"][chunk:chunk + 2]):
            tiles = swap_blocks([result(QUAD * t + s) for s in FIELDS], False)
            ret_d[0, t], ret_d[1, t] = tiles[:2]
            ret_d[2, t] = jnp.where(low, tiles[2], zero)
            ret_d[THREE, t] = jnp.where(low, roll(tiles[2], -2), zero)
            ends[t] = tiles[THREE]
        for kind in "AB":
            for t in range(*RET_EDGES[kind][chunk:chunk + 2]):
                w = RET[kind][t]
                per, nth = N // w, RET[kind][:t].count(w)
                for c in PAIR:
                    first = 12 + 10 * c if kind == "B" else 20 * c + OCT * (w < OCT)
                    v = None
                    for g in range(per):
                        part = roll(ends[per * nth + g], w * g - first)
                        v = part if v is None else jnp.where(p32 >= w * g, part, v)
                    ret[kind][c, t] = jnp.where(low, v, zero) if c else v

    def ret_part(kind, chunk):
        lo, hi = RET_EDGES[kind][chunk:chunk + 2]
        return ret[kind], pl.ds(lo, hi - lo)

    def ret_copy(kind, chunk, slot, r, c, frm):
        src, part = ret_part(kind, chunk)
        return remote(src.at[slot, part], back.at[frm, part], (s2, r2), dev_of(r, c), frm, chunk, r, c)

    def own_copy(kind, chunk, slot, d):
        src, part = ret_part(kind, chunk)
        return pltpu.make_async_copy(src.at[slot, part], back.at[d, part], own_sem.at[chunk])

    def send_back(chunk):
        for kind, slot, r, c in SOURCES:
            d = dev_of(r, c)

            @pl.when(me != d)
            def _():
                ret_copy(kind, chunk, slot, r, c, me).start()

            @pl.when(me == d)
            def _():
                own_copy(kind, chunk, slot, d).start()

    tab[0].wait()
    for f in VEC:
        wait_chunk(f)
        merge(*OUT_EDGES["D"][f:f + 2])
        field_x(f, f)
        if f == 0:
            for cp in tab[THREE:]:
                cp.wait()
            to_grid(0)
        elif f == 1:
            curl_x(2)
            to_grid(1)
            to_grid(5)
    tab[1].wait()
    tab[2].wait()
    to_grid(2)
    curl_x(0)
    to_grid(THREE)
    curl_x(1)
    to_grid(QUAD)

    @unrolled(THREE)
    def _(c):
        cross(c)
        to_spec(c)
        from_x(c)

    project()
    for chunk in PAIR:
        unmerge(chunk)
        send_back(chunk)
    wait_chunk(THREE)
    merge(*OUT_EDGES["D"][THREE:])
    field_x(6, THREE)
    to_grid(6)
    def flux_part(c, carry):
        flux(c)
        to_spec(c)
        from_x(c)
        return carry
    lax.fori_loop(0, THREE, flux_part, 0)

    diverge()
    unmerge(2)
    send_back(2)

    for kind, here in mine:
        @pl.when(here)
        def _():
            for k in PEERS:
                pr, pc = peer(k)
                for chunk in FIELDS:
                    out_copy(kind, chunk, my_slot[kind], pr, pc, me).wait_send()
                for chunk in VEC:
                    ret_copy(kind, chunk, 0, pr, pc, dev_of(pr, pc)).wait_recv()

    for kind, slot, r, c in SOURCES:
        d = dev_of(r, c)

        @pl.when(me != d)
        def _():
            for chunk in VEC:
                ret_copy(kind, chunk, slot, r, c, me).wait_send()

        @pl.when(me == d)
        def _():
            for chunk in VEC:
                own_copy(kind, chunk, slot, d).wait()


def out_kernel(back_hbm, tab_hbm, ore, oim, tre, tim, buf, tab, back, blank, stage, sem, in_sem, tab_sem):
    row, col = lax.axis_index("row"), lax.axis_index("col")
    dense = kinds_here(row)[0][1]
    loads = [pltpu.make_async_copy(back_hbm.at[:, :, pl.ds(2 * ri, 2)], back.at[:, :, pl.ds(2 * ri, 2)], in_sem.at[ri])
             for ri in PAIR]
    load = pltpu.make_async_copy(tab_hbm.at[dev_of(row, col)], tab, tab_sem)
    for cp in (*loads, load):
        cp.start()
    odd = lax.broadcasted_iota(jnp.int32, (1, LANES), 1) % FLOWS >= N

    def store(f, ri, which):
        first = (0, LOW_ROWS, 2 * LOW_ROWS)[which]
        part = pl.ds(first, LOW_ROWS if which < 2 else ROWS - first)
        dst = (ore, oim)[ri].at[f] if f < THREE else (tre, tim)[ri].at[0]
        src = blank if which == 1 else buf.at[f, ri, part]
        return pltpu.make_async_copy(src, dst.at[part], sem.at[f, ri, which])

    blank[...] = jnp.zeros_like(blank)
    for f in FIELDS:
        for ri in PAIR:
            store(f, ri, 1).start()

    @pl.when(jnp.logical_not(dense))
    def _():
        for f in FIELDS:
            for ri in PAIR:
                for first, size in ((0, LOW_ROWS), (2 * LOW_ROWS, ROWS - 2 * LOW_ROWS)):
                    buf[f, ri, pl.ds(first, size), :] = jnp.zeros((size, FLOWS), F32)
    load.wait()

    def place(ri, b, kind, tile, t, shift, which):
        if RET[kind][t] < OCT:
            stage[...] = tile
        for n, lane, w, start in units(kind, RET, t):
            at = lane - N * shift
            if n < 2 * KEPT:
                if which and n % 2 == 0:
                    continue
                f, i = (2 if which else n % 2), n // 2
            elif which or n >= THREE * KEPT:
                continue
            else:
                f, i = THREE, n - 2 * KEPT
            part = stage[at:at + w, :] if w < OCT else tile[at:at + w]
            buf[f, ri, pl.ds(SLOTS[i] * FLOWS + b + start, w, stride=2), :] = part

    def rebuild(ri, kind):
        tiles = len(RET[kind])
        mixed = [t for t in range(tiles) if min(u[0] for u in units(kind, RET, t)) < 2 * KEPT]
        held = {}
        for t in range(tiles):
            for b in PAIR:
                v = back[:, t, 2 * ri + b].reshape(FLOWS, LANES)
                if t not in mixed:
                    place(ri, b, kind, v.T, t, 0, False)
                    continue
                k = [tab[pl.ds((b * HALF + t) * THREE + q, 1)] for q in VEC]
                other = jnp.where(odd, roll(v, N), roll(v, -N))
                place(ri, b, kind, (v * k[0] + other * k[1]).T, t, 0, False)
                z = v * k[2]
                if b in held:
                    old, zo = held.pop(b)
                    zt = jnp.where(odd, zo, roll(z, -N)).T
                    place(ri, b, kind, zt, old, 0, True)
                    place(ri, b, kind, zt, t, 1, True)
                elif t == mixed[-1]:
                    place(ri, b, kind, z.T, t, 0, True)
                else:
                    held[b] = t, z
            ends = (5, 10, 13, 15) if kind == "D" else ()
            if t in ends:
                e = ends.index(t)
                for f in VEC if e < 2 else (THREE,):
                    store(f, ri, 2 * (e % 2)).start()
        if kind != "D":
            for f in FIELDS:
                for which in (0, 2):
                    store(f, ri, which).start()

    for ri in PAIR:
        loads[ri].wait()

        for kind, here in kinds_here(row):
            @pl.when(here)
            def _():
                rebuild(ri, kind)
    for f in FIELDS:
        for ri in PAIR:
            for which in VEC:
                store(f, ri, which).wait()


def solution(mesh):
    spec_vec = P('ens', None, None, 'row', 'col')
    spec_scal = P('ens', None, 'row', 'col')
    consts = tables()
    src_np = source_tables()
    hbm = pl.BlockSpec(memory_space=pl.ANY)
    dma = pltpu.SemaphoreType.DMA
    links = dma((OCT, QUAD))

    def f32(*lead):
        return pltpu.VMEM((*lead, *TILE), F32)

    def local_term(vel_re, vel_im, scal_re, scal_im):
        vec = [jnp.transpose(a, (1, 2, THREE, QUAD, 0)).reshape(THREE, ROWS, FLOWS) for a in (vel_re, vel_im)]
        scal = [jnp.transpose(a, (1, 2, THREE, 0)).reshape(1, ROWS, FLOWS) for a in (scal_re, scal_im)]
        back = pl.pallas_call(
            main_kernel,
            out_shape=jax.ShapeDtypeStruct((OCT, HALF, QUAD, *TILE), F32),
            in_specs=[hbm] * OCT,
            out_specs=hbm,
            scratch_shapes=[
                pltpu.VMEM((2, QUAD * KEPT_ROWS, FLOWS), F32), f32(OCT, len(OUT["D"]), QUAD),
                *[f32(2 * len(rows), len(OUT[kind]), QUAD) for kind, rows in KINDS.items()],
                f32(QUAD, QUAD * KEPT), pltpu.VMEM((2, 2, SEVEN, K, THREE * LANES), BF16), pltpu.VMEM((QUAD, SEVEN, K, K), F32),
                pltpu.VMEM((2, 2, THREE, THREE, K, K), BF16), pltpu.VMEM((2, 2, THREE, K, LANES), F32), f32(THREE, QUAD, KEPT),
                f32(QUAD, THREE, KEPT + 1), f32(HALF, QUAD),
                *[f32(2 * len(rows), len(RET[kind]), QUAD) for kind, rows in KINDS.items()], pltpu.VMEM((LANES, FLOWS), F32),
                pltpu.VMEM((2, 2, THREE, K, K), BF16), *[pltpu.VMEM(a.shape, a.dtype) for a in consts[1:]],
                dma((QUAD, 2, 2)), dma((9,)), dma((THREE,)), links, links, links, links,
            ],
            compiler_params=pltpu.CompilerParams(
                collective_id=0, has_side_effects=True, vmem_limit_bytes=60 * MIB),
            name="flow_home",
        )(*vec, *scal, *[jnp.asarray(a) for a in consts])
        outs = pl.pallas_call(
            out_kernel,
            out_shape=[jax.ShapeDtypeStruct((c, ROWS, FLOWS), F32) for c in (THREE, THREE, 1, 1)],
            in_specs=[hbm, hbm],
            out_specs=[hbm] * QUAD,
            scratch_shapes=[pltpu.VMEM((QUAD, 2, ROWS, FLOWS), F32), pltpu.VMEM(src_np.shape[1:], F32),
                            f32(OCT, HALF, QUAD), pltpu.VMEM((LOW_ROWS, FLOWS), F32), pltpu.VMEM((LANES, FLOWS), F32), dma((QUAD, 2, THREE)), dma((2,)), dma],
            compiler_params=pltpu.CompilerParams(vmem_limit_bytes=60 * MIB),
            name="lay_out",
        )(back, jnp.asarray(src_np))
        out_v = [jnp.transpose(a.reshape(THREE, N, OCT, OCT, FLOWS), (QUAD, 0, 1, 2, THREE)) for a in outs[:2]]
        out_s = [jnp.transpose(a.reshape(N, OCT, OCT, FLOWS), (THREE, 0, 1, 2)) for a in outs[2:]]
        return (*out_v, *out_s)

    return jax.shard_map(local_term, mesh=mesh, in_specs=(spec_vec, spec_vec, spec_scal, spec_scal),
                         out_specs=(spec_vec, spec_vec, spec_scal, spec_scal), check_vma=False)
```

```python
import math

import jax
import jax.numpy as jnp
import numpy as np
from jax import lax
from jax.experimental import pallas as pl
from jax.experimental.pallas import tpu as pltpu
from jax.sharding import PartitionSpec as P

N = 32
LANES = 128
FLOWS = 64
ROWS = 2048
TILE = (8, LANES)
K = 256
TINY = 1e-9
MIB = 1 << 20
THREE, QUAD, SEVEN, OCT, HALF = 3, 4, 7, 8, 16
PARTS = RE, IM = slice(0, 2), slice(2, QUAD)
PAIR, VEC, FIELDS, PEERS = range(2), range(THREE), range(QUAD), range(1, OCT)
MESH = pl.DeviceIdType.MESH
F32 = jnp.float32
BF16 = jnp.bfloat16
UNIT = 2 * math.pi / N
SLOTS = list(range(11)) + list(range(22, N))
KEPT = len(SLOTS)
KEPT_ROWS = KEPT * FLOWS
LOW_ROWS = 11 * FLOWS
KINDS = {"D": (0, THREE), "A": (1,), "B": (2,)}
OUT = {"D": (N,) * 21, "A": (OCT, OCT, QUAD, OCT, QUAD, OCT, OCT, QUAD), "B": (OCT,) * 6}
RET = {"D": (N,) * HALF, "A": (OCT, OCT, QUAD, OCT, OCT, QUAD), "B": (OCT,) * QUAD}
OUT_EDGES = {"D": (0, 6, 11, HALF, 21), "A": (0, THREE, 5, 6, OCT), "B": (0, 2, THREE, QUAD, 6)}
RET_EDGES = {"D": (0, QUAD, 10, HALF), "A": (0, 1, THREE, 6), "B": (0, 1, 2, QUAD)}
BACK = [((0, 1), (0,)), ((1, 2), (0,)), ((0, 2), (1,)), ((2, THREE), (0, 1))]
SOURCES = [(kind, k * len(rows) + i, r, k) for kind, rows in KINDS.items() for k in PAIR for i, r in enumerate(rows)]


def units(kind, table, t):
    widths = table[kind]
    w = widths[t]
    per, nth = N // w, widths[:t].count(w)
    first = 48 if kind == "B" else HALF * (w == QUAD)
    out = []
    for s in FIELDS:
        for g in range(per):
            slot, start = QUAD * (per * nth + g) + s, first
            if slot >= QUAD * KEPT:
                slot, start = QUAD * (KEPT - 1) + s, first if kind == "B" else OCT * min(g - 5, 1)
            out.append((slot, N * s + w * g, w, start))
    return out


def place_of(kind, table, w, nth):
    return [t for t, v in enumerate(table[kind]) if v == w][nth]


def mode(j):
    return j if j < N // 2 else j - N


def kept(m):
    return THREE * abs(m) < N


def home_mode(lane, parity):
    block, p = divmod(lane, N)
    y, high, half = p // QUAD, p % QUAD // 2, p % QUAD
    if block < 2:
        row, col = THREE * block, 0
    elif block == 2:
        row, col, half = THREE * high, 1, p % 2
    elif p < 12:
        row, col = 1, 0
    elif p < 20:
        row, col, y = 2, 0, y + THREE
    else:
        row, col, half, y = 1 + high, 1, p % 2, y - 5 + 6 * high
    if y > SEVEN:
        return None
    ky, kz = mode(OCT * row + y), OCT * col + 2 * half + parity
    return (ky, kz) if kept(ky) and kept(kz) else None


def basis(kx, ky, kz):
    flat, full = math.hypot(kx, ky), math.hypot(kx, ky, kz)
    if full == 0:
        return np.zeros(THREE), np.zeros(THREE)
    if flat == 0:
        return np.array([1.0, 0, 0]), np.array([0, 1.0, 0])
    e1 = np.array([ky, -kx, 0]) / flat
    return e1, np.array([kx * kz, ky * kz, -flat * flat]) / (flat * full)


def split3(x):
    x = np.asarray(x, np.float32)
    hi = x.astype(BF16)
    rest = x - hi.astype(np.float32)
    mid = rest.astype(BF16)
    return hi, mid, (rest - mid.astype(np.float32)).astype(BF16)


def tables():
    scale = float(N) ** -1.5
    half = N // 2
    points = [(y, z) for z in range(1, OCT) for y in range(N)] + [(y, z) for z in (0, OCT) for y in range(half)]
    yy, zz = np.array(points).T
    inv = np.zeros((2, 2, LANES, K))
    wave = np.zeros((2, QUAD, LANES), np.float32)
    home = np.zeros((2, 5, KEPT, 1, LANES), np.float32)
    for parity in PAIR:
        for lane in range(LANES):
            got = home_mode(lane, parity)
            if got is None:
                continue
            ky, kz = got
            ang = UNIT * (ky * (yy + 0.5) + kz * zz)
            inv[parity, 0, lane] = scale * np.cos(ang)
            inv[parity, 1, lane] = -scale * np.sin(ang)
            wave[parity, :, lane] = ky * UNIT, kz * UNIT, math.cos(UNIT * ky / 2), math.sin(UNIT * ky / 2)
            for i, j in enumerate(SLOTS):
                e1, e2 = basis(mode(j), ky, kz)
                home[parity, :, i, 0, lane] = *e1[:2], *e2
    fwd = np.swapaxes(inv, 2, THREE)
    weight = np.full((2, 1, LANES, 1), 2.0)
    for lane in range(LANES):
        got = home_mode(lane, 0)
        if got is not None and got[1] == 0:
            weight[0, 0, lane] = 1.0
    inv3 = np.stack(split3(inv * weight))
    fwd3 = np.concatenate(split3(fwd), axis=THREE)
    return inv3, fwd3, wave, home


def source_tables():
    out = np.zeros((OCT, 2, HALF, THREE, LANES), np.float32)
    for kind, _, row, col in SOURCES:
        for t in range(len(RET[kind])):
            for n, lane, w, start in units(kind, RET, t):
                for o in range(w):
                    y, half = divmod(start // 2 + o, QUAD)
                    for parity in PAIR:
                        ky, kz = mode(OCT * row + y), OCT * col + 2 * half + parity
                        to = out[dev_of(row, col), parity, t, :, lane + o]
                        if n >= 2 * KEPT:
                            to[0] = 1
                        elif kept(ky) and kept(kz):
                            e1, e2 = basis(mode(SLOTS[n // 2]), ky, kz)
                            to[:] = (e2[1], e1[1], e2[2]) if n % 2 else (e1[0], e2[0], 0)
    return out.reshape(OCT, -1, LANES)


def cmul_const(a, c, s):
    re, im = a
    if abs(s) < TINY:
        return (re, im) if c > 0 else (-re, -im)
    if abs(c) < TINY:
        return (-im, re) if s > 0 else (im, -re)
    if abs(abs(c) - abs(s)) < TINY:
        p, q = (re - im) * abs(c), (re + im) * abs(c)
        if c > 0:
            return (p, q) if s > 0 else (q, -p)
        return (-q, p) if s > 0 else (-p, -q)
    return re * c - im * s, re * s + im * c


def fft(vals, sign):
    n = len(vals)
    if n == 1:
        return list(vals)
    even, odd = fft(vals[0::2], sign), fft(vals[1::2], sign)
    out = [None] * n
    for k in range(n // 2):
        a, b = even[k], odd[k]
        if b is not None:
            ang = sign * 2 * math.pi * k / n
            b = cmul_const(b, math.cos(ang), math.sin(ang))
        if a is None and b is None:
            continue
        if b is None:
            out[k], out[k + n // 2] = a, a
        elif a is None:
            out[k], out[k + n // 2] = b, (-b[0], -b[1])
        else:
            out[k] = (a[0] + b[0], a[1] + b[1])
            out[k + n // 2] = (a[0] - b[0], a[1] - b[1])
    return out


def dot(a, b):
    return jnp.dot(a, b, preferred_element_type=F32)


def split_bf16(x):
    hi = x.astype(BF16)
    rest = x - hi.astype(F32)
    mid = rest.astype(BF16)
    low = (rest - mid.astype(F32)).astype(BF16)
    return hi, mid, low


def dev_of(row, col):
    return col * QUAD + row


def kinds_here(row):
    tests = {"D": jnp.logical_or(row == 0, row == THREE), "A": row == 1, "B": row == 2}
    return list(tests.items())


def unrolled(n):
    def run(body):
        lax.fori_loop(0, n, lambda i, carry: (body(i), carry)[1], 0, unroll=True)
    return run


def roll(x, shift):
    shift %= LANES
    return pltpu.roll(x, shift, x.ndim - 1) if shift else x


def main_kernel(vre, vim, sre, sim, inv_hbm, fwd_hbm, wave_hbm, home_hbm, back,
                xin, send, recv_d, recv_a, recv_b, merged, lhs, phys, prod, spec, bins, res, ends, ret_d, ret_a, ret_b, stage,
                inv, fwd, wave, home, in_sem, tab_sem, own_sem, s1, r1, s2, r2):
    row, col, ens = lax.axis_index("row"), lax.axis_index("col"), lax.axis_index("ens")
    me = dev_of(row, col)
    recv = {"D": recv_d, "A": recv_a, "B": recv_b}
    ret = {"D": ret_d, "A": ret_a, "B": ret_b}
    mine = kinds_here(row)
    my_slot = {"D": col * 2 + jnp.where(row == THREE, 1, 0), "A": col, "B": col}

    loads = []
    for f in FIELDS:
        for ri in PAIR:
            src = (vre, vim)[ri].at[f] if f < THREE else (sre, sim)[ri].at[0]
            for half, (a, size, b) in enumerate(((0, LOW_ROWS, 0), (2 * LOW_ROWS, KEPT_ROWS - LOW_ROWS, LOW_ROWS))):
                cp = pltpu.make_async_copy(
                    src.at[pl.ds(a, size)], xin.at[ri, pl.ds(KEPT_ROWS * f + b, size)], in_sem.at[f, ri, half])
                loads.append(cp)
    first, later = loads[:OCT], loads[OCT:]
    for cp in first:
        cp.start()
    wanted = [(wave_hbm, wave), (fwd_hbm, fwd), (home_hbm, home)]
    wanted += [(inv_hbm.at[part], inv.at[:, :, pair, pl.ds(LANES * h, LANES)])
               for pair, parts in enumerate(((0, 2), (1, 1), (0, 0))) for h, part in enumerate(parts)]
    tab = [pltpu.make_async_copy(src, dst, tab_sem.at[i]) for i, (src, dst) in enumerate(wanted)]
    barrier = pltpu.get_barrier_semaphore()

    def peer(k):
        return row ^ (k % QUAD), col ^ (k // QUAD)

    for k in PEERS:
        pr, pc = peer(k)
        pl.semaphore_signal(barrier, inc=1, device_id=(ens, pc, pr), device_id_type=MESH)

    def pack(kind, lo, hi):
        if kind == "D":
            def body(n, carry):
                t, rb = lax.div(n, QUAD), lax.rem(n, QUAD)
                blk = xin[lax.div(rb, 2), pl.ds(t * K + lax.rem(rb, 2), LANES, stride=2), :]
                send[:, t, rb] = blk.T.reshape(OCT, *TILE)
                return carry
            lax.fori_loop(QUAD * lo, QUAD * hi, body, 0, unroll=QUAD)
            return

        def few(rb, carry):
            ri, b = lax.div(rb, 2), lax.rem(rb, 2)
            for t in range(lo, hi):
                parts = [xin[ri, pl.ds(slot * FLOWS + start + b, w, stride=2), :] for slot, _, w, start in units(kind, OUT, t)]
                if OUT[kind][t] < OCT:
                    for (_, lane, w, _), part in zip(units(kind, OUT, t), parts):
                        stage[lane:lane + w, :] = part
                    blk = stage[...]
                else:
                    order = np.argsort([u[1] for u in units(kind, OUT, t)])
                    blk = jnp.concatenate([parts[i] for i in order], axis=0)
                send[:, t, rb] = blk.T.reshape(OCT, *TILE)
            return carry
        lax.fori_loop(0, QUAD, few, 0)

    def remote(src, dst, sems, i, j, chunk, r, c):
        return pltpu.make_async_remote_copy(
            src_ref=src, dst_ref=dst, send_sem=sems[0].at[i, chunk], recv_sem=sems[1].at[j, chunk],
            device_id=(ens, c, r), device_id_type=MESH)

    def out_copy(kind, chunk, slot, r, c, frm):
        lo, hi = OUT_EDGES[kind][chunk:chunk + 2]
        to = dev_of(r, c)
        part = pl.ds(lo, hi - lo)
        return remote(send.at[to, part], recv[kind].at[slot, part], (s1, r1), to, frm, chunk, r, c)

    for chunk in FIELDS:
        for cp in (first, later, (), ())[chunk]:
            cp.wait()
        if chunk == 0:
            for cp in (*later, *tab):
                cp.start()
        for kind, here in mine:
            @pl.when(here)
            def _():
                pack(kind, *OUT_EDGES[kind][chunk:chunk + 2])
        if chunk == 0:
            pl.semaphore_wait(barrier, SEVEN)
        for kind, here in mine:
            @pl.when(here)
            def _():
                lo, hi = OUT_EDGES[kind][chunk:chunk + 2]
                for k in PEERS:
                    out_copy(kind, chunk, my_slot[kind], *peer(k), me).start()
                recv[kind][my_slot[kind], lo:hi] = send[me, lo:hi]

    lane = lax.broadcasted_iota(jnp.int32, TILE, 1)
    low = lane % QUAD < 2
    p32 = lane % N
    left, even = lane < FLOWS, lane % FLOWS < N

    def wait_chunk(chunk):
        for kind, slot, r, c in SOURCES:
            @pl.when(me != dev_of(r, c))
            def _():
                out_copy(kind, chunk, slot, r, c, dev_of(r, c)).wait_recv()

    def swap_blocks(tiles, forward):
        def outer(a, b, c, d):
            ca, db = roll(jnp.where(left, c, a), FLOWS), roll(jnp.where(left, d, b), FLOWS)
            return jnp.where(left, a, ca), jnp.where(left, b, db), jnp.where(left, ca, c), jnp.where(left, db, d)

        def inner(a, b, c, d):
            return (jnp.where(even, a, roll(b, N)), jnp.where(even, roll(a, -N), b),
                    jnp.where(even, c, roll(d, N)), jnp.where(even, roll(c, -N), d))
        return inner(*outer(*tiles)) if forward else outer(*inner(*tiles))

    def merge(lo, hi):
        cos, sin = wave[:, pl.ds(2, 1)], wave[:, pl.ds(THREE, 1)]
        for t in range(lo, hi):
            got = []
            for part in PARTS:
                d = [recv_d[o, t, part] for o in FIELDS]
                g, g4 = OCT * (t % QUAD), QUAD * (t % OCT)
                a4 = place_of("A", OUT, QUAD, t // OCT)
                a8, at = (a4, 20) if t == KEPT - 1 else (place_of("A", OUT, OCT, t // QUAD), g)
                c1 = jnp.where(low, d[2], roll(d[THREE], 2))
                v = [(roll(recv_a[c, a8, part], 20 * c - at), roll(recv_a[c, a4, part], 20 * c + OCT - g4),
                      roll(recv_b[c, t // QUAD, part], 10 * c + 12 - g)) for c in PAIR]
                rest = jnp.where(low, jnp.where(p32 < 28, v[1][0], v[1][1]), v[1][2])
                s1_ = jnp.where(p32 < OCT, v[0][0], jnp.where(p32 < 12, v[0][1], jnp.where(p32 < 20, v[0][2], rest)))
                got.append(swap_blocks((d[0], d[1], c1, s1_), True))
            for s, (re, im) in enumerate(zip(*got)):
                merged[RE, QUAD * t + s] = re * cos + im * sin
                merged[IM, QUAD * t + s] = im * cos - re * sin

    def to_x(f, get):
        vals = [None] * N
        for i, j in enumerate(SLOTS):
            vals[j] = get(i)
        out = fft(vals, 1)
        for x in range(0, N, 2):
            for ri in PAIR:
                hi, mid, lo = split_bf16(jnp.concatenate([out[x][ri], out[x + 1][ri]], axis=1))
                for p, part in enumerate((lo, hi, mid)):
                    lhs[:, ri, f, OCT * x:OCT * x + HALF, LANES * p:LANES * p + LANES] = part

    def field_x(f, src):
        to_x(f, lambda i: (merged[RE, src * KEPT + i], merged[IM, src * KEPT + i]))

    def curl_x(f):
        c1, c2 = (f + 1) % THREE, (f + 2) % THREE
        ky, kz = wave[:, pl.ds(0, 1)], wave[:, pl.ds(1, 1)]

        def get(i):
            ks = (UNIT * mode(SLOTS[i]), ky, kz)
            m1, m2 = c1 * KEPT + i, c2 * KEPT + i
            im = ks[c1] * merged[RE, m2] - ks[c2] * merged[RE, m1]
            re = ks[c2] * merged[IM, m1] - ks[c1] * merged[IM, m2]
            return re, im
        to_x(THREE + f, get)

    def to_grid(f):
        sums = []
        for b in PAIR:
            parts = []
            for ri in PAIR:
                low_hi, hi_mid = lhs[b, ri, f, :, 0:K], lhs[b, ri, f, :, LANES:LANES + K]
                acc = dot(low_hi, inv[b, ri, 0]) + dot(hi_mid, inv[b, ri, 1])
                parts.append(acc + dot(hi_mid, inv[b, ri, 2]))
            sums.append((parts[0] + parts[1], parts[0] - parts[1]))
        for side in PAIR:
            phys[2 * side, f] = sums[0][side] + sums[1][side]
            phys[2 * side + 1, f] = sums[0][side] - sums[1][side]

    def to_spec(c, parities):
        for b in parities:
            for ri in PAIR:
                hi, mid, lo = (prod[b, ri, p, c] for p in VEC)
                both = dot(hi, fwd[b, ri, :, 0:K]) + dot(mid, fwd[b, ri, :, 0:K])
                small = dot(lo, fwd[b, ri, :, 0:LANES]) + dot(hi, fwd[b, ri, :, K:])
                spec[b, ri, c] = small + both[:, LANES:] + both[:, :LANES]

    def product(c, point):
        for at in range(0, K, FLOWS):
            rows = slice(at, at + FLOWS)
            n = [point(lambda f: phys[q, f, rows]) for q in FIELDS]
            for b in PAIR:
                side = [n[0] - n[1], n[2] - n[THREE]] if b else [n[0] + n[1], n[2] + n[THREE]]
                for ri in PAIR:
                    v = side[0] - side[1] if ri else side[0] + side[1]
                    for p, part in enumerate(split_bf16(v)):
                        prod[b, ri, p, c, rows] = part

    def cross(c):
        c1, c2 = lax.rem(c + 1, THREE), lax.rem(c + 2, THREE)
        product(c, lambda at: at(c1) * at(THREE + c2) - at(c2) * at(THREE + c1))

    def flux(c):
        product(c, lambda at: at(c) * at(6))

    def from_x(c, lo, hi):
        vals = [tuple(spec[lo:hi, ri, c, OCT * x:OCT * x + OCT] for ri in PAIR) for x in range(N)]
        out = fft(vals, -1)
        for i, j in enumerate(SLOTS):
            bins[c, lo:hi, i], bins[c, lo + 2:hi + 2, i] = out[j]

    def phase(re, im, b):
        cos, sin = wave[b, pl.ds(2, 1)], wave[b, pl.ds(THREE, 1)]
        return re * cos - im * sin, re * sin + im * cos

    def project(b):
        for lo in range(0, KEPT, SEVEN):
            i = slice(lo, lo + SEVEN)
            e = [home[b, k, i] for k in range(5)]
            n = [[bins[c, 2 * ri + b, i] for c in VEC] for ri in PAIR]
            one = [e[0] * v[0] + e[1] * v[1] for v in n]
            two = [e[2] * v[0] + e[THREE] * v[1] + e[QUAD] * v[2] for v in n]
            for which, v in enumerate((one, two)):
                for ri, w in enumerate(phase(*v, b)):
                    res[b, ri, which, i] = w

    def diverge():
        for i, j in enumerate(SLOTS):
            ks = (UNIT * mode(j), wave[:, pl.ds(0, 1)], wave[:, pl.ds(1, 1)])
            re, im = phase(*[sum(ks[c] * bins[c, part, i] for c in VEC) for part in PARTS], slice(0, 2))
            res[:, 0, 2, i] = im
            res[:, 1, 2, i] = -re
        res[:, :, 2, KEPT] = jnp.zeros((2, 2, *TILE), F32)

    def result(n, b):
        return res[b, :, n % 2, n // 2] if n < 2 * KEPT else res[b, :, 2, n - 2 * KEPT]

    def unmerge(chunk, b):
        zero = jnp.zeros(TILE, F32)
        def dense(t, four):
            tiles = swap_blocks(four, False)
            ret_d[0, t, b], ret_d[1, t, b] = tiles[:2]
            ret_d[2, t, b] = jnp.where(low, tiles[2], zero)
            ret_d[THREE, t, b] = jnp.where(low, roll(tiles[2], -2), zero)
            ends[t, b] = tiles[THREE]

        def two_components(t, carry):
            dense(t, [res[b, :, s % 2, 2 * t + s // 2] for s in FIELDS])
            return carry

        lo, hi = RET_EDGES["D"][chunk:chunk + 2]
        if chunk < 2:
            lax.fori_loop(lo, hi, two_components, 0, unroll=2)
        else:
            for t in range(lo, hi):
                dense(t, [result(QUAD * t + s, b) for s in FIELDS])
        for kind in "AB":
            for t in range(*RET_EDGES[kind][chunk:chunk + 2]):
                w = RET[kind][t]
                per, nth = N // w, RET[kind][:t].count(w)
                for c in PAIR:
                    first = 12 + 10 * c if kind == "B" else 20 * c + OCT * (w < OCT)
                    v = None
                    for g in range(per):
                        part = roll(ends[per * nth + g, b], w * g - first)
                        v = part if v is None else jnp.where(p32 >= w * g, part, v)
                    ret[kind][c, t, b] = jnp.where(low, v, zero) if c else v

    def ret_part(kind, chunk):
        t, b = BACK[chunk]
        lo, hi = (RET_EDGES[kind][i] for i in t)
        return ret[kind], (pl.ds(lo, hi - lo), pl.ds(b[0], len(b)))

    def ret_copy(kind, chunk, slot, r, c, frm):
        src, part = ret_part(kind, chunk)
        return remote(src.at[slot, *part], back.at[frm, *part], (s2, r2), dev_of(r, c), frm, chunk, r, c)

    def own_copy(kind, chunk, slot, d):
        src, part = ret_part(kind, chunk)
        return pltpu.make_async_copy(src.at[slot, *part], back.at[d, *part], own_sem.at[chunk])

    def send_back(chunk):
        for kind, slot, r, c in SOURCES:
            d = dev_of(r, c)

            @pl.when(me != d)
            def _():
                ret_copy(kind, chunk, slot, r, c, me).start()

            @pl.when(me == d)
            def _():
                own_copy(kind, chunk, slot, d).start()

    tab[0].wait()
    for f in VEC:
        wait_chunk(f)
        merge(*OUT_EDGES["D"][f:f + 2])
        field_x(f, f)
        if f == 0:
            for cp in tab[THREE:]:
                cp.wait()
            to_grid(0)
        elif f == 1:
            curl_x(2)
            to_grid(1)
            to_grid(5)
    tab[1].wait()
    tab[2].wait()
    to_grid(2)
    curl_x(0)
    to_grid(THREE)
    curl_x(1)
    to_grid(QUAD)

    @unrolled(THREE)
    def _(c):
        cross(c)
        to_spec(c, (0,))
        from_x(c, 0, 1)

    def give(b):
        project(b)
        for chunk in PAIR:
            unmerge(chunk, b)
            if b + chunk != 1 or b == 0:
                send_back(2 if b else chunk)

    def second_parity(c, carry):
        to_spec(c, (1,))
        from_x(c, 1, 2)
        return carry

    give(0)
    lax.fori_loop(0, THREE, second_parity, 0)
    give(1)
    wait_chunk(THREE)
    merge(*OUT_EDGES["D"][THREE:])
    field_x(6, THREE)
    to_grid(6)
    def flux_part(c, carry):
        flux(c)
        to_spec(c, PAIR)
        from_x(c, 0, 2)
        return carry
    lax.fori_loop(0, THREE, flux_part, 0)

    diverge()
    lax.fori_loop(0, 2, lambda b, carry: (unmerge(2, b), carry)[1], 0)
    send_back(THREE)

    for kind, here in mine:
        @pl.when(here)
        def _():
            for k in PEERS:
                pr, pc = peer(k)
                for chunk in FIELDS:
                    out_copy(kind, chunk, my_slot[kind], pr, pc, me).wait_send()
                for chunk in range(len(BACK)):
                    ret_copy(kind, chunk, 0, pr, pc, dev_of(pr, pc)).wait_recv()

    for kind, slot, r, c in SOURCES:
        d = dev_of(r, c)

        @pl.when(me != d)
        def _():
            for chunk in range(len(BACK)):
                ret_copy(kind, chunk, slot, r, c, me).wait_send()

        @pl.when(me == d)
        def _():
            for chunk in range(len(BACK)):
                own_copy(kind, chunk, slot, d).wait()


def out_kernel(back_hbm, tab_hbm, ore, oim, tre, tim, buf, tab, back, blank, stage, sem, in_sem, tab_sem):
    row, col = lax.axis_index("row"), lax.axis_index("col")
    dense = kinds_here(row)[0][1]
    loads = [pltpu.make_async_copy(back_hbm.at[:, :, :, ri], back.at[:, :, :, ri], in_sem.at[ri])
             for ri in PAIR]
    load = pltpu.make_async_copy(tab_hbm.at[dev_of(row, col)], tab, tab_sem)
    for cp in (*loads, load):
        cp.start()
    odd = lax.broadcasted_iota(jnp.int32, (1, LANES), 1) % FLOWS >= N

    def store(f, ri, which):
        first = (0, LOW_ROWS, 2 * LOW_ROWS)[which]
        part = pl.ds(first, LOW_ROWS if which < 2 else ROWS - first)
        dst = (ore, oim)[ri].at[f] if f < THREE else (tre, tim)[ri].at[0]
        src = blank if which == 1 else buf.at[f, ri, part]
        return pltpu.make_async_copy(src, dst.at[part], sem.at[f, ri, which])

    blank[...] = jnp.zeros_like(blank)
    for f in FIELDS:
        for ri in PAIR:
            store(f, ri, 1).start()

    @pl.when(jnp.logical_not(dense))
    def _():
        for f in FIELDS:
            for ri in PAIR:
                for first, size in ((0, LOW_ROWS), (2 * LOW_ROWS, ROWS - 2 * LOW_ROWS)):
                    buf[f, ri, pl.ds(first, size), :] = jnp.zeros((size, FLOWS), F32)
    load.wait()

    def place(ri, b, kind, tile, t, shift, which):
        if RET[kind][t] < OCT:
            stage[...] = tile
        for n, lane, w, start in units(kind, RET, t):
            at = lane - N * shift
            if n < 2 * KEPT:
                if which and n % 2 == 0:
                    continue
                f, i = (2 if which else n % 2), n // 2
            elif which or n >= THREE * KEPT:
                continue
            else:
                f, i = THREE, n - 2 * KEPT
            part = stage[at:at + w, :] if w < OCT else tile[at:at + w]
            buf[f, ri, pl.ds(SLOTS[i] * FLOWS + b + start, w, stride=2), :] = part

    def rebuild(ri, kind):
        tiles = len(RET[kind])
        mixed = [t for t in range(tiles) if min(u[0] for u in units(kind, RET, t)) < 2 * KEPT]
        held = {}
        for t in range(tiles):
            for b in PAIR:
                v = back[:, t, b, ri].reshape(FLOWS, LANES)
                if t not in mixed:
                    place(ri, b, kind, v.T, t, 0, False)
                    continue
                k = [tab[pl.ds((b * HALF + t) * THREE + q, 1)] for q in VEC]
                other = jnp.where(odd, roll(v, N), roll(v, -N))
                place(ri, b, kind, (v * k[0] + other * k[1]).T, t, 0, False)
                z = v * k[2]
                if b in held:
                    old, zo = held.pop(b)
                    zt = jnp.where(odd, zo, roll(z, -N)).T
                    place(ri, b, kind, zt, old, 0, True)
                    place(ri, b, kind, zt, t, 1, True)
                elif t == mixed[-1]:
                    place(ri, b, kind, z.T, t, 0, True)
                else:
                    held[b] = t, z
            ends = (5, 10, 13, 15) if kind == "D" else ()
            if t in ends:
                e = ends.index(t)
                for f in VEC if e < 2 else (THREE,):
                    store(f, ri, 2 * (e % 2)).start()
        if kind != "D":
            for f in FIELDS:
                for which in (0, 2):
                    store(f, ri, which).start()

    for ri in PAIR:
        loads[ri].wait()

        for kind, here in kinds_here(row):
            @pl.when(here)
            def _():
                rebuild(ri, kind)
    for f in FIELDS:
        for ri in PAIR:
            for which in VEC:
                store(f, ri, which).wait()


def solution(mesh):
    spec_vec = P('ens', None, None, 'row', 'col')
    spec_scal = P('ens', None, 'row', 'col')
    consts = tables()
    src_np = source_tables()
    hbm = pl.BlockSpec(memory_space=pl.ANY)
    dma = pltpu.SemaphoreType.DMA
    links = dma((OCT, len(BACK)))

    def f32(*lead):
        return pltpu.VMEM((*lead, *TILE), F32)

    def local_term(vel_re, vel_im, scal_re, scal_im):
        vec = [jnp.transpose(a, (1, 2, THREE, QUAD, 0)).reshape(THREE, ROWS, FLOWS) for a in (vel_re, vel_im)]
        scal = [jnp.transpose(a, (1, 2, THREE, 0)).reshape(1, ROWS, FLOWS) for a in (scal_re, scal_im)]
        back = pl.pallas_call(
            main_kernel,
            out_shape=jax.ShapeDtypeStruct((OCT, HALF, 2, 2, *TILE), F32),
            in_specs=[hbm] * OCT,
            out_specs=hbm,
            scratch_shapes=[
                pltpu.VMEM((2, QUAD * KEPT_ROWS, FLOWS), F32), f32(OCT, len(OUT["D"]), QUAD),
                *[f32(2 * len(rows), len(OUT[kind]), QUAD) for kind, rows in KINDS.items()],
                f32(QUAD, QUAD * KEPT), pltpu.VMEM((2, 2, SEVEN, K, THREE * LANES), BF16), pltpu.VMEM((QUAD, SEVEN, K, K), F32),
                pltpu.VMEM((2, 2, THREE, THREE, K, K), BF16), pltpu.VMEM((2, 2, THREE, K, LANES), F32), f32(THREE, QUAD, KEPT),
                f32(2, 2, THREE, KEPT + 1), f32(HALF, 2, 2),
                *[f32(2 * len(rows), len(RET[kind]), 2, 2) for kind, rows in KINDS.items()], pltpu.VMEM((LANES, FLOWS), F32),
                pltpu.VMEM((2, 2, THREE, K, K), BF16), *[pltpu.VMEM(a.shape, a.dtype) for a in consts[1:]],
                dma((QUAD, 2, 2)), dma((9,)), dma((len(BACK),)), links, links, links, links,
            ],
            compiler_params=pltpu.CompilerParams(
                collective_id=0, has_side_effects=True, vmem_limit_bytes=60 * MIB),
            name="flow_home",
        )(*vec, *scal, *[jnp.asarray(a) for a in consts])
        outs = pl.pallas_call(
            out_kernel,
            out_shape=[jax.ShapeDtypeStruct((c, ROWS, FLOWS), F32) for c in (THREE, THREE, 1, 1)],
            in_specs=[hbm, hbm],
            out_specs=[hbm] * QUAD,
            scratch_shapes=[pltpu.VMEM((QUAD, 2, ROWS, FLOWS), F32), pltpu.VMEM(src_np.shape[1:], F32),
                            f32(OCT, HALF, 2, 2), pltpu.VMEM((LOW_ROWS, FLOWS), F32), pltpu.VMEM((LANES, FLOWS), F32), dma((QUAD, 2, THREE)), dma((2,)), dma],
            compiler_params=pltpu.CompilerParams(vmem_limit_bytes=60 * MIB),
            name="lay_out",
        )(back, jnp.asarray(src_np))
        out_v = [jnp.transpose(a.reshape(THREE, N, OCT, OCT, FLOWS), (QUAD, 0, 1, 2, THREE)) for a in outs[:2]]
        out_s = [jnp.transpose(a.reshape(N, OCT, OCT, FLOWS), (THREE, 0, 1, 2)) for a in outs[2:]]
        return (*out_v, *out_s)

    return jax.shard_map(local_term, mesh=mesh, in_specs=(spec_vec, spec_vec, spec_scal, spec_scal),
                         out_specs=(spec_vec, spec_vec, spec_scal, spec_scal), check_vma=False)
```

```python
import math

import jax
import jax.numpy as jnp
import numpy as np
from jax import lax
from jax.experimental import pallas as pl
from jax.experimental.pallas import tpu as pltpu
from jax.sharding import PartitionSpec as P

N = 32
LANES = 128
FLOWS = 64
ROWS = 2048
TILE = (8, LANES)
K = 256
TINY = 1e-9
MIB = 1 << 20
THREE, QUAD, SEVEN, OCT, HALF = 3, 4, 7, 8, 16
PARTS = RE, IM = slice(0, 2), slice(2, QUAD)
PAIR, VEC, FIELDS, PEERS = range(2), range(THREE), range(QUAD), range(1, OCT)
MESH = pl.DeviceIdType.MESH
F32 = jnp.float32
BF16 = jnp.bfloat16
UNIT = 2 * math.pi / N
SLOTS = list(range(11)) + list(range(22, N))
KEPT = len(SLOTS)
KEPT_ROWS = KEPT * FLOWS
LOW_ROWS = 11 * FLOWS
KINDS = {"D": (0, THREE), "A": (1,), "B": (2,)}
OUT = {"D": (N,) * 21, "A": (OCT, OCT, QUAD, OCT, QUAD, OCT, OCT, QUAD), "B": (OCT,) * 6}
RET = {"D": (N,) * HALF, "A": (OCT, OCT, QUAD, OCT, OCT, QUAD), "B": (OCT,) * QUAD}
OUT_EDGES = {"D": (0, 6, 11, HALF, 21), "A": (0, THREE, 5, 6, OCT), "B": (0, 2, THREE, QUAD, 6)}
RET_EDGES = {"D": (0, QUAD, 10, HALF), "A": (0, 1, THREE, 6), "B": (0, 1, 2, QUAD)}
BACK = [((0, 1), (0,)), ((1, 2), (0,)), ((0, 2), (1,)), ((2, THREE), (0, 1))]
SOURCES = [(kind, k * len(rows) + i, r, k) for kind, rows in KINDS.items() for k in PAIR for i, r in enumerate(rows)]


def units(kind, table, t):
    widths = table[kind]
    w = widths[t]
    per, nth = N // w, widths[:t].count(w)
    first = 48 if kind == "B" else HALF * (w == QUAD)
    out = []
    for s in FIELDS:
        for g in range(per):
            slot, start = QUAD * (per * nth + g) + s, first
            if slot >= QUAD * KEPT:
                slot, start = QUAD * (KEPT - 1) + s, first if kind == "B" else OCT * min(g - 5, 1)
            out.append((slot, N * s + w * g, w, start))
    return out


def place_of(kind, table, w, nth):
    return [t for t, v in enumerate(table[kind]) if v == w][nth]


def mode(j):
    return j if j < N // 2 else j - N


def kept(m):
    return THREE * abs(m) < N


def home_mode(lane, parity):
    block, p = divmod(lane, N)
    y, high, half = p // QUAD, p % QUAD // 2, p % QUAD
    if block < 2:
        row, col = THREE * block, 0
    elif block == 2:
        row, col, half = THREE * high, 1, p % 2
    elif p < 12:
        row, col = 1, 0
    elif p < 20:
        row, col, y = 2, 0, y + THREE
    else:
        row, col, half, y = 1 + high, 1, p % 2, y - 5 + 6 * high
    if y > SEVEN:
        return None
    ky, kz = mode(OCT * row + y), OCT * col + 2 * half + parity
    return (ky, kz) if kept(ky) and kept(kz) else None


def basis(kx, ky, kz):
    flat, full = math.hypot(kx, ky), math.hypot(kx, ky, kz)
    if full == 0:
        return np.zeros(THREE), np.zeros(THREE)
    if flat == 0:
        return np.array([1.0, 0, 0]), np.array([0, 1.0, 0])
    e1 = np.array([ky, -kx, 0]) / flat
    return e1, np.array([kx * kz, ky * kz, -flat * flat]) / (flat * full)


def split3(x):
    x = np.asarray(x, np.float32)
    hi = x.astype(BF16)
    rest = x - hi.astype(np.float32)
    mid = rest.astype(BF16)
    return hi, mid, (rest - mid.astype(np.float32)).astype(BF16)


def tables():
    scale = float(N) ** -1.5
    half = N // 2
    points = [(y, z) for z in range(1, OCT) for y in range(N)] + [(y, z) for z in (0, OCT) for y in range(half)]
    yy, zz = np.array(points).T
    inv = np.zeros((2, 2, LANES, K))
    wave = np.zeros((2, QUAD, LANES), np.float32)
    home = np.zeros((2, 5, KEPT, 1, LANES), np.float32)
    for parity in PAIR:
        for lane in range(LANES):
            got = home_mode(lane, parity)
            if got is None:
                continue
            ky, kz = got
            ang = UNIT * (ky * (yy + 0.5) + kz * zz)
            inv[parity, 0, lane] = scale * np.cos(ang)
            inv[parity, 1, lane] = -scale * np.sin(ang)
            wave[parity, :, lane] = ky * UNIT, kz * UNIT, math.cos(UNIT * ky / 2), math.sin(UNIT * ky / 2)
            for i, j in enumerate(SLOTS):
                e1, e2 = basis(mode(j), ky, kz)
                home[parity, :, i, 0, lane] = *e1[:2], *e2
    fwd = np.swapaxes(inv, 2, THREE)
    weight = np.full((2, 1, LANES, 1), 2.0)
    for lane in range(LANES):
        got = home_mode(lane, 0)
        if got is not None and got[1] == 0:
            weight[0, 0, lane] = 1.0
    inv3 = np.stack(split3(inv * weight))
    fwd3 = np.concatenate(split3(fwd), axis=THREE)
    return inv3, fwd3, wave, home


def source_tables():
    out = np.zeros((OCT, 2, HALF, THREE, LANES), np.float32)
    for kind, _, row, col in SOURCES:
        for t in range(len(RET[kind])):
            for n, lane, w, start in units(kind, RET, t):
                for o in range(w):
                    y, half = divmod(start // 2 + o, QUAD)
                    for parity in PAIR:
                        ky, kz = mode(OCT * row + y), OCT * col + 2 * half + parity
                        to = out[dev_of(row, col), parity, t, :, lane + o]
                        if n >= 2 * KEPT:
                            to[0] = 1
                        elif kept(ky) and kept(kz):
                            e1, e2 = basis(mode(SLOTS[n // 2]), ky, kz)
                            to[:] = (e2[1], e1[1], e2[2]) if n % 2 else (e1[0], e2[0], 0)
    return out.reshape(OCT, -1, LANES)


def cmul_const(a, c, s):
    re, im = a
    if abs(s) < TINY:
        return (re, im) if c > 0 else (-re, -im)
    if abs(c) < TINY:
        return (-im, re) if s > 0 else (im, -re)
    if abs(abs(c) - abs(s)) < TINY:
        p, q = (re - im) * abs(c), (re + im) * abs(c)
        if c > 0:
            return (p, q) if s > 0 else (q, -p)
        return (-q, p) if s > 0 else (-p, -q)
    return re * c - im * s, re * s + im * c


def fft(vals, sign):
    n = len(vals)
    if n == 1:
        return list(vals)
    even, odd = fft(vals[0::2], sign), fft(vals[1::2], sign)
    out = [None] * n
    for k in range(n // 2):
        a, b = even[k], odd[k]
        if b is not None:
            ang = sign * 2 * math.pi * k / n
            b = cmul_const(b, math.cos(ang), math.sin(ang))
        if a is None and b is None:
            continue
        if b is None:
            out[k], out[k + n // 2] = a, a
        elif a is None:
            out[k], out[k + n // 2] = b, (-b[0], -b[1])
        else:
            out[k] = (a[0] + b[0], a[1] + b[1])
            out[k + n // 2] = (a[0] - b[0], a[1] - b[1])
    return out


def dot(a, b):
    return jnp.dot(a, b, preferred_element_type=F32)


def split_bf16(x):
    hi = x.astype(BF16)
    rest = x - hi.astype(F32)
    mid = rest.astype(BF16)
    low = (rest - mid.astype(F32)).astype(BF16)
    return hi, mid, low


def dev_of(row, col):
    return col * QUAD + row


def kinds_here(row):
    tests = {"D": jnp.logical_or(row == 0, row == THREE), "A": row == 1, "B": row == 2}
    return list(tests.items())


def unrolled(n):
    def run(body):
        lax.fori_loop(0, n, lambda i, carry: (body(i), carry)[1], 0, unroll=True)
    return run


def roll(x, shift):
    shift %= LANES
    return pltpu.roll(x, shift, x.ndim - 1) if shift else x


def main_kernel(vre, vim, sre, sim, inv_hbm, fwd_hbm, wave_hbm, home_hbm, back,
                xin, send, recv_d, recv_a, recv_b, merged, lhs, phys, prod, spec, bins, res, ends, ret_d, ret_a, ret_b, stage,
                inv, fwd, wave, home, in_sem, tab_sem, own_sem, s1, r1, s2, r2):
    row, col, ens = lax.axis_index("row"), lax.axis_index("col"), lax.axis_index("ens")
    me = dev_of(row, col)
    recv = {"D": recv_d, "A": recv_a, "B": recv_b}
    ret = {"D": ret_d, "A": ret_a, "B": ret_b}
    mine = kinds_here(row)
    my_slot = {"D": col * 2 + jnp.where(row == THREE, 1, 0), "A": col, "B": col}

    loads = []
    for f in FIELDS:
        for ri in PAIR:
            src = (vre, vim)[ri].at[f] if f < THREE else (sre, sim)[ri].at[0]
            for half, (a, size, b) in enumerate(((0, LOW_ROWS, 0), (2 * LOW_ROWS, KEPT_ROWS - LOW_ROWS, LOW_ROWS))):
                cp = pltpu.make_async_copy(
                    src.at[pl.ds(a, size)], xin.at[ri, pl.ds(KEPT_ROWS * f + b, size)], in_sem.at[f, ri, half])
                loads.append(cp)
    first, later = loads[:OCT], loads[OCT:]
    for cp in first:
        cp.start()
    wanted = [(wave_hbm, wave), (fwd_hbm, fwd), (home_hbm, home)]
    wanted += [(inv_hbm.at[part], inv.at[:, :, pair, pl.ds(LANES * h, LANES)])
               for pair, parts in enumerate(((0, 2), (1, 1), (0, 0))) for h, part in enumerate(parts)]
    tab = [pltpu.make_async_copy(src, dst, tab_sem.at[i]) for i, (src, dst) in enumerate(wanted)]
    barrier = pltpu.get_barrier_semaphore()

    def peer(k):
        return row ^ (k % QUAD), col ^ (k // QUAD)

    for k in PEERS:
        pr, pc = peer(k)
        pl.semaphore_signal(barrier, inc=1, device_id=(ens, pc, pr), device_id_type=MESH)

    def pack(kind, lo, hi):
        if kind == "D":
            def body(n, carry):
                t, rb = lax.div(n, QUAD), lax.rem(n, QUAD)
                blk = xin[lax.div(rb, 2), pl.ds(t * K + lax.rem(rb, 2), LANES, stride=2), :]
                send[:, t, rb] = blk.T.reshape(OCT, *TILE)
                return carry
            lax.fori_loop(QUAD * lo, QUAD * hi, body, 0, unroll=2)
            return

        def few(rb, carry):
            ri, b = lax.div(rb, 2), lax.rem(rb, 2)
            for t in range(lo, hi):
                parts = [xin[ri, pl.ds(slot * FLOWS + start + b, w, stride=2), :] for slot, _, w, start in units(kind, OUT, t)]
                if OUT[kind][t] < OCT:
                    for (_, lane, w, _), part in zip(units(kind, OUT, t), parts):
                        stage[lane:lane + w, :] = part
                    blk = stage[...]
                else:
                    order = np.argsort([u[1] for u in units(kind, OUT, t)])
                    blk = jnp.concatenate([parts[i] for i in order], axis=0)
                send[:, t, rb] = blk.T.reshape(OCT, *TILE)
            return carry
        lax.fori_loop(0, QUAD, few, 0)

    def remote(src, dst, sems, i, j, chunk, r, c):
        return pltpu.make_async_remote_copy(
            src_ref=src, dst_ref=dst, send_sem=sems[0].at[i, chunk], recv_sem=sems[1].at[j, chunk],
            device_id=(ens, c, r), device_id_type=MESH)

    def out_copy(kind, chunk, slot, r, c, frm):
        lo, hi = OUT_EDGES[kind][chunk:chunk + 2]
        to = dev_of(r, c)
        part = pl.ds(lo, hi - lo)
        return remote(send.at[to, part], recv[kind].at[slot, part], (s1, r1), to, frm, chunk, r, c)

    for chunk in FIELDS:
        for cp in (first, later, (), ())[chunk]:
            cp.wait()
        if chunk == 0:
            for cp in (*later, *tab):
                cp.start()
        for kind, here in mine:
            @pl.when(here)
            def _():
                pack(kind, *OUT_EDGES[kind][chunk:chunk + 2])
        if chunk == 0:
            pl.semaphore_wait(barrier, SEVEN)
        for kind, here in mine:
            @pl.when(here)
            def _():
                lo, hi = OUT_EDGES[kind][chunk:chunk + 2]
                for k in PEERS:
                    out_copy(kind, chunk, my_slot[kind], *peer(k), me).start()
                recv[kind][my_slot[kind], lo:hi] = send[me, lo:hi]

    lane = lax.broadcasted_iota(jnp.int32, TILE, 1)
    low = lane % QUAD < 2
    p32 = lane % N
    left, even = lane < FLOWS, lane % FLOWS < N

    def wait_chunk(chunk):
        for kind, slot, r, c in SOURCES:
            @pl.when(me != dev_of(r, c))
            def _():
                out_copy(kind, chunk, slot, r, c, dev_of(r, c)).wait_recv()

    def swap_blocks(tiles, forward):
        def outer(a, b, c, d):
            ca, db = roll(jnp.where(left, c, a), FLOWS), roll(jnp.where(left, d, b), FLOWS)
            return jnp.where(left, a, ca), jnp.where(left, b, db), jnp.where(left, ca, c), jnp.where(left, db, d)

        def inner(a, b, c, d):
            return (jnp.where(even, a, roll(b, N)), jnp.where(even, roll(a, -N), b),
                    jnp.where(even, c, roll(d, N)), jnp.where(even, roll(c, -N), d))
        return inner(*outer(*tiles)) if forward else outer(*inner(*tiles))

    def merge(lo, hi):
        cos, sin = wave[:, pl.ds(2, 1)], wave[:, pl.ds(THREE, 1)]
        for t in range(lo, hi):
            got = []
            for part in PARTS:
                d = [recv_d[o, t, part] for o in FIELDS]
                g, g4 = OCT * (t % QUAD), QUAD * (t % OCT)
                a4 = place_of("A", OUT, QUAD, t // OCT)
                a8, at = (a4, 20) if t == KEPT - 1 else (place_of("A", OUT, OCT, t // QUAD), g)
                c1 = jnp.where(low, d[2], roll(d[THREE], 2))
                v = [(roll(recv_a[c, a8, part], 20 * c - at), roll(recv_a[c, a4, part], 20 * c + OCT - g4),
                      roll(recv_b[c, t // QUAD, part], 10 * c + 12 - g)) for c in PAIR]
                rest = jnp.where(low, jnp.where(p32 < 28, v[1][0], v[1][1]), v[1][2])
                s1_ = jnp.where(p32 < OCT, v[0][0], jnp.where(p32 < 12, v[0][1], jnp.where(p32 < 20, v[0][2], rest)))
                got.append(swap_blocks((d[0], d[1], c1, s1_), True))
            for s, (re, im) in enumerate(zip(*got)):
                merged[RE, QUAD * t + s] = re * cos + im * sin
                merged[IM, QUAD * t + s] = im * cos - re * sin

    def to_x(f, get):
        vals = [None] * N
        for i, j in enumerate(SLOTS):
            vals[j] = get(i)
        out = fft(vals, 1)
        for x in range(0, N, 2):
            for ri in PAIR:
                hi, mid, lo = split_bf16(jnp.concatenate([out[x][ri], out[x + 1][ri]], axis=1))
                for p, part in enumerate((lo, hi, mid)):
                    lhs[:, ri, f, OCT * x:OCT * x + HALF, LANES * p:LANES * p + LANES] = part

    def field_x(f, src):
        to_x(f, lambda i: (merged[RE, src * KEPT + i], merged[IM, src * KEPT + i]))

    def curl_x(f):
        c1, c2 = (f + 1) % THREE, (f + 2) % THREE
        ky, kz = wave[:, pl.ds(0, 1)], wave[:, pl.ds(1, 1)]

        def get(i):
            ks = (UNIT * mode(SLOTS[i]), ky, kz)
            m1, m2 = c1 * KEPT + i, c2 * KEPT + i
            im = ks[c1] * merged[RE, m2] - ks[c2] * merged[RE, m1]
            re = ks[c2] * merged[IM, m1] - ks[c1] * merged[IM, m2]
            return re, im
        to_x(THREE + f, get)

    def to_grid(f):
        sums = []
        for b in PAIR:
            parts = []
            for ri in PAIR:
                low_hi, hi_mid = lhs[b, ri, f, :, 0:K], lhs[b, ri, f, :, LANES:LANES + K]
                acc = dot(low_hi, inv[b, ri, 0]) + dot(hi_mid, inv[b, ri, 1])
                parts.append(acc + dot(hi_mid, inv[b, ri, 2]))
            sums.append((parts[0] + parts[1], parts[0] - parts[1]))
        for side in PAIR:
            phys[2 * side, f] = sums[0][side] + sums[1][side]
            phys[2 * side + 1, f] = sums[0][side] - sums[1][side]

    def to_spec(c, parities):
        for b in parities:
            for ri in PAIR:
                hi, mid, lo = (prod[b, ri, p, c] for p in VEC)
                both = dot(hi, fwd[b, ri, :, 0:K]) + dot(mid, fwd[b, ri, :, 0:K])
                small = dot(lo, fwd[b, ri, :, 0:LANES]) + dot(hi, fwd[b, ri, :, K:])
                spec[b, ri, c] = small + both[:, LANES:] + both[:, :LANES]

    def product(c, point):
        for at in range(0, K, FLOWS):
            rows = slice(at, at + FLOWS)
            n = [point(lambda f: phys[q, f, rows]) for q in FIELDS]
            for b in PAIR:
                side = [n[0] - n[1], n[2] - n[THREE]] if b else [n[0] + n[1], n[2] + n[THREE]]
                for ri in PAIR:
                    v = side[0] - side[1] if ri else side[0] + side[1]
                    for p, part in enumerate(split_bf16(v)):
                        prod[b, ri, p, c, rows] = part

    def cross(c):
        c1, c2 = lax.rem(c + 1, THREE), lax.rem(c + 2, THREE)
        product(c, lambda at: at(c1) * at(THREE + c2) - at(c2) * at(THREE + c1))

    def flux(c):
        product(c, lambda at: at(c) * at(6))

    def from_x(c, lo, hi):
        vals = [tuple(spec[lo:hi, ri, c, OCT * x:OCT * x + OCT] for ri in PAIR) for x in range(N)]
        out = fft(vals, -1)
        for i, j in enumerate(SLOTS):
            bins[c, lo:hi, i], bins[c, lo + 2:hi + 2, i] = out[j]

    def phase(re, im, b):
        cos, sin = wave[b, pl.ds(2, 1)], wave[b, pl.ds(THREE, 1)]
        return re * cos - im * sin, re * sin + im * cos

    def project(b):
        for lo in range(0, KEPT, SEVEN):
            i = slice(lo, lo + SEVEN)
            e = [home[b, k, i] for k in range(5)]
            n = [[bins[c, 2 * ri + b, i] for c in VEC] for ri in PAIR]
            one = [e[0] * v[0] + e[1] * v[1] for v in n]
            two = [e[2] * v[0] + e[THREE] * v[1] + e[QUAD] * v[2] for v in n]
            for which, v in enumerate((one, two)):
                for ri, w in enumerate(phase(*v, b)):
                    res[b, ri, which, i] = w

    def diverge():
        for i, j in enumerate(SLOTS):
            ks = (UNIT * mode(j), wave[:, pl.ds(0, 1)], wave[:, pl.ds(1, 1)])
            re, im = phase(*[sum(ks[c] * bins[c, part, i] for c in VEC) for part in PARTS], slice(0, 2))
            res[:, 0, 2, i] = im
            res[:, 1, 2, i] = -re
        res[:, :, 2, KEPT] = jnp.zeros((2, 2, *TILE), F32)

    def result(n, b):
        return res[b, :, n % 2, n // 2] if n < 2 * KEPT else res[b, :, 2, n - 2 * KEPT]

    def unmerge(chunk, b):
        zero = jnp.zeros(TILE, F32)
        def dense(t, four):
            tiles = swap_blocks(four, False)
            ret_d[0, t, b], ret_d[1, t, b] = tiles[:2]
            ret_d[2, t, b] = jnp.where(low, tiles[2], zero)
            ret_d[THREE, t, b] = jnp.where(low, roll(tiles[2], -2), zero)
            ends[t, b] = tiles[THREE]

        def two_components(t, carry):
            dense(t, [res[b, :, s % 2, 2 * t + s // 2] for s in FIELDS])
            return carry

        lo, hi = RET_EDGES["D"][chunk:chunk + 2]
        if chunk < 2:
            lax.fori_loop(lo, hi, two_components, 0, unroll=2 if chunk else QUAD)
        else:
            for t in range(lo, hi):
                dense(t, [result(QUAD * t + s, b) for s in FIELDS])
        for kind in "AB":
            for t in range(*RET_EDGES[kind][chunk:chunk + 2]):
                w = RET[kind][t]
                per, nth = N // w, RET[kind][:t].count(w)
                for c in PAIR:
                    first = 12 + 10 * c if kind == "B" else 20 * c + OCT * (w < OCT)
                    v = None
                    for g in range(per):
                        part = roll(ends[per * nth + g, b], w * g - first)
                        v = part if v is None else jnp.where(p32 >= w * g, part, v)
                    ret[kind][c, t, b] = jnp.where(low, v, zero) if c else v

    def ret_part(kind, chunk):
        t, b = BACK[chunk]
        lo, hi = (RET_EDGES[kind][i] for i in t)
        return ret[kind], (pl.ds(lo, hi - lo), pl.ds(b[0], len(b)))

    def ret_copy(kind, chunk, slot, r, c, frm):
        src, part = ret_part(kind, chunk)
        return remote(src.at[slot, *part], back.at[frm, *part], (s2, r2), dev_of(r, c), frm, chunk, r, c)

    def own_copy(kind, chunk, slot, d):
        src, part = ret_part(kind, chunk)
        return pltpu.make_async_copy(src.at[slot, *part], back.at[d, *part], own_sem.at[chunk])

    def send_back(chunk):
        for kind, slot, r, c in SOURCES:
            d = dev_of(r, c)

            @pl.when(me != d)
            def _():
                ret_copy(kind, chunk, slot, r, c, me).start()

            @pl.when(me == d)
            def _():
                own_copy(kind, chunk, slot, d).start()

    tab[0].wait()
    for f in VEC:
        wait_chunk(f)
        merge(*OUT_EDGES["D"][f:f + 2])
        field_x(f, f)
        if f == 0:
            for cp in tab[THREE:]:
                cp.wait()
            to_grid(0)
        elif f == 1:
            curl_x(2)
            to_grid(1)
            to_grid(5)
    tab[1].wait()
    tab[2].wait()
    to_grid(2)
    curl_x(0)
    to_grid(THREE)
    curl_x(1)
    to_grid(QUAD)

    @unrolled(THREE)
    def _(c):
        cross(c)
        to_spec(c, (0,))
        from_x(c, 0, 1)

    def give(b):
        project(b)
        for chunk in PAIR:
            unmerge(chunk, b)
            if b + chunk != 1 or b == 0:
                send_back(2 if b else chunk)

    def second_parity(c, carry):
        to_spec(c, (1,))
        from_x(c, 1, 2)
        return carry

    give(0)
    lax.fori_loop(0, THREE, second_parity, 0)
    give(1)
    wait_chunk(THREE)
    merge(*OUT_EDGES["D"][THREE:])
    field_x(6, THREE)
    to_grid(6)
    def flux_part(c, carry):
        flux(c)
        to_spec(c, PAIR)
        from_x(c, 0, 2)
        return carry
    lax.fori_loop(0, THREE, flux_part, 0)

    diverge()
    lax.fori_loop(0, 2, lambda b, carry: (unmerge(2, b), carry)[1], 0)
    send_back(THREE)

    for kind, here in mine:
        @pl.when(here)
        def _():
            for k in PEERS:
                pr, pc = peer(k)
                for chunk in FIELDS:
                    out_copy(kind, chunk, my_slot[kind], pr, pc, me).wait_send()
                for chunk in range(len(BACK)):
                    ret_copy(kind, chunk, 0, pr, pc, dev_of(pr, pc)).wait_recv()

    for kind, slot, r, c in SOURCES:
        d = dev_of(r, c)

        @pl.when(me != d)
        def _():
            for chunk in range(len(BACK)):
                ret_copy(kind, chunk, slot, r, c, me).wait_send()

        @pl.when(me == d)
        def _():
            for chunk in range(len(BACK)):
                own_copy(kind, chunk, slot, d).wait()


def out_kernel(back_hbm, tab_hbm, ore, oim, tre, tim, buf, tab, back, blank, stage, sem, in_sem, tab_sem):
    row, col = lax.axis_index("row"), lax.axis_index("col")
    dense = kinds_here(row)[0][1]
    loads = [pltpu.make_async_copy(back_hbm.at[:, :, :, ri], back.at[:, :, :, ri], in_sem.at[ri])
             for ri in PAIR]
    load = pltpu.make_async_copy(tab_hbm.at[dev_of(row, col)], tab, tab_sem)
    for cp in (*loads, load):
        cp.start()
    odd = lax.broadcasted_iota(jnp.int32, (1, LANES), 1) % FLOWS >= N

    def store(f, ri, which):
        first = (0, LOW_ROWS, 2 * LOW_ROWS)[which]
        part = pl.ds(first, LOW_ROWS if which < 2 else ROWS - first)
        dst = (ore, oim)[ri].at[f] if f < THREE else (tre, tim)[ri].at[0]
        src = blank if which == 1 else buf.at[f, ri, part]
        return pltpu.make_async_copy(src, dst.at[part], sem.at[f, ri, which])

    blank[...] = jnp.zeros_like(blank)
    for f in FIELDS:
        for ri in PAIR:
            store(f, ri, 1).start()

    @pl.when(jnp.logical_not(dense))
    def _():
        for f in FIELDS:
            for ri in PAIR:
                for first, size in ((0, LOW_ROWS), (2 * LOW_ROWS, ROWS - 2 * LOW_ROWS)):
                    buf[f, ri, pl.ds(first, size), :] = jnp.zeros((size, FLOWS), F32)
    load.wait()

    def place(ri, b, kind, tile, t, shift, which):
        if RET[kind][t] < OCT:
            stage[...] = tile
        for n, lane, w, start in units(kind, RET, t):
            at = lane - N * shift
            if n < 2 * KEPT:
                if which and n % 2 == 0:
                    continue
                f, i = (2 if which else n % 2), n // 2
            elif which or n >= THREE * KEPT:
                continue
            else:
                f, i = THREE, n - 2 * KEPT
            part = stage[at:at + w, :] if w < OCT else tile[at:at + w]
            buf[f, ri, pl.ds(SLOTS[i] * FLOWS + b + start, w, stride=2), :] = part

    def rebuild(ri, kind):
        tiles = len(RET[kind])
        mixed = [t for t in range(tiles) if min(u[0] for u in units(kind, RET, t)) < 2 * KEPT]
        held = {}
        for t in range(tiles):
            for b in PAIR:
                v = back[:, t, b, ri].reshape(FLOWS, LANES)
                if t not in mixed:
                    place(ri, b, kind, v.T, t, 0, False)
                    continue
                k = [tab[pl.ds((b * HALF + t) * THREE + q, 1)] for q in VEC]
                other = jnp.where(odd, roll(v, N), roll(v, -N))
                place(ri, b, kind, (v * k[0] + other * k[1]).T, t, 0, False)
                z = v * k[2]
                if b in held:
                    old, zo = held.pop(b)
                    zt = jnp.where(odd, zo, roll(z, -N)).T
                    place(ri, b, kind, zt, old, 0, True)
                    place(ri, b, kind, zt, t, 1, True)
                elif t == mixed[-1]:
                    place(ri, b, kind, z.T, t, 0, True)
                else:
                    held[b] = t, z
            ends = (5, 10, 13, 15) if kind == "D" else ()
            if t in ends:
                e = ends.index(t)
                for f in VEC if e < 2 else (THREE,):
                    store(f, ri, 2 * (e % 2)).start()
        if kind != "D":
            for f in FIELDS:
                for which in (0, 2):
                    store(f, ri, which).start()

    for ri in PAIR:
        loads[ri].wait()

        for kind, here in kinds_here(row):
            @pl.when(here)
            def _():
                rebuild(ri, kind)
    for f in FIELDS:
        for ri in PAIR:
            for which in VEC:
                store(f, ri, which).wait()


def solution(mesh):
    spec_vec = P('ens', None, None, 'row', 'col')
    spec_scal = P('ens', None, 'row', 'col')
    consts = tables()
    src_np = source_tables()
    hbm = pl.BlockSpec(memory_space=pl.ANY)
    dma = pltpu.SemaphoreType.DMA
    links = dma((OCT, len(BACK)))

    def f32(*lead):
        return pltpu.VMEM((*lead, *TILE), F32)

    def local_term(vel_re, vel_im, scal_re, scal_im):
        vec = [jnp.transpose(a, (1, 2, THREE, QUAD, 0)).reshape(THREE, ROWS, FLOWS) for a in (vel_re, vel_im)]
        scal = [jnp.transpose(a, (1, 2, THREE, 0)).reshape(1, ROWS, FLOWS) for a in (scal_re, scal_im)]
        back = pl.pallas_call(
            main_kernel,
            out_shape=jax.ShapeDtypeStruct((OCT, HALF, 2, 2, *TILE), F32),
            in_specs=[hbm] * OCT,
            out_specs=hbm,
            scratch_shapes=[
                pltpu.VMEM((2, QUAD * KEPT_ROWS, FLOWS), F32), f32(OCT, len(OUT["D"]), QUAD),
                *[f32(2 * len(rows), len(OUT[kind]), QUAD) for kind, rows in KINDS.items()],
                f32(QUAD, QUAD * KEPT), pltpu.VMEM((2, 2, SEVEN, K, THREE * LANES), BF16), pltpu.VMEM((QUAD, SEVEN, K, K), F32),
                pltpu.VMEM((2, 2, THREE, THREE, K, K), BF16), pltpu.VMEM((2, 2, THREE, K, LANES), F32), f32(THREE, QUAD, KEPT),
                f32(2, 2, THREE, KEPT + 1), f32(HALF, 2, 2),
                *[f32(2 * len(rows), len(RET[kind]), 2, 2) for kind, rows in KINDS.items()], pltpu.VMEM((LANES, FLOWS), F32),
                pltpu.VMEM((2, 2, THREE, K, K), BF16), *[pltpu.VMEM(a.shape, a.dtype) for a in consts[1:]],
                dma((QUAD, 2, 2)), dma((9,)), dma((len(BACK),)), links, links, links, links,
            ],
            compiler_params=pltpu.CompilerParams(
                collective_id=0, has_side_effects=True, vmem_limit_bytes=60 * MIB),
            name="flow_home",
        )(*vec, *scal, *[jnp.asarray(a) for a in consts])
        outs = pl.pallas_call(
            out_kernel,
            out_shape=[jax.ShapeDtypeStruct((c, ROWS, FLOWS), F32) for c in (THREE, THREE, 1, 1)],
            in_specs=[hbm, hbm],
            out_specs=[hbm] * QUAD,
            scratch_shapes=[pltpu.VMEM((QUAD, 2, ROWS, FLOWS), F32), pltpu.VMEM(src_np.shape[1:], F32),
                            f32(OCT, HALF, 2, 2), pltpu.VMEM((LOW_ROWS, FLOWS), F32), pltpu.VMEM((LANES, FLOWS), F32), dma((QUAD, 2, THREE)), dma((2,)), dma],
            compiler_params=pltpu.CompilerParams(vmem_limit_bytes=60 * MIB),
            name="lay_out",
        )(back, jnp.asarray(src_np))
        out_v = [jnp.transpose(a.reshape(THREE, N, OCT, OCT, FLOWS), (QUAD, 0, 1, 2, THREE)) for a in outs[:2]]
        out_s = [jnp.transpose(a.reshape(N, OCT, OCT, FLOWS), (THREE, 0, 1, 2)) for a in outs[2:]]
        return (*out_v, *out_s)

    return jax.shard_map(local_term, mesh=mesh, in_specs=(spec_vec, spec_vec, spec_scal, spec_scal),
                         out_specs=(spec_vec, spec_vec, spec_scal, spec_scal), check_vma=False)
```
